32 devices in a mesh: shard: 4 (over x, core), context: 4 (over z), tensor: 2 (over y).
Axes of the slice: x: 2, y: 2, z: 4, core: 2. Of those that a mesh axis runs over, the one named last changes fastest.
Arguments:
- hidden_in: bfloat16 [2048, 1536], P(('shard', 'context')), may hold values from -6 to 6
- segment_ids: int32 [4, 512], P('shard'), may hold values from 0 to 2, never falling along the last dimension, each value on 1 to 256 neighbouring positions
- attn_gain: bfloat16 [1536], P(('shard', 'context')), may hold values from 0.25 to 1.75
- qkv_weight: bfloat16 [1536, 2048], P(('shard', 'context'), 'tensor'), may hold values from -0.15625 to 0.15625
- qkv_bias: bfloat16 [16, 128], P('tensor', ('shard', 'context')), may hold values from -3 to 3
- out_weight: bfloat16 [1536, 1536], P('tensor', ('shard', 'context')), may hold values from -0.625 to 0.625
- ffn_gain: bfloat16 [1536], P(('shard', 'context')), may hold values from 0.25 to 1.75
- gate_weight: bfloat16 [1536, 8960], P(('shard', 'context'), 'tensor'), may hold values from -0.15625 to 0.15625
- up_weight: bfloat16 [1536, 8960], P(('shard', 'context'), 'tensor'), may hold values from -0.15625 to 0.15625
- down_weight: bfloat16 [8960, 1536], P('tensor', ('shard', 'context')), may hold values from -0.0625 to 0.0625
- out_cotangent: bfloat16 [2048, 1536], P(('shard', 'context')), may hold values from -6 to 6
Outputs:
- block_out: bfloat16 [2048, 1536], P(('shard', 'context'))
- input_grad: float32 [2048, 1536], P(('shard', 'context'))
- attn_gain_grad: float32 [1536], P(('shard', 'context'))
- qkv_weight_grad: float32 [1536, 2048], P(('shard', 'context'), 'tensor')
- qkv_bias_grad: float32 [16, 128], P('tensor', ('shard', 'context'))
- out_weight_grad: float32 [1536, 1536], P('tensor', ('shard', 'context'))
- ffn_gain_grad: float32 [1536], P(('shard', 'context'))
- gate_weight_grad: float32 [1536, 8960], P(('shard', 'context'), 'tensor')
- up_weight_grad: float32 [1536, 8960], P(('shard', 'context'), 'tensor')
- down_weight_grad: float32 [8960, 1536], P('tensor', ('shard', 'context'))
The draws below stay inside these ranges and needn't reach their ends.
Inputs may be any that keep to these rules, and one draw needn't show every extreme that they name: `segment_ids`: in every group the sequence numbers start at 0 and never fall; a sequence has at most 256 tokens, and one sequence of each group has exactly 256.
All inputs are finite; a program needn't handle non-finite values.
Results may differ from the reference program's by a relative error of at most 0.018.
Values may be sent and summed in bfloat16 or wider, within the bound.
A program may use at most 256 MiB of HBM per device.

```python
import math
import jax
import jax.numpy as jnp
import numpy as np
from jax import lax

D = 1536
H = 12
KVH = 2
HD = 128
FF = 8960
SEQS = 3
GROUP = 512
GROUPS = 4
TOKENS = 2048
MAXLEN = 256
HQ = 1536
HEADS_ALL = 16
QKV = 2048
N_TENSOR = 2


def block_levels(rng, dims, split, smallest, largest):
    loudness, own = 1.0, jax.random.fold_in(rng, 6)
    for axis_at, blocks in split:
        heights = jnp.exp(jax.random.uniform(jax.random.fold_in(own, axis_at), (blocks,), jnp.float32, smallest / len(split), largest / len(split)))
        loudness = loudness * jnp.repeat(heights, dims[axis_at] // blocks).reshape([-1 if axis == axis_at else 1 for axis in range(len(dims))])
    return loudness


def length_profile(number_of, total, reach, lean):
    loads = [(1 << 20) // math.isqrt(standing ** lean) + 1 for standing in range(2, number_of + 1)]
    rest, given = total - reach - (number_of - 1), [1] * (number_of - 1)
    while rest > 0:
        movable = [i for i in range(number_of - 1) if given[i] < reach]
        pool, budget = sum([loads[i] for i in movable]), rest
        for i in movable:
            more = min(reach - given[i], max(1, budget * loads[i] // pool), rest)
            given[i] = given[i] + more
            rest = rest - more
    return np.array([reach] + given)


def ragged(rng, count, total, most, slope):
    if count == 2:
        one = jax.random.randint(rng, (), max(1, total - most), min(most, total - 1) + 1)
        return jnp.stack([one, total - one])
    sizes = jnp.asarray(length_profile(count, total, most, slope), jnp.int32)
    pairs = (count - 1) // 2
    source_of, sink = sizes[1:1 + 2 * pairs:2], sizes[2:2 + 2 * pairs:2]
    room = jnp.minimum(source_of - 1, most - sink)
    passed = jax.random.randint(jax.random.fold_in(rng, 1), (pairs,), 0, 1 << 20) % (room + 1)
    sizes = sizes.at[1:1 + 2 * pairs:2].set(source_of - passed).at[2:2 + 2 * pairs:2].set(sink + passed)
    return sizes[jax.random.permutation(jax.random.fold_in(rng, 2), count)]


def gaussian(stream_key, extent, width, limit, shards=(), kind=jnp.bfloat16):
    result = width * jax.random.normal(stream_key, extent, jnp.float32)
    if shards:
        result = result * block_levels(stream_key, extent, shards, -0.22, 0.18)
    return jnp.clip(result, -limit, limit).astype(kind)


def setup_inputs(seed: int = 0) -> dict:
    key_of = jax.random.split(jax.random.key(seed), 12)
    hidden_in = gaussian(key_of[0], (TOKENS, D), 1.0, 6.0, ((0, 16),))
    segment_ids = jax.vmap(lambda own: jnp.searchsorted(jnp.cumsum(ragged(own, SEQS, GROUP, MAXLEN, 2)), jnp.arange(GROUP), side="right"))(jax.random.split(key_of[1], GROUPS)).reshape((GROUPS, GROUP)).astype(jnp.int32)
    attn_gain = jnp.clip(1.0 + 0.15 * jax.random.normal(key_of[2], (D,), jnp.float32), 0.25, 1.75).astype(jnp.bfloat16)
    qkv_weight = gaussian(key_of[3], (D, QKV), D ** -0.5, 0.15625, ((0, 16), (1, 2)))
    qkv_bias = gaussian(key_of[4], (HEADS_ALL, HD), 0.5, 3.0, ((0, 2), (1, 16)))
    out_weight = gaussian(key_of[5], (HQ, D), (HQ // 16) ** -0.5, 0.625, ((0, 2), (1, 16)))
    ffn_gain = jnp.clip(1.0 + 0.15 * jax.random.normal(key_of[6], (D,), jnp.float32), 0.25, 1.75).astype(jnp.bfloat16)
    gate_weight = gaussian(key_of[7], (D, FF), D ** -0.5, 0.15625, ((0, 16), (1, 2)))
    up_weight = gaussian(key_of[8], (D, FF), D ** -0.5, 0.15625, ((0, 16), (1, 2)))
    down_weight = gaussian(key_of[9], (FF, D), FF ** -0.5, 0.0625, ((0, 2), (1, 16)))
    out_cotangent = gaussian(key_of[10], (TOKENS, D), 1.0, 6.0, ((0, 16),))
    return dict(hidden_in=hidden_in, segment_ids=segment_ids, attn_gain=attn_gain, qkv_weight=qkv_weight, qkv_bias=qkv_bias, out_weight=out_weight, ffn_gain=ffn_gain, gate_weight=gate_weight, up_weight=up_weight, down_weight=down_weight, out_cotangent=out_cotangent)


EPSILON = 1e-06
THETA = 1000000.0

def contract_last(left, right):
    return lax.dot_general(left, right, (((1,), (1,)), ((), ())), preferred_element_type=jnp.float32)

def contract_first(left, right):
    return lax.dot_general(left, right, (((0,), (0,)), ((), ())), preferred_element_type=jnp.float32)

def norm_forward(values, gain):
    factor = lax.rsqrt(lax.optimization_barrier(jnp.mean(values * values, axis=1, keepdims=True)) + EPSILON)
    unit = values * factor
    return ((unit * gain.astype(jnp.float32)).astype(jnp.bfloat16), unit, factor)

def norm_backward(grad_out, unit, factor, gain):
    gain_grad = lax.optimization_barrier(jnp.sum(grad_out * unit, axis=0))
    scaled = grad_out * gain.astype(jnp.float32)
    return (gain_grad, factor * (scaled - unit * lax.optimization_barrier(jnp.mean(scaled * unit, axis=1, keepdims=True))))

def rotary_tables(positions, head_dim):
    half = head_dim // 2
    freqs = THETA ** (-(2.0 * jnp.arange(half, dtype=jnp.float32)) / head_dim)
    angles = positions.astype(jnp.float32)[:, None] * freqs[None, :]
    return (jnp.cos(angles), jnp.sin(angles))

def rotate_pairs(values, cosine, sine):
    half = values.shape[-1] // 2
    first = values[..., :half]
    second = values[..., half:]
    cos_b = cosine[:, None, :]
    sin_b = sine[:, None, :]
    return jnp.concatenate([first * cos_b - second * sin_b, second * cos_b + first * sin_b], axis=-1)

def unrotate_pairs(grads, cosine, sine):
    half = grads.shape[-1] // 2
    first = grads[..., :half]
    second = grads[..., half:]
    cos_b = cosine[:, None, :]
    sin_b = sine[:, None, :]
    return jnp.concatenate([first * cos_b + second * sin_b, second * cos_b - first * sin_b], axis=-1)

def head_forward(query, keys, values, allowed, scale):
    scores = jnp.where(allowed, contract_last(query, keys) * scale, -1e+30)
    peak = lax.optimization_barrier(jnp.max(scores, axis=1, keepdims=True))
    total = lax.optimization_barrier(jnp.sum(jnp.exp(scores - peak), axis=1, keepdims=True))
    lse = peak + jnp.log(total)
    probs = jnp.exp(scores - lse).astype(jnp.bfloat16)
    out = jnp.dot(probs, values, preferred_element_type=jnp.float32).astype(jnp.bfloat16)
    return (out, lse[:, 0])

def head_backward(query, keys, values, allowed, scale, out, lse, grad):
    scores = jnp.where(allowed, contract_last(query, keys) * scale, -1e+30)
    probs = jnp.exp(scores - lse[:, None])
    dprob = contract_last(grad, values)
    delta = lax.optimization_barrier(jnp.sum(grad.astype(jnp.float32) * out.astype(jnp.float32), axis=1, keepdims=True))
    dscore = (probs * (dprob - delta)).astype(jnp.bfloat16)
    dquery = jnp.dot(dscore, keys, preferred_element_type=jnp.float32) * scale
    dkeys = contract_first(dscore, query) * scale
    dvalues = contract_first(probs.astype(jnp.bfloat16), grad)
    return (dquery, dkeys, dvalues)

def group_attention(queries, keys, values, allowed, scale):

    def one_kv(items):
        group_q, key_one, value_one = items
        return lax.map(lambda query: head_forward(query, key_one, value_one, allowed, scale), group_q)
    return lax.map(one_kv, (queries, keys, values))

def group_attention_back(queries, keys, values, allowed, scale, outs, lses, grads):

    def one_kv(items):
        group_q, key_one, value_one, out_g, lse_g, grad_g = items
        dquery, dkeys, dvalues = lax.map(lambda inner: head_backward(inner[0], key_one, value_one, allowed, scale, inner[1], inner[2], inner[3]), (group_q, out_g, lse_g, grad_g))
        return (dquery, lax.optimization_barrier(jnp.sum(dkeys, axis=0)), lax.optimization_barrier(jnp.sum(dvalues, axis=0)))
    return lax.map(one_kv, (queries, keys, values, outs, lses, grads))

def group_pass(weights, hidden, segments, cotangent):
    attn_gain, qkv_weight, qkv_bias, out_weight, ffn_gain, gate_weight, up_weight, down_weight = weights
    rows = hidden.shape[0]
    parts = N_TENSOR
    local_heads = H // parts
    local_kv = KVH // parts
    repeat = H // KVH
    per_part = (local_heads + 2 * local_kv) * HD
    scale = HD ** (-0.5)
    index = jnp.arange(rows, dtype=jnp.int32)
    earlier = lax.optimization_barrier(jnp.sum((segments[None, :] < segments[:, None]).astype(jnp.int32), axis=1))
    positions = index - earlier
    allowed = (segments[:, None] == segments[None, :]) & (index[:, None] >= index[None, :])
    cosine, sine = rotary_tables(positions, HD)
    hidden_f = hidden.astype(jnp.float32)
    normed1, unit1, factor1 = norm_forward(hidden_f, attn_gain)
    projected = jnp.dot(normed1, qkv_weight, preferred_element_type=jnp.float32) + qkv_bias.reshape(-1).astype(jnp.float32)
    projected = projected.reshape(rows, parts, per_part)
    query_f = projected[:, :, :local_heads * HD].reshape(rows, H, HD)
    keys_f = projected[:, :, local_heads * HD:(local_heads + local_kv) * HD].reshape(rows, KVH, HD)
    values_b = projected[:, :, (local_heads + local_kv) * HD:].reshape(rows, KVH, HD).astype(jnp.bfloat16)
    query_b = rotate_pairs(query_f, cosine, sine).astype(jnp.bfloat16)
    keys_b = rotate_pairs(keys_f, cosine, sine).astype(jnp.bfloat16)
    query_g = jnp.transpose(query_b.reshape(rows, KVH, repeat, HD), (1, 2, 0, 3))
    keys_g = jnp.transpose(keys_b, (1, 0, 2))
    values_g = jnp.transpose(values_b, (1, 0, 2))
    outs, lses = group_attention(query_g, keys_g, values_g, allowed, scale)
    attn = jnp.transpose(outs, (2, 0, 1, 3)).reshape(rows, H * HD)
    resid1 = hidden_f + jnp.dot(attn, out_weight, preferred_element_type=jnp.float32)
    normed2, unit2, factor2 = norm_forward(resid1, ffn_gain)
    gate = jnp.dot(normed2, gate_weight, preferred_element_type=jnp.float32)
    up_val = jnp.dot(normed2, up_weight, preferred_element_type=jnp.float32)
    sigma = jax.nn.sigmoid(gate)
    silu_val = gate * sigma
    act = (silu_val * up_val).astype(jnp.bfloat16)
    block = (resid1 + jnp.dot(act, down_weight, preferred_element_type=jnp.float32)).astype(jnp.bfloat16)
    grad_down = contract_first(act, cotangent)
    d_act = contract_last(cotangent, down_weight)
    d_gate = (d_act * up_val * sigma * (1.0 + gate * (1.0 - sigma))).astype(jnp.bfloat16)
    d_up = (d_act * silu_val).astype(jnp.bfloat16)
    grad_gate = contract_first(normed2, d_gate)
    grad_up = contract_first(normed2, d_up)
    d_normed2 = contract_last(d_gate, gate_weight) + contract_last(d_up, up_weight)
    grad_g2, d_back2 = norm_backward(d_normed2, unit2, factor2, ffn_gain)
    d_resid1 = cotangent.astype(jnp.float32) + d_back2
    d_resid1b = d_resid1.astype(jnp.bfloat16)
    grad_out = contract_first(attn, d_resid1b)
    d_attn = contract_last(d_resid1b, out_weight).astype(jnp.bfloat16)
    d_attn_g = jnp.transpose(d_attn.reshape(rows, KVH, repeat, HD), (1, 2, 0, 3))
    dquery, dkeys, dvalues = group_attention_back(query_g, keys_g, values_g, allowed, scale, outs, lses, d_attn_g)
    dquery = unrotate_pairs(jnp.transpose(dquery, (2, 0, 1, 3)).reshape(rows, H, HD), cosine, sine)
    dkeys = unrotate_pairs(jnp.transpose(dkeys, (1, 0, 2)), cosine, sine)
    dvalues = jnp.transpose(dvalues, (1, 0, 2))
    d_proj = jnp.concatenate([dquery.reshape(rows, parts, local_heads * HD), dkeys.reshape(rows, parts, local_kv * HD), dvalues.reshape(rows, parts, local_kv * HD)], axis=2).reshape(rows, QKV)
    grad_bias = lax.optimization_barrier(jnp.sum(d_proj, axis=0)).reshape(HEADS_ALL, HD)
    d_projb = d_proj.astype(jnp.bfloat16)
    grad_qkv = contract_first(normed1, d_projb)
    d_normed1 = contract_last(d_projb, qkv_weight)
    grad_g1, d_back1 = norm_backward(d_normed1, unit1, factor1, attn_gain)
    input_g = d_resid1 + d_back1
    return (block, input_g, (grad_g1, grad_qkv, grad_bias, grad_out, grad_g2, grad_gate, grad_up, grad_down))

def reference(hidden_in, segment_ids, attn_gain, qkv_weight, qkv_bias, out_weight, ffn_gain, gate_weight, up_weight, down_weight, out_cotangent):
    weights = (attn_gain, qkv_weight, qkv_bias, out_weight, ffn_gain, gate_weight, up_weight, down_weight)
    zeros = tuple((jnp.zeros(w.shape, jnp.float32) for w in weights))

    def step(carry, items):
        hidden, segments, cotangent = items
        block, input_g, grads = group_pass(weights, hidden, segments, cotangent)
        return (tuple((c + g for c, g in zip(carry, grads))), (block, input_g))
    totals, (blocks, input_gs) = lax.scan(step, zeros, (hidden_in.reshape(GROUPS, GROUP, D), segment_ids, out_cotangent.reshape(GROUPS, GROUP, D)))
    return (blocks.reshape(TOKENS, D), input_gs.reshape(TOKENS, D), totals[0], totals[1], totals[2], totals[3], totals[4], totals[5], totals[6], totals[7])
```

```python
import functools

import jax
import jax.numpy as jnp
from jax import lax
from jax.experimental import pallas as pl
from jax.experimental.pallas import tpu as pltpu
from jax.sharding import PartitionSpec as P

H = 12
KVH = 2
HD = 128
LANES = 128
SUBLANES = 16
BF16 = jnp.bfloat16
F32 = jnp.float32

EPSILON = 1e-06
THETA = 1000000.0

OWNERS = ("shard", "context")
TEAM = ("context", "tensor")
MESH = pl.DeviceIdType.MESH
VMEM_BYTES = 62 * 1024 * 1024


def dot(left, right):
    return jnp.dot(left, right, preferred_element_type=F32)


def contract_last(left, right):
    return lax.dot_general(left, right, (((1,), (1,)), ((), ())), preferred_element_type=F32)


def contract_first(left, right):
    return lax.dot_general(left, right, (((0,), (0,)), ((), ())), preferred_element_type=F32)


def batched(left, right, left_dim, right_dim):
    return lax.dot_general(
        left, right, (((left_dim,), (right_dim,)), ((0,), (0,))), preferred_element_type=F32
    )


def norm_forward(values, gain):
    factor = lax.rsqrt(jnp.mean(values * values, axis=1, keepdims=True) + EPSILON)
    unit = values * factor
    return ((unit * gain).astype(BF16), unit, factor)


def norm_backward(grad_out, unit, factor, gain):
    gain_grad = jnp.sum(grad_out * unit, axis=0)
    scaled = grad_out * gain
    return (gain_grad, factor * (scaled - unit * jnp.mean(scaled * unit, axis=1, keepdims=True)))


def rotary_tables(positions):
    half = HD // 2
    freqs = THETA ** (-(2.0 * jnp.arange(half, dtype=F32)) / HD)
    angles = positions.astype(F32)[:, None] * freqs[None, :]
    cosine, sine = jnp.cos(angles), jnp.sin(angles)
    return (
        jnp.concatenate([cosine, cosine], axis=1),
        jnp.concatenate([-sine, sine], axis=1),
    )


def swap_halves(values):
    half = values.shape[-1] // 2
    return jnp.concatenate([values[..., half:], values[..., :half]], axis=-1)


def rotate(values, cosine, sine):
    return values * cosine + swap_halves(values) * sine


def unrotate(values, cosine, sine):
    return values * cosine - swap_halves(values) * sine


class Place:
    def __init__(self, ns, nz):
        self.ns, self.nz, self.no = ns, nz, ns // 2
        self.s, self.z, self.y = (lax.axis_index(a) for a in ("shard", "context", "tensor"))
        self.core = lax.rem(self.s, 2)
        self.outer = lax.div(self.s, 2)
        self.mate = self.s + 1 - 2 * self.core
        self.twin = 1 - self.y

    def z_to(self, d):
        return lax.rem(self.z + d, self.nz)

    def z_from(self, d):
        return lax.rem(self.z - d + self.nz, self.nz)

    def s_to(self, o):
        return lax.rem(self.outer + o, self.no) * 2 + self.core

    def s_from(self, o):
        return lax.rem(self.outer - o + self.no, self.no) * 2 + self.core

    def mate_from(self, o):
        return lax.rem(self.outer - o + self.no, self.no) * 2 + 1 - self.core

    def greet(self):
        barrier = pltpu.get_barrier_semaphore()
        peers = [{"context": self.z_to(d)} for d in range(1, self.nz)]
        peers += [{"shard": self.s_to(o)} for o in range(1, self.no)]
        peers += [{"shard": self.mate}, {"tensor": self.twin}]
        for peer in peers:
            pl.semaphore_signal(barrier, inc=1, device_id=peer, device_id_type=MESH)
        pl.semaphore_wait(barrier, len(peers))


class Sends:
    def __init__(self):
        self.remote, self.local = [], []

    def go(self, src, dst, send, recv, **peer):
        copy = pltpu.make_async_remote_copy(
            src_ref=src, dst_ref=dst, send_sem=send, recv_sem=recv,
            device_id=peer, device_id_type=MESH,
        )
        copy.start()
        self.remote.append(copy)

    def here(self, src, dst, sem):
        copy = pltpu.make_async_copy(src, dst, sem)
        copy.start()
        self.local.append(copy)

    def drain(self):
        for copy in self.remote:
            copy.wait_send()
        for copy in self.local:
            copy.wait()
        self.remote, self.local = [], []


def landed(ref, send, recv, **peer):
    pltpu.make_async_remote_copy(
        src_ref=ref, dst_ref=ref, send_sem=send, recv_sem=recv,
        device_id=peer, device_id_type=MESH,
    ).wait_recv()


class Spread:
    def __init__(self, at, sends, src, dst, sems):
        self.at, self.sends, self.src, self.dst = at, sends, src, dst
        self.copy = None
        self.own, self.zs, self.zr, self.xs, self.xr, self.cs, self.cr = sems

    @staticmethod
    def sems(ns, nz):
        dma, no = pltpu.SemaphoreType.DMA, ns // 2
        return [
            dma, dma((nz,)), dma((nz,)), dma((nz, no)), dma((nz, no)), dma((no, nz)), dma((no, nz)),
        ]

    def over_z(self):
        at = self.at
        for d in range(1, at.nz):
            z2 = at.z_to(d)
            self.sends.go(self.src(z2), self.dst(at.s, at.z), self.zs.at[d], self.zr.at[d], context=z2)

    def over_s(self, d, ref):
        at = self.at
        for o in range(1, at.no):
            self.sends.go(
                ref, self.dst(at.s, at.z_from(d)), self.xs.at[d, o], self.xr.at[d, o],
                shard=at.s_to(o),
            )
        self.sends.go(
            ref, self.dst(at.s, at.z_from(d)), self.cs.at[0, d], self.cr.at[0, d], shard=at.mate
        )

    def own_block(self):
        at = self.at
        self.over_s(0, self.src(at.z))
        self.copy = pltpu.make_async_copy(self.src(at.z), self.dst(at.s, at.z), self.own)
        self.copy.start()

    def pass_z(self, d):
        at = self.at
        ref = self.dst(at.s, at.z_from(d))
        landed(ref, self.zs.at[d], self.zr.at[d], context=at.z_from(d))
        self.over_s(d, ref)

    def pass_s(self, o, d):
        at = self.at
        s1 = at.s_from(o)
        ref = self.dst(s1, at.z_from(d))
        landed(ref, self.xs.at[d, o], self.xr.at[d, o], shard=s1)
        self.sends.go(ref, ref, self.cs.at[o, d], self.cr.at[o, d], shard=at.mate)

    def finish(self):
        at = self.at
        self.copy.wait()
        for o in range(at.no):
            for d in range(at.nz):
                ref = self.dst(at.mate_from(o), at.z_from(d))
                landed(ref, self.cs.at[o, d], self.cr.at[o, d], shard=at.mate)

    def pass_all(self):
        for d in range(1, self.at.nz):
            self.pass_z(d)
        for o in range(1, self.at.no):
            for d in range(self.at.nz):
                self.pass_s(o, d)


class Tokens:
    def __init__(self, at, sends, ref, sems):
        self.at, self.sends, self.ref = at, sends, ref
        self.zs, self.zr, self.ys, self.yr = sems

    @staticmethod
    def sems(nz):
        dma = pltpu.SemaphoreType.DMA
        return [dma((nz,)), dma((nz,)), dma((nz,)), dma((nz,))]

    def over_z(self, src):
        at = self.at
        for d in range(1, at.nz):
            self.sends.go(
                src, self.ref.at[at.z, at.y], self.zs.at[d], self.zr.at[d], context=at.z_to(d)
            )

    def over_y(self, d, src):
        at = self.at
        self.sends.go(
            src, self.ref.at[at.z_from(d), at.y], self.ys.at[d], self.yr.at[d], tensor=at.twin
        )

    def pass_z(self, d):
        at = self.at
        ref = self.ref.at[at.z_from(d), at.y]
        landed(ref, self.zs.at[d], self.zr.at[d], context=at.z_from(d))
        self.over_y(d, ref)

    def wait_y(self, d):
        at = self.at
        ref = self.ref.at[at.z_from(d), at.twin]
        landed(ref, self.ys.at[d], self.yr.at[d], tensor=at.twin)


def whole_lines(small, blocks, depth):
    tiles = []
    for t in range(blocks * depth // LANES):
        tile = jnp.zeros((8, LANES), F32)
        lane = lax.broadcasted_iota(jnp.int32, (8, LANES), 1) + t * LANES
        for b in range(t * LANES // depth, min(blocks, -(-(t + 1) * LANES // depth))):
            line = small[b, :8, :].astype(F32)
            shift = (b * depth - t * LANES) % LANES
            moved = pltpu.roll(line, shift, 1) if shift else line
            tile = jnp.where((lane >= b * depth) & (lane < (b + 1) * depth), moved, tile)
        tiles.append(tile)
    return jnp.concatenate(tiles, axis=1)


def front_kernel(ns, nz, heads, kv, *refs):
    ins, outs, (small, ypart, yland, *sems) = refs[:10], refs[10:22], refs[22:]
    (wa_in, small_in, gate_in, up_in, down_in, hidden, cot_in, cosine, sine, mask) = ins
    (wa, gate_w, up_w, down_w, lines, n2, cot, resid, query, kv_all, probs, attn) = outs
    n_spread = len(Spread.sems(ns, nz))
    n_tokens = len(Tokens.sems(nz))
    at, sends = Place(ns, nz), Sends()
    depth = wa_in.shape[0]
    rows, width = hidden.shape
    half = rows // 2
    q_cols = heads * HD
    qkv_cols = q_cols + 2 * kv * HD

    def spread(i, src, dst):
        return Spread(at, sends, src, dst, sems[i * n_spread:(i + 1) * n_spread])

    def block(ref):
        return lambda s1, z1: ref.at[pl.ds(pl.multiple_of((s1 * nz + z1) * depth, SUBLANES), depth)]

    w_attn = spread(0, lambda z2: wa_in, block(wa))
    w_small = spread(1, lambda z2: small_in, lambda s1, z1: small.at[s1 * nz + z1])
    ffn = [
        spread(2 + i, lambda z2, src=src: src.at[z2], block(dst))
        for i, (src, dst) in enumerate(((gate_in, gate_w), (up_in, up_w), (down_in, down_w)))
    ]
    rest = sems[5 * n_spread:]
    t_cot = Tokens(at, sends, cot, rest[:n_tokens])
    t_n2 = Tokens(at, sends, n2, rest[n_tokens:2 * n_tokens])
    kvs, kvr, yps, ypr, cot_sem = rest[2 * n_tokens:]

    at.greet()
    w_small.over_z()
    w_small.own_block()
    w_attn.over_z()
    w_attn.own_block()
    ffn[0].over_z()
    ffn[0].own_block()
    my_half = cot_in.at[pl.ds(pl.multiple_of(at.y * half, SUBLANES), half)]
    sends.here(cot_in.at[pl.ds(0, half)], cot.at[at.z, 0], cot_sem.at[0])
    sends.here(cot_in.at[pl.ds(half, half)], cot.at[at.z, 1], cot_sem.at[1])

    hidden_f = hidden[...].astype(F32)
    factor1 = lax.rsqrt(jnp.mean(hidden_f * hidden_f, axis=1, keepdims=True) + EPSILON)
    w_small.pass_all()
    w_attn.pass_all()
    w_small.finish()
    gains = whole_lines(small, ns * nz, depth)
    lines[...] = gains
    normed1 = (hidden[...].astype(F32) * factor1 * gains[0:1, :]).astype(BF16)
    w_attn.finish()

    width_each = HD // (ns * nz)
    lane = lax.broadcasted_iota(jnp.int32, (8, LANES), 1)
    bias = jnp.zeros((8, LANES), F32)
    for b in range(ns * nz):
        line = small[b, 8:16, :].astype(F32)
        moved = pltpu.roll(line, b * width_each, 1) if b else line
        bias = jnp.where((lane >= b * width_each) & (lane < (b + 1) * width_each), moved, bias)
    cos_t, sin_t = cosine[...], sine[...]

    def projected(head):
        part = jnp.dot(
            normed1, wa[:, head * HD:(head + 1) * HD], preferred_element_type=F32
        )
        return part + bias[head:head + 1, :]

    def rotated(values):
        return values * cos_t + pltpu.roll(values, HD // 2, 1) * sin_t

    for j in range(kv):
        kv_all[at.z, :, j * HD:(j + 1) * HD] = rotated(projected(heads + j)).astype(BF16)
        kv_all[at.z, :, (kv + j) * HD:(kv + j + 1) * HD] = projected(heads + kv + j).astype(BF16)
    for d in range(1, nz):
        sends.go(kv_all.at[at.z], kv_all.at[at.z], kvs.at[d], kvr.at[d], context=at.z_to(d))
    ffn[1].over_z()
    ffn[1].own_block()
    t_cot.over_z(my_half)
    ffn[0].pass_all()
    for h in range(heads):
        query[:, h * HD:(h + 1) * HD] = rotated(projected(h)).astype(BF16)
    for d in range(1, nz):
        src = kv_all.at[at.z_from(d)]
        landed(src, kvs.at[d], kvr.at[d], context=at.z_from(d))

    scale = HD ** (-0.5)
    group_rows = nz * rows
    keep = mask[...] > 0
    repeat = heads // kv
    for h in range(heads):
        j = h // repeat
        keys = kv_all[:, :, j * HD:(j + 1) * HD].reshape(group_rows, HD)
        values = kv_all[:, :, (kv + j) * HD:(kv + j + 1) * HD].reshape(group_rows, HD)
        scores = lax.dot_general(
            query[:, h * HD:(h + 1) * HD], keys, (((1,), (1,)), ((), ())),
            preferred_element_type=F32,
        )
        scores = jnp.where(keep, scores * scale, -1e30)
        peak = jnp.max(scores, axis=1, keepdims=True)
        lse = peak + jnp.log(jnp.sum(jnp.exp(scores - peak), axis=1, keepdims=True))
        p = jnp.exp(scores - lse)
        probs[h * rows:(h + 1) * rows, :] = p
        out = jnp.dot(p.astype(BF16), values, preferred_element_type=F32)
        attn[:, h * HD:(h + 1) * HD] = out.astype(BF16)
    part = lax.dot_general(
        attn[...], wa[:, qkv_cols:qkv_cols + q_cols], (((1,), (1,)), ((), ())),
        preferred_element_type=F32,
    ).astype(BF16)
    ypart[0] = part[:half]
    ypart[1] = part[half:]
    sends.go(ypart.at[at.twin], yland, yps, ypr, tensor=at.twin)
    ffn[2].over_z()
    ffn[2].own_block()
    for d in range(1, nz):
        t_cot.pass_z(d)
    ffn[1].pass_all()

    landed(yland, yps, ypr, tensor=at.twin)
    base = pl.multiple_of(at.y * half, SUBLANES)
    total = ypart[at.y].astype(F32) + yland[...].astype(F32)
    res = hidden[pl.ds(base, half), :].astype(F32) + total
    resid[...] = res
    factor2 = lax.rsqrt(jnp.mean(res * res, axis=1, keepdims=True) + EPSILON)
    n2[at.z, at.y] = (res * factor2 * gains[1:2, :]).astype(BF16)
    t_n2.over_z(n2.at[at.z, at.y])
    t_n2.over_y(0, n2.at[at.z, at.y])
    for d in range(1, nz):
        t_n2.pass_z(d)
    ffn[2].pass_all()
    for d in range(nz):
        t_n2.wait_y(d)
    for d in range(1, nz):
        t_cot.wait_y(d)
    for item in ffn:
        item.finish()
    sends.drain()


def front(ns, nz, heads, kv, wa_in, small_in, ffn_in, hidden, cot, cosine, sine, mask):
    rows, width = hidden.shape
    owners = ns * nz
    half = rows // 2
    unit = ffn_in[0].shape[2]
    wide = owners * wa_in.shape[0]
    dma = pltpu.SemaphoreType.DMA
    shape = jax.ShapeDtypeStruct
    vmem = pl.BlockSpec(memory_space=pltpu.VMEM)
    anyspace = pl.BlockSpec(memory_space=pl.ANY)
    return pl.pallas_call(
        functools.partial(front_kernel, ns, nz, heads, kv),
        out_shape=[
            shape((wide, wa_in.shape[1]), BF16),
            *[shape((wide, unit), BF16)] * 3,
            shape((8, wide), F32),
            shape((nz, 2, half, width), BF16),
            shape((nz, 2, half, width), BF16),
            shape((half, width), F32),
            shape((rows, heads * HD), BF16),
            shape((nz, rows, 2 * kv * HD), BF16),
            shape((heads * rows, nz * rows), F32),
            shape((rows, heads * HD), BF16),
        ],
        in_specs=[anyspace] * 5 + [vmem, anyspace] + [vmem] * 3,
        out_specs=[vmem] + [anyspace] * 3 + [vmem] * 8,
        scratch_shapes=[
            pltpu.VMEM((owners, 16, LANES), BF16),
            pltpu.VMEM((2, half, width), BF16),
            pltpu.VMEM((half, width), BF16),
        ]
        + Spread.sems(ns, nz) * 5
        + Tokens.sems(nz) * 2
        + [dma((nz,)), dma((nz,)), dma, dma, dma((2,))],
        compiler_params=pltpu.CompilerParams(
            collective_id=0, has_side_effects=True, vmem_limit_bytes=VMEM_BYTES
        ),
    )(wa_in, small_in, *ffn_in, hidden, cot, cosine, sine, mask)


def fast_step(
    ns,
    nz,
    hidden_in,
    segment_ids,
    attn_gain,
    qkv_weight,
    qkv_bias,
    out_weight,
    ffn_gain,
    gate_weight,
    up_weight,
    down_weight,
    out_cotangent,
):
    rows, width = hidden_in.shape
    depth, hidden_units = gate_weight.shape
    parts = 2
    heads = H // parts
    kv = KVH // parts
    repeat = heads // kv
    scale = HD ** (-0.5)
    block_index = lax.axis_index("context")
    part_index = lax.axis_index("tensor")
    half_rows = rows // parts
    unit_cols = -(-hidden_units // (nz * LANES)) * LANES
    padded = unit_cols * nz
    q_cols = heads * HD
    k_cols = kv * HD

    def by_place(weight):
        full = jnp.pad(weight, ((0, 0), (0, padded - hidden_units)))
        return jnp.transpose(full.reshape(depth, nz, unit_cols), (1, 0, 2))

    ffn_in = [by_place(w) for w in (gate_weight, up_weight, down_weight.T)]
    wa_in = jnp.concatenate([qkv_weight, out_weight.T], axis=1)
    gains_in = jnp.pad(jnp.stack([attn_gain, ffn_gain]), ((0, 6), (0, LANES - depth)))
    bias_in = jnp.pad(qkv_bias, ((0, 0), (0, LANES - qkv_bias.shape[1])))
    small_in = jnp.concatenate([gains_in, bias_in], axis=0)

    seg_all = segment_ids[0]
    group_rows = seg_all.shape[0]
    first_row = block_index * rows
    index_all = jnp.arange(group_rows, dtype=jnp.int32)
    seg_local = lax.dynamic_slice_in_dim(seg_all, first_row, rows)
    index_local = first_row + jnp.arange(rows, dtype=jnp.int32)
    earlier = jnp.sum((seg_all[None, :] < seg_local[:, None]).astype(jnp.int32), axis=1)
    allowed = (seg_local[:, None] == seg_all[None, :]) & (
        index_local[:, None] >= index_all[None, :]
    )
    cosine, sine = rotary_tables(index_local - earlier)

    wa, gate_full, up_full, down_full, lines, n2, cot, resid_half, query, kv_all, p_soft, attn = front(
        ns, nz, heads, kv, wa_in, small_in, ffn_in, hidden_in, out_cotangent, cosine, sine,
        allowed.astype(F32),
    )
    gain_one, gain_two = lines[0], lines[1]
    qkv_full = wa[:, : q_cols + 2 * k_cols]
    out_full = wa[:, q_cols + 2 * k_cols :]
    normed2 = n2.reshape(group_rows, width)
    cot = cot.reshape(group_rows, width)
    hidden_f = hidden_in.astype(F32)
    normed1, unit1, factor1 = norm_forward(hidden_f, gain_one)
    _, unit2, factor2 = norm_forward(resid_half, gain_two)
    query = jnp.transpose(query.reshape(rows, heads, HD), (1, 0, 2)).reshape(kv, repeat * rows, HD)
    kv_rows = kv_all.reshape(group_rows, 2 * kv, HD)
    keys = jnp.transpose(kv_rows[:, :kv], (1, 0, 2))
    values = jnp.transpose(kv_rows[:, kv:], (1, 0, 2))
    p_soft = p_soft.reshape(kv, repeat * rows, group_rows)
    probs = p_soft.astype(BF16)
    outs = jnp.transpose(attn.reshape(rows, heads, HD), (1, 0, 2)).reshape(kv, repeat * rows, HD)
    mine = part_index * half_rows
    cot_half = lax.dynamic_slice_in_dim(out_cotangent, mine, half_rows)
    blocks = nz
    gate = dot(normed2, gate_full)
    up_val = dot(normed2, up_full)
    sigma = jax.nn.sigmoid(gate)
    silu_val = gate * sigma
    act = (silu_val * up_val).astype(BF16)
    ffn_part = contract_last(act, down_full).astype(BF16)
    d_act = dot(cot, down_full)
    d_gate = (d_act * up_val * sigma * (1.0 + gate * (1.0 - sigma))).astype(BF16)
    d_up = (d_act * silu_val).astype(BF16)
    dn2_part = (contract_last(d_gate, gate_full) + contract_last(d_up, up_full)).astype(BF16)
    ffn_half = lax.psum_scatter(ffn_part, TEAM, scatter_dimension=0, tiled=True)
    block_half = (resid_half + ffn_half.astype(F32)).astype(BF16)
    block_out = lax.all_gather(block_half, "tensor", axis=0, tiled=True)
    dn2_half = lax.psum_scatter(dn2_part, TEAM, scatter_dimension=0, tiled=True).astype(F32)
    grad_g2, d_back2 = norm_backward(dn2_half, unit2, factor2, gain_two)
    d_resid_half = cot_half.astype(F32) + d_back2

    def give_back(grad):
        part = lax.psum_scatter(grad.astype(BF16), "shard", scatter_dimension=0, tiled=True)
        part = part.reshape(blocks, depth, unit_cols)
        part = lax.all_to_all(part, "context", split_axis=0, concat_axis=2, tiled=True)
        return part.reshape(depth, padded)[:, :hidden_units].astype(F32)

    sum_gate = give_back(contract_first(normed2, d_gate))
    sum_up = give_back(contract_first(normed2, d_up))
    sum_down = give_back(contract_first(cot, act)).T

    d_resid_b = lax.all_gather(d_resid_half.astype(BF16), "tensor", axis=0, tiled=True)
    grad_out = contract_first(d_resid_b, attn)
    d_attn = dot(d_resid_b, out_full).astype(BF16)
    d_outs = jnp.transpose(d_attn.reshape(rows, heads, HD), (1, 0, 2)).reshape(
        kv, repeat * rows, HD
    )
    d_prob = batched(d_outs, values, 2, 2)
    delta = jnp.sum(d_outs.astype(F32) * outs.astype(F32), axis=2, keepdims=True)
    d_score = (p_soft * (d_prob - delta)).astype(BF16)
    d_query = batched(d_score, keys, 2, 1) * scale
    d_keys = batched(d_score, query, 1, 1) * scale
    d_values = batched(probs, d_outs, 1, 1)
    d_kv = jnp.concatenate([d_keys, d_values], axis=0).astype(BF16)
    d_kv = lax.psum_scatter(d_kv, "context", scatter_dimension=1, tiled=True).astype(F32)
    d_query = unrotate(d_query.reshape(heads, rows, HD), cosine, sine)
    d_keys = unrotate(d_kv[:kv], cosine, sine)
    d_proj = jnp.transpose(jnp.concatenate([d_query, d_keys, d_kv[kv:]], axis=0), (1, 0, 2))
    grad_bias = jnp.sum(d_proj, axis=0)
    d_projb = d_proj.reshape(rows, -1).astype(BF16)
    grad_qkv = contract_first(normed1, d_projb)
    dn1_part = contract_last(d_projb, qkv_full).astype(BF16)
    dn1_half = lax.psum_scatter(dn1_part, "tensor", scatter_dimension=0, tiled=True).astype(F32)
    unit1_half = lax.dynamic_slice_in_dim(unit1, mine, half_rows)
    factor1_half = lax.dynamic_slice_in_dim(factor1, mine, half_rows)
    grad_g1, d_back1 = norm_backward(dn1_half, unit1_half, factor1_half, gain_one)
    input_grad = lax.all_gather(d_resid_half + d_back1, "tensor", axis=0, tiled=True)

    gains = lax.psum(jnp.stack([grad_g1, grad_g2]), "tensor")
    sum_gains = lax.psum_scatter(gains, OWNERS, scatter_dimension=1, tiled=True)
    sum_qkv = lax.psum_scatter(grad_qkv.astype(BF16), OWNERS, scatter_dimension=0, tiled=True)
    sum_bias = lax.psum_scatter(grad_bias, OWNERS, scatter_dimension=1, tiled=True)
    sum_out = lax.psum_scatter(grad_out.astype(BF16), OWNERS, scatter_dimension=0, tiled=True)
    return (
        block_out,
        input_grad,
        sum_gains[0],
        sum_qkv.astype(F32),
        sum_bias,
        sum_out.astype(F32).T,
        sum_gains[1],
        sum_gate,
        sum_up,
        sum_down,
    )


def general_step(
    hidden_in,
    segment_ids,
    attn_gain,
    qkv_weight,
    qkv_bias,
    out_weight,
    ffn_gain,
    gate_weight,
    up_weight,
    down_weight,
    out_cotangent,
):
    rows, width = hidden_in.shape
    depth = gate_weight.shape[0]
    hidden_units = gate_weight.shape[1]
    parts = lax.axis_size("tensor")
    blocks = lax.axis_size("context")
    heads = H // parts
    kv = KVH // parts
    repeat = H // KVH
    scale = HD ** (-0.5)
    block_index = lax.axis_index("context")
    part_index = lax.axis_index("tensor")
    half_rows = rows // parts
    unit_cols = -(-hidden_units // (blocks * LANES)) * LANES
    padded = unit_cols * blocks

    def spread(weight):
        full = jnp.pad(weight, ((0, 0), (0, padded - hidden_units)))
        mine = lax.all_to_all(full, "context", split_axis=1, concat_axis=0, tiled=True)
        mine = mine.reshape(blocks * depth, unit_cols)
        return lax.all_gather(mine, "shard", axis=0, tiled=True)

    gate_full = spread(gate_weight)
    up_full = spread(up_weight)
    down_full = spread(down_weight.T)
    gain_one = lax.all_gather(attn_gain, OWNERS, axis=0, tiled=True).astype(F32)
    gain_two = lax.all_gather(ffn_gain, OWNERS, axis=0, tiled=True).astype(F32)
    bias = lax.all_gather(qkv_bias, OWNERS, axis=1, tiled=True).reshape(-1).astype(F32)
    qkv_full = lax.all_gather(qkv_weight, OWNERS, axis=0, tiled=True)
    out_full = lax.all_gather(out_weight.T, OWNERS, axis=0, tiled=True)

    seg_all = segment_ids[0]
    group_rows = seg_all.shape[0]
    first_row = block_index * rows
    index_all = jnp.arange(group_rows, dtype=jnp.int32)
    earlier = jnp.sum((seg_all[None, :] < seg_all[:, None]).astype(jnp.int32), axis=1)
    positions = index_all - earlier
    seg_local = lax.dynamic_slice_in_dim(seg_all, first_row, rows)
    index_local = first_row + jnp.arange(rows, dtype=jnp.int32)
    allowed = (seg_local[:, None] == seg_all[None, :]) & (
        index_local[:, None] >= index_all[None, :]
    )
    cosine, sine = rotary_tables(positions)
    cos_local = lax.dynamic_slice_in_dim(cosine, first_row, rows)
    sin_local = lax.dynamic_slice_in_dim(sine, first_row, rows)

    hidden_all = lax.all_gather(hidden_in, "context", axis=0, tiled=True)
    normed_all, _, _ = norm_forward(hidden_all.astype(F32), gain_one)
    hidden_f = hidden_in.astype(F32)
    normed1, unit1, factor1 = norm_forward(hidden_f, gain_one)
    q_cols = heads * HD
    k_cols = kv * HD
    query_f = dot(normed1, qkv_full[:, :q_cols]) + bias[:q_cols]
    kv_f = dot(normed_all, qkv_full[:, q_cols:]) + bias[q_cols:]
    query = jnp.transpose(query_f.reshape(rows, heads, HD), (1, 0, 2))
    query = rotate(query, cos_local, sin_local).astype(BF16)
    keys = jnp.transpose(kv_f[:, :k_cols].reshape(group_rows, kv, HD), (1, 0, 2))
    keys = rotate(keys, cosine, sine).astype(BF16)
    values = jnp.transpose(kv_f[:, k_cols:].reshape(group_rows, kv, HD), (1, 0, 2)).astype(BF16)
    query = query.reshape(kv, repeat * rows, HD)
    mask = jnp.tile(allowed, (repeat, 1))
    scores = jnp.where(mask, batched(query, keys, 2, 2) * scale, -1e30)
    peak = jnp.max(scores, axis=2, keepdims=True)
    lse = peak + jnp.log(jnp.sum(jnp.exp(scores - peak), axis=2, keepdims=True))
    p_soft = jnp.exp(scores - lse)
    probs = p_soft.astype(BF16)
    outs = batched(probs, values, 2, 1).astype(BF16)
    attn = jnp.transpose(outs.reshape(heads, rows, HD), (1, 0, 2)).reshape(rows, q_cols)
    attn_part = contract_last(attn, out_full).astype(BF16)

    mine = part_index * half_rows
    attn_half = lax.psum_scatter(attn_part, "tensor", scatter_dimension=0, tiled=True)
    resid_half = lax.dynamic_slice_in_dim(hidden_f, mine, half_rows) + attn_half.astype(F32)
    normed2_half, unit2, factor2 = norm_forward(resid_half, gain_two)
    normed2 = lax.all_gather(normed2_half, TEAM, axis=0, tiled=True)
    cot_half = lax.dynamic_slice_in_dim(out_cotangent, mine, half_rows)
    cot = lax.all_gather(cot_half, TEAM, axis=0, tiled=True)

    gate = dot(normed2, gate_full)
    up_val = dot(normed2, up_full)
    sigma = jax.nn.sigmoid(gate)
    silu_val = gate * sigma
    act = (silu_val * up_val).astype(BF16)
    ffn_part = contract_last(act, down_full).astype(BF16)
    d_act = dot(cot, down_full)
    d_gate = (d_act * up_val * sigma * (1.0 + gate * (1.0 - sigma))).astype(BF16)
    d_up = (d_act * silu_val).astype(BF16)
    dn2_part = (contract_last(d_gate, gate_full) + contract_last(d_up, up_full)).astype(BF16)
    ffn_half = lax.psum_scatter(ffn_part, TEAM, scatter_dimension=0, tiled=True)
    block_half = (resid_half + ffn_half.astype(F32)).astype(BF16)
    block_out = lax.all_gather(block_half, "tensor", axis=0, tiled=True)
    dn2_half = lax.psum_scatter(dn2_part, TEAM, scatter_dimension=0, tiled=True).astype(F32)
    grad_g2, d_back2 = norm_backward(dn2_half, unit2, factor2, gain_two)
    d_resid_half = cot_half.astype(F32) + d_back2

    def give_back(grad):
        part = lax.psum_scatter(grad.astype(BF16), "shard", scatter_dimension=0, tiled=True)
        part = part.reshape(blocks, depth, unit_cols)
        part = lax.all_to_all(part, "context", split_axis=0, concat_axis=2, tiled=True)
        return part.reshape(depth, padded)[:, :hidden_units].astype(F32)

    sum_gate = give_back(contract_first(normed2, d_gate))
    sum_up = give_back(contract_first(normed2, d_up))
    sum_down = give_back(contract_first(cot, act)).T

    d_resid_b = lax.all_gather(d_resid_half.astype(BF16), "tensor", axis=0, tiled=True)
    grad_out = contract_first(d_resid_b, attn)
    d_attn = dot(d_resid_b, out_full).astype(BF16)
    d_outs = jnp.transpose(d_attn.reshape(rows, heads, HD), (1, 0, 2)).reshape(
        kv, repeat * rows, HD
    )
    d_prob = batched(d_outs, values, 2, 2)
    delta = jnp.sum(d_outs.astype(F32) * outs.astype(F32), axis=2, keepdims=True)
    d_score = (p_soft * (d_prob - delta)).astype(BF16)
    d_query = batched(d_score, keys, 2, 1) * scale
    d_keys = batched(d_score, query, 1, 1) * scale
    d_values = batched(probs, d_outs, 1, 1)
    d_kv = jnp.concatenate([d_keys, d_values], axis=0).astype(BF16)
    d_kv = lax.psum_scatter(d_kv, "context", scatter_dimension=1, tiled=True).astype(F32)
    d_query = unrotate(d_query.reshape(heads, rows, HD), cos_local, sin_local)
    d_keys = unrotate(d_kv[:kv], cos_local, sin_local)
    d_proj = jnp.transpose(jnp.concatenate([d_query, d_keys, d_kv[kv:]], axis=0), (1, 0, 2))
    grad_bias = jnp.sum(d_proj, axis=0)
    d_projb = d_proj.reshape(rows, -1).astype(BF16)
    grad_qkv = contract_first(normed1, d_projb)
    dn1_part = contract_last(d_projb, qkv_full).astype(BF16)
    dn1_half = lax.psum_scatter(dn1_part, "tensor", scatter_dimension=0, tiled=True).astype(F32)
    unit1_half = lax.dynamic_slice_in_dim(unit1, mine, half_rows)
    factor1_half = lax.dynamic_slice_in_dim(factor1, mine, half_rows)
    grad_g1, d_back1 = norm_backward(dn1_half, unit1_half, factor1_half, gain_one)
    input_grad = lax.all_gather(d_resid_half + d_back1, "tensor", axis=0, tiled=True)

    gains = lax.psum(jnp.stack([grad_g1, grad_g2]), "tensor")
    sum_gains = lax.psum_scatter(gains, OWNERS, scatter_dimension=1, tiled=True)
    sum_qkv = lax.psum_scatter(grad_qkv.astype(BF16), OWNERS, scatter_dimension=0, tiled=True)
    sum_bias = lax.psum_scatter(grad_bias, OWNERS, scatter_dimension=1, tiled=True)
    sum_out = lax.psum_scatter(grad_out.astype(BF16), OWNERS, scatter_dimension=0, tiled=True)
    return (
        block_out,
        input_grad,
        sum_gains[0],
        sum_qkv.astype(F32),
        sum_bias,
        sum_out.astype(F32).T,
        sum_gains[1],
        sum_gate,
        sum_up,
        sum_down,
    )


def solution(mesh):
    ns, nz, parts = (mesh.shape[a] for a in ("shard", "context", "tensor"))
    rows = P(OWNERS, None)

    def local(*args):
        depth = args[7].shape[0]
        if depth % SUBLANES == 0 and ns % 2 == 0 and ns > 2 and nz > 1 and parts == 2:
            return fast_step(ns, nz, *args)
        return general_step(*args)

    placed = (
        rows,
        P("shard", None),
        P(OWNERS),
        P(OWNERS, "tensor"),
        P("tensor", OWNERS),
        P("tensor", OWNERS),
        P(OWNERS),
        P(OWNERS, "tensor"),
        P(OWNERS, "tensor"),
        P("tensor", OWNERS),
        rows,
    )
    return jax.shard_map(
        local,
        mesh=mesh,
        in_specs=placed,
        out_specs=(
            rows,
            rows,
            P(OWNERS),
            P(OWNERS, "tensor"),
            P("tensor", OWNERS),
            P("tensor", OWNERS),
            P(OWNERS),
            P(OWNERS, "tensor"),
            P(OWNERS, "tensor"),
            P("tensor", OWNERS),
        ),
        check_vma=False,
    )
```

```python
import functools

import jax
import jax.numpy as jnp
from jax import lax
from jax.experimental import pallas as pl
from jax.experimental.pallas import tpu as pltpu
from jax.sharding import PartitionSpec as P

H = 12
KVH = 2
HD = 128
LANES = 128
SUBLANES = 16
BF16 = jnp.bfloat16
F32 = jnp.float32

EPSILON = 1e-06
THETA = 1000000.0

OWNERS = ("shard", "context")
TEAM = ("context", "tensor")
MESH = pl.DeviceIdType.MESH
VMEM_BYTES = 62 * 1024 * 1024


def dot(left, right):
    return jnp.dot(left, right, preferred_element_type=F32)


def contract_last(left, right):
    return lax.dot_general(left, right, (((1,), (1,)), ((), ())), preferred_element_type=F32)


def contract_first(left, right):
    return lax.dot_general(left, right, (((0,), (0,)), ((), ())), preferred_element_type=F32)


def batched(left, right, left_dim, right_dim):
    return lax.dot_general(
        left, right, (((left_dim,), (right_dim,)), ((0,), (0,))), preferred_element_type=F32
    )


def norm_forward(values, gain):
    factor = lax.rsqrt(jnp.mean(values * values, axis=1, keepdims=True) + EPSILON)
    unit = values * factor
    return ((unit * gain).astype(BF16), unit, factor)


def norm_backward(grad_out, unit, factor, gain):
    gain_grad = jnp.sum(grad_out * unit, axis=0)
    scaled = grad_out * gain
    return (gain_grad, factor * (scaled - unit * jnp.mean(scaled * unit, axis=1, keepdims=True)))


def rotary_tables(positions):
    half = HD // 2
    freqs = THETA ** (-(2.0 * jnp.arange(half, dtype=F32)) / HD)
    angles = positions.astype(F32)[:, None] * freqs[None, :]
    cosine, sine = jnp.cos(angles), jnp.sin(angles)
    return (
        jnp.concatenate([cosine, cosine], axis=1),
        jnp.concatenate([-sine, sine], axis=1),
    )


def swap_halves(values):
    half = values.shape[-1] // 2
    return jnp.concatenate([values[..., half:], values[..., :half]], axis=-1)


def rotate(values, cosine, sine):
    return values * cosine + swap_halves(values) * sine


def unrotate(values, cosine, sine):
    return values * cosine - swap_halves(values) * sine


class Place:
    def __init__(self, ns, nz):
        self.ns, self.nz, self.no = ns, nz, ns // 2
        self.s, self.z, self.y = (lax.axis_index(a) for a in ("shard", "context", "tensor"))
        self.core = lax.rem(self.s, 2)
        self.outer = lax.div(self.s, 2)
        self.mate = self.s + 1 - 2 * self.core
        self.twin = 1 - self.y

    def z_to(self, d):
        return lax.rem(self.z + d, self.nz)

    def z_from(self, d):
        return lax.rem(self.z - d + self.nz, self.nz)

    def s_to(self, o):
        return lax.rem(self.outer + o, self.no) * 2 + self.core

    def s_from(self, o):
        return lax.rem(self.outer - o + self.no, self.no) * 2 + self.core

    def mate_from(self, o):
        return lax.rem(self.outer - o + self.no, self.no) * 2 + 1 - self.core

    def mate_to(self, o):
        return lax.rem(self.outer + o, self.no) * 2 + 1 - self.core

    def greet(self, everyone=False):
        barrier = pltpu.get_barrier_semaphore()
        peers = [{"context": self.z_to(d)} for d in range(1, self.nz)]
        if everyone:
            peers += [{"shard": lax.rem(self.s + k, self.ns)} for k in range(1, self.ns)]
        else:
            peers += [{"shard": self.s_to(o)} for o in range(1, self.no)] + [{"shard": self.mate}]
        peers += [{"tensor": self.twin}]
        for peer in peers:
            pl.semaphore_signal(barrier, inc=1, device_id=peer, device_id_type=MESH)
        pl.semaphore_wait(barrier, len(peers))


class Sends:
    def __init__(self):
        self.remote, self.local = [], []

    def go(self, src, dst, send, recv, **peer):
        copy = pltpu.make_async_remote_copy(
            src_ref=src, dst_ref=dst, send_sem=send, recv_sem=recv,
            device_id=peer, device_id_type=MESH,
        )
        copy.start()
        self.remote.append(copy)

    def here(self, src, dst, sem):
        copy = pltpu.make_async_copy(src, dst, sem)
        copy.start()
        self.local.append(copy)

    def drain(self):
        for copy in self.remote:
            copy.wait_send()
        for copy in self.local:
            copy.wait()
        self.remote, self.local = [], []


def landed(ref, send, recv, **peer):
    pltpu.make_async_remote_copy(
        src_ref=ref, dst_ref=ref, send_sem=send, recv_sem=recv,
        device_id=peer, device_id_type=MESH,
    ).wait_recv()


class Spread:
    def __init__(self, at, sends, src, dst, sems):
        self.at, self.sends, self.src, self.dst = at, sends, src, dst
        self.copy = None
        self.own, self.zs, self.zr, self.xs, self.xr, self.cs, self.cr = sems

    @staticmethod
    def sems(ns, nz):
        dma, no = pltpu.SemaphoreType.DMA, ns // 2
        return [
            dma, dma((nz,)), dma((nz,)), dma((nz, no)), dma((nz, no)), dma((no, nz)), dma((no, nz)),
        ]

    def over_z(self):
        at = self.at
        for d in range(1, at.nz):
            z2 = at.z_to(d)
            self.sends.go(self.src(z2), self.dst(at.s, at.z), self.zs.at[d], self.zr.at[d], context=z2)

    def over_s(self, d, ref):
        at = self.at
        for o in range(1, at.no):
            self.sends.go(
                ref, self.dst(at.s, at.z_from(d)), self.xs.at[d, o], self.xr.at[d, o],
                shard=at.s_to(o),
            )
        self.sends.go(
            ref, self.dst(at.s, at.z_from(d)), self.cs.at[0, d], self.cr.at[0, d], shard=at.mate
        )

    def own_block(self):
        at = self.at
        self.over_s(0, self.src(at.z))
        self.copy = pltpu.make_async_copy(self.src(at.z), self.dst(at.s, at.z), self.own)
        self.copy.start()

    def pass_z(self, d):
        at = self.at
        ref = self.dst(at.s, at.z_from(d))
        landed(ref, self.zs.at[d], self.zr.at[d], context=at.z_from(d))
        self.over_s(d, ref)

    def pass_s(self, o, d):
        at = self.at
        s1 = at.s_from(o)
        ref = self.dst(s1, at.z_from(d))
        landed(ref, self.xs.at[d, o], self.xr.at[d, o], shard=s1)
        self.sends.go(ref, ref, self.cs.at[o, d], self.cr.at[o, d], shard=at.mate)

    def finish(self):
        at = self.at
        self.copy.wait()
        for o in range(at.no):
            for d in range(at.nz):
                ref = self.dst(at.mate_from(o), at.z_from(d))
                landed(ref, self.cs.at[o, d], self.cr.at[o, d], shard=at.mate)

    def pass_all(self):
        for d in range(1, self.at.nz):
            self.pass_z(d)
        for o in range(1, self.at.no):
            for d in range(self.at.nz):
                self.pass_s(o, d)


class Tokens:
    def __init__(self, at, sends, ref, sems):
        self.at, self.sends, self.ref = at, sends, ref
        self.zs, self.zr, self.ys, self.yr = sems

    @staticmethod
    def sems(nz):
        dma = pltpu.SemaphoreType.DMA
        return [dma((nz,)), dma((nz,)), dma((nz,)), dma((nz,))]

    def over_z(self, src):
        at = self.at
        for d in range(1, at.nz):
            self.sends.go(
                src, self.ref.at[at.z, at.y], self.zs.at[d], self.zr.at[d], context=at.z_to(d)
            )

    def over_y(self, d, src):
        at = self.at
        self.sends.go(
            src, self.ref.at[at.z_from(d), at.y], self.ys.at[d], self.yr.at[d], tensor=at.twin
        )

    def pass_z(self, d):
        at = self.at
        ref = self.ref.at[at.z_from(d), at.y]
        landed(ref, self.zs.at[d], self.zr.at[d], context=at.z_from(d))
        self.over_y(d, ref)

    def wait_y(self, d):
        at = self.at
        ref = self.ref.at[at.z_from(d), at.twin]
        landed(ref, self.ys.at[d], self.yr.at[d], tensor=at.twin)


def whole_lines(small, blocks, depth):
    tiles = []
    for t in range(blocks * depth // LANES):
        tile = jnp.zeros((8, LANES), F32)
        lane = lax.broadcasted_iota(jnp.int32, (8, LANES), 1) + t * LANES
        for b in range(t * LANES // depth, min(blocks, -(-(t + 1) * LANES // depth))):
            line = small[b, :8, :].astype(F32)
            shift = (b * depth - t * LANES) % LANES
            moved = pltpu.roll(line, shift, 1) if shift else line
            tile = jnp.where((lane >= b * depth) & (lane < (b + 1) * depth), moved, tile)
        tiles.append(tile)
    return jnp.concatenate(tiles, axis=1)


def front_kernel(ns, nz, heads, kv, *refs):
    ins, outs, (small, ypart, yland, *sems) = refs[:10], refs[10:22], refs[22:]
    (wa_in, small_in, gate_in, up_in, down_in, hidden, cot_in, cosine, sine, mask) = ins
    (wa, gate_w, up_w, down_w, lines, n2, cot, resid, query, kv_all, probs, attn) = outs
    n_spread = len(Spread.sems(ns, nz))
    n_tokens = len(Tokens.sems(nz))
    at, sends = Place(ns, nz), Sends()
    depth = wa_in.shape[0]
    rows, width = hidden.shape
    half = rows // 2
    q_cols = heads * HD
    qkv_cols = q_cols + 2 * kv * HD

    def spread(i, src, dst):
        return Spread(at, sends, src, dst, sems[i * n_spread:(i + 1) * n_spread])

    def block(ref):
        return lambda s1, z1: ref.at[pl.ds(pl.multiple_of((s1 * nz + z1) * depth, SUBLANES), depth)]

    w_attn = spread(0, lambda z2: wa_in, block(wa))
    w_small = spread(1, lambda z2: small_in, lambda s1, z1: small.at[s1 * nz + z1])
    ffn = [
        spread(2 + i, lambda z2, src=src: src.at[z2], block(dst))
        for i, (src, dst) in enumerate(((gate_in, gate_w), (up_in, up_w), (down_in, down_w)))
    ]
    rest = sems[5 * n_spread:]
    t_cot = Tokens(at, sends, cot, rest[:n_tokens])
    t_n2 = Tokens(at, sends, n2, rest[n_tokens:2 * n_tokens])
    kvs, kvr, yps, ypr, cot_sem = rest[2 * n_tokens:]

    at.greet()
    w_small.over_z()
    w_small.own_block()
    w_attn.over_z()
    w_attn.own_block()
    ffn[0].over_z()
    ffn[0].own_block()
    my_half = cot_in.at[pl.ds(pl.multiple_of(at.y * half, SUBLANES), half)]
    sends.here(cot_in.at[pl.ds(0, half)], cot.at[at.z, 0], cot_sem.at[0])
    sends.here(cot_in.at[pl.ds(half, half)], cot.at[at.z, 1], cot_sem.at[1])

    hidden_f = hidden[...].astype(F32)
    factor1 = lax.rsqrt(jnp.mean(hidden_f * hidden_f, axis=1, keepdims=True) + EPSILON)
    w_small.pass_all()
    w_attn.pass_all()
    w_small.finish()
    gains = whole_lines(small, ns * nz, depth)
    lines[...] = gains
    normed1 = (hidden[...].astype(F32) * factor1 * gains[0:1, :]).astype(BF16)
    w_attn.finish()

    width_each = HD // (ns * nz)
    lane = lax.broadcasted_iota(jnp.int32, (8, LANES), 1)
    bias = jnp.zeros((8, LANES), F32)
    for b in range(ns * nz):
        line = small[b, 8:16, :].astype(F32)
        moved = pltpu.roll(line, b * width_each, 1) if b else line
        bias = jnp.where((lane >= b * width_each) & (lane < (b + 1) * width_each), moved, bias)
    cos_t, sin_t = cosine[...], sine[...]

    def projected(head):
        part = jnp.dot(
            normed1, wa[:, head * HD:(head + 1) * HD], preferred_element_type=F32
        )
        return part + bias[head:head + 1, :]

    def rotated(values):
        return values * cos_t + pltpu.roll(values, HD // 2, 1) * sin_t

    for j in range(kv):
        kv_all[at.z, :, j * HD:(j + 1) * HD] = rotated(projected(heads + j)).astype(BF16)
        kv_all[at.z, :, (kv + j) * HD:(kv + j + 1) * HD] = projected(heads + kv + j).astype(BF16)
    for d in range(1, nz):
        sends.go(kv_all.at[at.z], kv_all.at[at.z], kvs.at[d], kvr.at[d], context=at.z_to(d))
    ffn[1].over_z()
    ffn[1].own_block()
    t_cot.over_z(my_half)
    ffn[0].pass_all()
    for h in range(heads):
        query[:, h * HD:(h + 1) * HD] = rotated(projected(h)).astype(BF16)
    for d in range(1, nz):
        src = kv_all.at[at.z_from(d)]
        landed(src, kvs.at[d], kvr.at[d], context=at.z_from(d))

    scale = HD ** (-0.5)
    group_rows = nz * rows
    keep = mask[...] > 0
    repeat = heads // kv
    for h in range(heads):
        j = h // repeat
        keys = kv_all[:, :, j * HD:(j + 1) * HD].reshape(group_rows, HD)
        values = kv_all[:, :, (kv + j) * HD:(kv + j + 1) * HD].reshape(group_rows, HD)
        scores = lax.dot_general(
            query[:, h * HD:(h + 1) * HD], keys, (((1,), (1,)), ((), ())),
            preferred_element_type=F32,
        )
        scores = jnp.where(keep, scores * scale, -1e30)
        peak = jnp.max(scores, axis=1, keepdims=True)
        lse = peak + jnp.log(jnp.sum(jnp.exp(scores - peak), axis=1, keepdims=True))
        p = jnp.exp(scores - lse)
        probs[h * rows:(h + 1) * rows, :] = p
        out = jnp.dot(p.astype(BF16), values, preferred_element_type=F32)
        attn[:, h * HD:(h + 1) * HD] = out.astype(BF16)
    part = lax.dot_general(
        attn[...], wa[:, qkv_cols:qkv_cols + q_cols], (((1,), (1,)), ((), ())),
        preferred_element_type=F32,
    ).astype(BF16)
    ypart[0] = part[:half]
    ypart[1] = part[half:]
    sends.go(ypart.at[at.twin], yland, yps, ypr, tensor=at.twin)
    ffn[2].over_z()
    ffn[2].own_block()
    for d in range(1, nz):
        t_cot.pass_z(d)
    ffn[1].pass_all()

    landed(yland, yps, ypr, tensor=at.twin)
    base = pl.multiple_of(at.y * half, SUBLANES)
    total = ypart[at.y].astype(F32) + yland[...].astype(F32)
    res = hidden[pl.ds(base, half), :].astype(F32) + total
    resid[...] = res
    factor2 = lax.rsqrt(jnp.mean(res * res, axis=1, keepdims=True) + EPSILON)
    n2[at.z, at.y] = (res * factor2 * gains[1:2, :]).astype(BF16)
    t_n2.over_z(n2.at[at.z, at.y])
    t_n2.over_y(0, n2.at[at.z, at.y])
    for d in range(1, nz):
        t_n2.pass_z(d)
    ffn[2].pass_all()
    for d in range(nz):
        t_n2.wait_y(d)
    for d in range(1, nz):
        t_cot.wait_y(d)
    for item in ffn:
        item.finish()
    sends.drain()


def front(ns, nz, heads, kv, wa_in, small_in, ffn_in, hidden, cot, cosine, sine, mask):
    rows, width = hidden.shape
    owners = ns * nz
    half = rows // 2
    unit = ffn_in[0].shape[2]
    wide = owners * wa_in.shape[0]
    dma = pltpu.SemaphoreType.DMA
    shape = jax.ShapeDtypeStruct
    vmem = pl.BlockSpec(memory_space=pltpu.VMEM)
    anyspace = pl.BlockSpec(memory_space=pl.ANY)
    return pl.pallas_call(
        functools.partial(front_kernel, ns, nz, heads, kv),
        out_shape=[
            shape((wide, wa_in.shape[1]), BF16),
            *[shape((wide, unit), BF16)] * 3,
            shape((8, wide), F32),
            shape((nz, 2, half, width), BF16),
            shape((nz, 2, half, width), BF16),
            shape((half, width), F32),
            shape((rows, heads * HD), BF16),
            shape((nz, rows, 2 * kv * HD), BF16),
            shape((heads * rows, nz * rows), F32),
            shape((rows, heads * HD), BF16),
        ],
        in_specs=[anyspace] * 5 + [vmem, anyspace] + [vmem] * 3,
        out_specs=[vmem] + [anyspace] * 3 + [vmem] * 8,
        scratch_shapes=[
            pltpu.VMEM((owners, 16, LANES), BF16),
            pltpu.VMEM((2, half, width), BF16),
            pltpu.VMEM((half, width), BF16),
        ]
        + Spread.sems(ns, nz) * 5
        + Tokens.sems(nz) * 2
        + [dma((nz,)), dma((nz,)), dma, dma, dma((2,))],
        compiler_params=pltpu.CompilerParams(
            collective_id=0, has_side_effects=True, vmem_limit_bytes=VMEM_BYTES
        ),
    )(wa_in, small_in, *ffn_in, hidden, cot, cosine, sine, mask)


def ffn_kernel(gate_in, up_in, down_in, n2, cot, act, d_gate, d_up, ffn_part, dn2_part, *scratch):
    gate_w, up_w, down_w, gate, up_val, d_act, sem = scratch
    loads = [
        pltpu.make_async_copy(src, dst, sem.at[i])
        for i, (src, dst) in enumerate(((gate_in, gate_w), (up_in, up_w), (down_in, down_w)))
    ]
    for load in loads:
        load.start()
    for load, left, weight, out in zip(loads, (n2, n2, cot), (gate_w, up_w, down_w), (gate, up_val, d_act)):
        load.wait()
        out[...] = jnp.dot(left[...], weight[...], preferred_element_type=F32)

    tall = 32

    @pl.loop(0, gate.shape[0] // tall)
    def _(i):
        line = pl.ds(pl.multiple_of(i * tall, tall), tall)
        g, u, d = gate[line, :], up_val[line, :], d_act[line, :]
        sigma = jax.nn.sigmoid(g)
        silu_val = g * sigma
        act[line, :] = (silu_val * u).astype(BF16)
        d_gate[line, :] = (d * u * sigma * (1.0 + g * (1.0 - sigma))).astype(BF16)
        d_up[line, :] = (d * silu_val).astype(BF16)

    def back(left, weight):
        return lax.dot_general(
            left[...], weight[...], (((1,), (1,)), ((), ())), preferred_element_type=F32
        )

    dn2_part[...] = (back(d_gate, gate_w) + back(d_up, up_w)).astype(BF16)
    ffn_part[...] = back(act, down_w).astype(BF16)


def ffn(gate_w, up_w, down_w, n2, cot):
    rows, width = n2.shape
    unit = gate_w.shape[1]
    shape = jax.ShapeDtypeStruct
    vmem = pl.BlockSpec(memory_space=pltpu.VMEM)
    anyspace = pl.BlockSpec(memory_space=pl.ANY)
    return pl.pallas_call(
        ffn_kernel,
        out_shape=[shape((rows, unit), BF16)] * 3 + [shape((rows, width), BF16)] * 2,
        in_specs=[anyspace] * 3 + [vmem] * 2,
        out_specs=[vmem] * 5,
        scratch_shapes=[pltpu.VMEM((width, unit), BF16)] * 3
        + [pltpu.VMEM((rows, unit), F32)] * 3
        + [pltpu.SemaphoreType.DMA((3,))],
        compiler_params=pltpu.CompilerParams(vmem_limit_bytes=VMEM_BYTES),
    )(gate_w, up_w, down_w, n2, cot)


def turn_first(left, right):
    return lax.dot_general(left, right, (((0,), (0,)), ((), ())), preferred_element_type=F32)


def turn_last(left, right):
    return lax.dot_general(left, right, (((1,), (1,)), ((), ())), preferred_element_type=F32)


class Return:
    def __init__(self, at, sends, make, bufs, out, sems):
        self.at, self.sends, self.make, self.out = at, sends, make, out
        self.stage, self.acc, self.landc, self.landx = bufs
        self.cs, self.cr, self.xs, self.xr, self.zs, self.zr, self.own = sems
        self.depth = self.acc.shape[1] // at.nz
        self.copy = None

    @staticmethod
    def sems(ns, nz):
        dma, no = pltpu.SemaphoreType.DMA, ns // 2
        return [dma((no,)), dma((no,)), dma((no,)), dma((no,)), dma((nz,)), dma((nz,)), dma]

    @staticmethod
    def bufs(ns, nz, depth, cols):
        no = ns // 2
        return [pltpu.VMEM((n, nz * depth, cols), BF16) for n in (no, no, no, no)]

    def give(self, o):
        at = self.at
        self.stage[o] = self.make(at.mate_to(o)).astype(BF16)
        self.sends.go(
            self.stage.at[o], self.landc.at[o], self.cs.at[o], self.cr.at[o], shard=at.mate
        )
        self.acc[o] = self.make(at.s_to(o)).astype(BF16)

    def give_all(self):
        for o in (*range(1, self.at.no), 0):
            self.give(o)

    def add(self, o, others):
        @pl.loop(0, self.at.nz)
        def _(i):
            line = pl.ds(pl.multiple_of(i * self.depth, SUBLANES), self.depth)
            total = self.acc[o, line, :].astype(F32)
            for other, k in others:
                total = total + other[k, line, :].astype(F32)
            self.acc[o, line, :] = total.astype(BF16)

    def over_s(self):
        at = self.at
        for o in range(1, at.no):
            landed(self.landc.at[o], self.cs.at[o], self.cr.at[o], shard=at.mate)
            self.add(o, [(self.landc, o)])
            self.sends.go(
                self.acc.at[o], self.landx.at[o], self.xs.at[o], self.xr.at[o], shard=at.s_to(o)
            )

    def piece(self, z2):
        return self.acc.at[0, pl.ds(pl.multiple_of(z2 * self.depth, SUBLANES), self.depth)]

    def over_z(self):
        at = self.at
        landed(self.landc.at[0], self.cs.at[0], self.cr.at[0], shard=at.mate)
        for o in range(1, at.no):
            landed(self.landx.at[o], self.xs.at[o], self.xr.at[o], shard=at.s_from(o))
        self.add(0, [(self.landc, 0)] + [(self.landx, o) for o in range(1, at.no)])
        for d in range(1, at.nz):
            z2 = at.z_to(d)
            self.sends.go(
                self.piece(z2), self.out.at[at.z], self.zs.at[d], self.zr.at[d], context=z2
            )
        self.copy = pltpu.make_async_copy(self.piece(at.z), self.out.at[at.z], self.own)
        self.copy.start()

    def finish(self):
        at = self.at
        self.copy.wait()
        for d in range(1, at.nz):
            z1 = at.z_from(d)
            landed(self.out.at[z1], self.zs.at[d], self.zr.at[d], context=z1)


class Reduce:
    def __init__(self, at, sends, parts, bufs, sems):
        self.at, self.sends, self.parts = at, sends, parts
        self.landy, self.stage, self.landz = bufs
        self.ys, self.yr, self.zs, self.zr = sems
        self.own = None

    @staticmethod
    def sems(nz):
        dma = pltpu.SemaphoreType.DMA
        return [dma((nz,)), dma((nz,)), dma((nz,)), dma((nz,))]

    @staticmethod
    def bufs(nz, half, width):
        return [pltpu.VMEM((nz, half, width), BF16)] * 3

    def over_y(self):
        at = self.at
        for d in (*range(1, at.nz), 0):
            self.sends.go(
                self.parts.at[at.z_to(d), at.twin], self.landy.at[d], self.ys.at[d],
                self.yr.at[d], tensor=at.twin,
            )

    def pass_y(self):
        at = self.at
        for d in (*range(1, at.nz), 0):
            landed(self.landy.at[d], self.ys.at[d], self.yr.at[d], tensor=at.twin)
            total = self.parts[at.z_to(d), at.y].astype(F32) + self.landy[d].astype(F32)
            self.stage[d] = total.astype(BF16)
            if d:
                self.sends.go(
                    self.stage.at[d], self.landz.at[d], self.zs.at[d], self.zr.at[d],
                    context=at.z_to(d),
                )

    def total(self):
        at = self.at
        total = self.stage[0].astype(F32)
        for d in range(1, at.nz):
            landed(self.landz.at[d], self.zs.at[d], self.zr.at[d], context=at.z_from(d))
            total = total + self.landz[d].astype(F32)
        return total


def piece_of_lines(lines, b, depth):
    first, off = divmod(b * depth, LANES)
    tile = lines[:, first * LANES:(first + 1) * LANES]
    if not off:
        return tile
    tile = pltpu.roll(tile, LANES - off, 1)
    if off + depth <= LANES:
        return tile
    after = pltpu.roll(lines[:, (first + 1) * LANES:(first + 2) * LANES], LANES - off, 1)
    lane = lax.broadcasted_iota(jnp.int32, (8, LANES), 1)
    return jnp.where(lane < LANES - off, tile, after)


N_BACK_IN = 18


def back_kernel(ns, nz, heads, kv, *refs):
    ins, refs = refs[:N_BACK_IN], refs[N_BACK_IN:]
    (wa_in, n2_in, cot_in, act_in, d_gate_in, d_up_in, probs_in, dn2_part, ffn_part, hidden, resid,
     cot_own, lines, query, kv_all, attn, cosine, sine) = ins
    (block_out, input_grad, attn_grad, small_out, *ffn_out), refs = refs[:7], refs[7:]
    (wa, n2, cot, act, d_gate, d_up, probs), refs = refs[:7], refs[7:]
    fetch_sem, refs = refs[0], refs[1:]
    at, sends = Place(ns, nz), Sends()
    depth = lines.shape[1] // (ns * nz)
    rows, width = hidden.shape
    half = rows // 2
    group_rows = nz * rows
    q_cols = heads * HD
    qkv_cols = q_cols + 2 * kv * HD
    wide = nz * depth
    scale = HD ** (-0.5)
    n_ret, n_red = len(Return.sems(ns, nz)), len(Reduce.sems(nz))

    loads = {}
    for i, (name, src, dst) in enumerate((
        ("n2", n2_in, n2), ("d_gate", d_gate_in, d_gate), ("d_up", d_up_in, d_up),
        ("cot", cot_in, cot), ("act", act_in, act), ("wa", wa_in, wa), ("probs", probs_in, probs),
    )):
        loads[name] = pltpu.make_async_copy(src, dst, fetch_sem.at[i])
        loads[name].start()

    def columns(ref, s1):
        return ref[:, pl.ds(pl.multiple_of(s1 * wide, LANES), wide)]

    rets = []
    makers = (
        lambda s1: turn_first(columns(n2, s1), d_gate[...]),
        lambda s1: turn_first(columns(n2, s1), d_up[...]),
        lambda s1: turn_first(columns(cot, s1), act[...]),
    )
    for i in range(3):
        bufs, sems, refs = refs[:4], refs[4:4 + n_ret], refs[4 + n_ret:]
        rets.append(Return(at, sends, makers[i], bufs, ffn_out[i], sems))
    bufs, sems, attn_land, refs = refs[:4], refs[4:4 + n_ret], refs[4 + n_ret], refs[5 + n_ret:]
    normed1_b, d_resid_b, d_projb, refs = refs[0], refs[1], refs[2], refs[3:]

    def attn_maker(s1):
        grad_qkv = turn_first(columns(normed1_b, s1), d_projb[...])
        both = d_resid_b[:, :, pl.ds(pl.multiple_of(s1 * wide, LANES), wide)].reshape(rows, wide)
        grad_out = turn_first(both, attn[...])
        return jnp.concatenate([grad_qkv, grad_out], axis=1)

    r_attn = Return(at, sends, attn_maker, bufs, attn_land, sems)
    reduces = []
    for parts in (dn2_part, ffn_part):
        bufs, sems, refs = refs[:3], refs[3:3 + n_red], refs[3 + n_red:]
        reduces.append(Reduce(at, sends, parts, bufs, sems))
    r_dn2, r_ffn = reduces
    (d_resid_f, d_attn, d_score, dkv, dkv_land, dn1_part, dn1_land, small, small_land, small_z,
     small_zland, small_y, small_yland, dkvs, dkvr, shs, shr, szs, szr, ysems, yrecv) = refs

    at.greet(everyone=True)
    r_dn2.over_y()
    loads["n2"].wait()
    loads["d_gate"].wait()
    rets[0].give_all()
    r_dn2.pass_y()
    r_ffn.over_y()
    loads["d_up"].wait()
    rets[1].give_all()
    rets[0].over_s()

    res = resid[...]
    factor2 = lax.rsqrt(jnp.mean(res * res, axis=1, keepdims=True) + EPSILON)
    unit2 = res * factor2
    dn2 = r_dn2.total()
    grad_g2 = jnp.sum(dn2 * unit2, axis=0, keepdims=True)
    scaled = dn2 * lines[1:2, :]
    back2 = factor2 * (scaled - unit2 * jnp.mean(scaled * unit2, axis=1, keepdims=True))
    base = pl.multiple_of(at.y * half, SUBLANES)
    d_res = cot_own[pl.ds(base, half), :].astype(F32) + back2
    d_resid_f[at.y] = d_res
    d_resid_b[at.y] = d_res.astype(BF16)
    mine_b, mine_f = d_resid_b.at[at.y], d_resid_f.at[at.y]
    sends.go(mine_b, mine_b, ysems.at[0], yrecv.at[0], tensor=at.twin)
    sends.go(mine_f, mine_f, ysems.at[1], yrecv.at[1], tensor=at.twin)

    loads["cot"].wait()
    loads["act"].wait()
    rets[2].give_all()
    rets[1].over_s()
    r_ffn.pass_y()
    hidden_f = hidden[...].astype(F32)
    factor1 = lax.rsqrt(jnp.mean(hidden_f * hidden_f, axis=1, keepdims=True) + EPSILON)
    normed1_b[...] = (hidden_f * factor1 * lines[0:1, :]).astype(BF16)
    loads["wa"].wait()
    loads["probs"].wait()
    other_b = d_resid_b.at[at.twin]
    landed(other_b, ysems.at[0], yrecv.at[0], tensor=at.twin)

    d_attn[...] = jnp.dot(
        d_resid_b[...].reshape(rows, width), wa[:, qkv_cols:qkv_cols + q_cols],
        preferred_element_type=F32,
    ).astype(BF16)
    rets[2].over_s()
    cos_t, sin_t = cosine[...], sine[...]

    def unrotated(values):
        return values * cos_t - pltpu.roll(values, HD // 2, 1) * sin_t

    bias_rows = [None] * (heads + 2 * kv)

    def place(head, grad):
        bias_rows[head] = jnp.sum(grad, axis=0, keepdims=True)
        d_projb[:, head * HD:(head + 1) * HD] = grad.astype(BF16)

    repeat = heads // kv
    for j in range(kv):
        keys = kv_all[:, :, j * HD:(j + 1) * HD].reshape(group_rows, HD)
        values = kv_all[:, :, (kv + j) * HD:(kv + j + 1) * HD].reshape(group_rows, HD)
        d_values = jnp.zeros((group_rows, HD), F32)
        d_keys = jnp.zeros((group_rows, HD), F32)
        for h in range(j * repeat, (j + 1) * repeat):
            d_out = d_attn[:, h * HD:(h + 1) * HD]
            p = probs[h * rows:(h + 1) * rows, :]
            d_prob = turn_last(d_out, values)
            delta = jnp.sum(
                d_out.astype(F32) * attn[:, h * HD:(h + 1) * HD].astype(F32), axis=1, keepdims=True
            )
            d_s = (p * (d_prob - delta)).astype(BF16)
            d_score[...] = d_s
            place(h, unrotated(jnp.dot(d_s, keys, preferred_element_type=F32) * scale))
            d_keys = d_keys + turn_first(d_score[...], query[:, h * HD:(h + 1) * HD])
            d_values = d_values + turn_first(p.astype(BF16), d_out)
        for i, grad in ((j, d_keys * scale), (kv + j, d_values)):
            dkv[:, :, i * HD:(i + 1) * HD] = grad.astype(BF16).reshape(nz, rows, HD)
    for d in range(1, nz):
        sends.go(dkv.at[at.z_to(d)], dkv_land.at[d], dkvs.at[d], dkvr.at[d], context=at.z_to(d))
    rets[0].over_z()
    d_own = dkv[at.z].astype(F32)
    for d in range(1, nz):
        landed(dkv_land.at[d], dkvs.at[d], dkvr.at[d], context=at.z_from(d))
        d_own = d_own + dkv_land[d].astype(F32)
    for j in range(kv):
        place(heads + j, unrotated(d_own[:, j * HD:(j + 1) * HD]))
        place(heads + kv + j, d_own[:, (kv + j) * HD:(kv + j + 1) * HD])
    dn1_part[...] = turn_last(d_projb[...], wa[:, :qkv_cols]).astype(BF16)
    sends.go(dn1_part, dn1_land, ysems.at[2], yrecv.at[2], tensor=at.twin)
    r_attn.give_all()
    rets[1].over_z()
    r_attn.over_s()

    out_half = r_ffn.total() + resid[...]
    block_out[at.y] = out_half.astype(BF16)
    sends.go(block_out.at[at.y], block_out.at[at.y], ysems.at[3], yrecv.at[3], tensor=at.twin)

    landed(dn1_land, ysems.at[2], yrecv.at[2], tensor=at.twin)
    landed(d_resid_f.at[at.twin], ysems.at[1], yrecv.at[1], tensor=at.twin)
    dn1 = dn1_part[...].astype(F32) + dn1_land[...].astype(F32)
    hidden_f = hidden[...].astype(F32)
    factor1 = lax.rsqrt(jnp.mean(hidden_f * hidden_f, axis=1, keepdims=True) + EPSILON)
    unit1 = hidden_f * factor1
    row = lax.broadcasted_iota(jnp.int32, (rows, 1), 0)
    my_row = (row >= at.y * half) & (row < (at.y + 1) * half)
    grad_g1 = jnp.sum(jnp.where(my_row, dn1 * unit1, 0.0), axis=0, keepdims=True)
    scaled = dn1 * lines[0:1, :]
    back1 = factor1 * (scaled - unit1 * jnp.mean(scaled * unit1, axis=1, keepdims=True))
    input_grad[...] = d_resid_f[...].reshape(rows, width) + back1

    gains = jnp.concatenate([grad_g1, grad_g2, jnp.zeros((6, width), F32)], axis=0)
    bias = jnp.concatenate(bias_rows, axis=0)
    each = HD // (ns * nz)
    for b in range(ns * nz):
        moved = pltpu.roll(bias, LANES - b * each, 1) if b else bias
        small[b // nz, b % nz] = jnp.concatenate([piece_of_lines(gains, b, depth), moved], axis=0)
    for k in range(1, ns):
        s2 = lax.rem(at.s + k, ns)
        sends.go(small.at[s2], small_land.at[k], shs.at[k], shr.at[k], shard=s2)
    rets[2].over_z()
    total = small[at.s]
    for k in range(1, ns):
        s1 = lax.rem(at.s - k + ns, ns)
        landed(small_land.at[k], shs.at[k], shr.at[k], shard=s1)
        total = total + small_land[k]
    small_z[...] = total
    for d in range(1, nz):
        sends.go(small_z.at[at.z_to(d)], small_zland.at[d], szs.at[d], szr.at[d], context=at.z_to(d))
    r_attn.over_z()
    total = small_z[at.z]
    for d in range(1, nz):
        landed(small_zland.at[d], szs.at[d], szr.at[d], context=at.z_from(d))
        total = total + small_zland[d]
    small_y[...] = total
    sends.go(small_y, small_yland, ysems.at[4], yrecv.at[4], tensor=at.twin)
    for ret in rets:
        ret.finish()
    landed(small_yland, ysems.at[4], yrecv.at[4], tensor=at.twin)
    small_out[:8, :] = small_y[:8, :] + small_yland[:8, :]
    small_out[8:, :] = small_y[8:, :]
    landed(block_out.at[at.twin], ysems.at[3], yrecv.at[3], tensor=at.twin)
    r_attn.finish()
    total = attn_land[0].astype(F32)
    for z1 in range(1, nz):
        total = total + attn_land[z1].astype(F32)
    attn_grad[...] = total
    sends.drain()


def back(ns, nz, heads, kv, wa, n2, cot, act, d_gate, d_up, probs, dn2_part, ffn_part, hidden, resid,
         cot_own, lines, query, kv_all, attn, cosine, sine):
    rows, width = hidden.shape
    owners, half, group_rows = ns * nz, rows // 2, nz * rows
    depth, unit = width // owners, act.shape[1]
    q_cols = heads * HD
    cols = wa.shape[1]
    dma = pltpu.SemaphoreType.DMA
    shape = jax.ShapeDtypeStruct
    vmem = pl.BlockSpec(memory_space=pltpu.VMEM)
    anyspace = pl.BlockSpec(memory_space=pl.ANY)
    parts = (nz, 2, half, width)
    big = (wa, n2, cot, act, d_gate, d_up, probs)
    scratch = [pltpu.VMEM(a.shape, a.dtype) for a in big] + [dma((len(big),))]
    for _ in range(3):
        scratch += Return.bufs(ns, nz, depth, unit) + Return.sems(ns, nz)
    scratch += Return.bufs(ns, nz, depth, cols) + Return.sems(ns, nz)
    scratch += [
        pltpu.VMEM((nz, depth, cols), BF16),
        pltpu.VMEM((rows, width), BF16),
        pltpu.VMEM((2, half, width), BF16),
        pltpu.VMEM((rows, cols - q_cols), BF16),
    ]
    for _ in range(2):
        scratch += Reduce.bufs(nz, half, width) + Reduce.sems(nz)
    scratch += [
        pltpu.VMEM((2, half, width), F32),
        pltpu.VMEM((rows, q_cols), BF16),
        pltpu.VMEM((rows, group_rows), BF16),
        pltpu.VMEM((nz, rows, 2 * kv * HD), BF16),
        pltpu.VMEM((nz, rows, 2 * kv * HD), BF16),
        pltpu.VMEM((rows, width), BF16),
        pltpu.VMEM((rows, width), BF16),
        pltpu.VMEM((ns, nz, 16, LANES), F32),
        pltpu.VMEM((ns, nz, 16, LANES), F32),
        pltpu.VMEM((nz, 16, LANES), F32),
        pltpu.VMEM((nz, 16, LANES), F32),
        pltpu.VMEM((16, LANES), F32),
        pltpu.VMEM((16, LANES), F32),
        dma((nz,)), dma((nz,)), dma((ns,)), dma((ns,)), dma((nz,)), dma((nz,)), dma((5,)), dma((5,)),
    ]
    return pl.pallas_call(
        functools.partial(back_kernel, ns, nz, heads, kv),
        out_shape=[
            shape((2, half, width), BF16),
            shape((rows, width), F32),
            shape((depth, cols), F32),
            shape((16, LANES), F32),
            *[shape((nz, depth, unit), BF16)] * 3,
        ],
        in_specs=[anyspace] * 7 + [vmem] * 11,
        out_specs=[vmem] * 4 + [anyspace] * 3,
        scratch_shapes=scratch,
        compiler_params=pltpu.CompilerParams(
            collective_id=1, has_side_effects=True, vmem_limit_bytes=VMEM_BYTES
        ),
    )(*big, dn2_part.reshape(parts), ffn_part.reshape(parts), hidden, resid, cot_own, lines, query,
      kv_all, attn, cosine, sine)


def fast_step(
    ns,
    nz,
    hidden_in,
    segment_ids,
    attn_gain,
    qkv_weight,
    qkv_bias,
    out_weight,
    ffn_gain,
    gate_weight,
    up_weight,
    down_weight,
    out_cotangent,
):
    rows, width = hidden_in.shape
    depth, hidden_units = gate_weight.shape
    parts = 2
    heads = H // parts
    kv = KVH // parts
    block_index = lax.axis_index("context")
    unit_cols = -(-hidden_units // (nz * LANES)) * LANES
    padded = unit_cols * nz
    q_cols = heads * HD
    k_cols = kv * HD

    def by_place(weight):
        full = jnp.pad(weight, ((0, 0), (0, padded - hidden_units)))
        return jnp.transpose(full.reshape(depth, nz, unit_cols), (1, 0, 2))

    ffn_in = [by_place(w) for w in (gate_weight, up_weight, down_weight.T)]
    wa_in = jnp.concatenate([qkv_weight, out_weight.T], axis=1)
    gains_in = jnp.pad(jnp.stack([attn_gain, ffn_gain]), ((0, 6), (0, LANES - depth)))
    bias_in = jnp.pad(qkv_bias, ((0, 0), (0, LANES - qkv_bias.shape[1])))
    small_in = jnp.concatenate([gains_in, bias_in], axis=0)

    seg_all = segment_ids[0]
    group_rows = seg_all.shape[0]
    first_row = block_index * rows
    index_all = jnp.arange(group_rows, dtype=jnp.int32)
    seg_local = lax.dynamic_slice_in_dim(seg_all, first_row, rows)
    index_local = first_row + jnp.arange(rows, dtype=jnp.int32)
    earlier = jnp.sum((seg_all[None, :] < seg_local[:, None]).astype(jnp.int32), axis=1)
    allowed = (seg_local[:, None] == seg_all[None, :]) & (
        index_local[:, None] >= index_all[None, :]
    )
    cosine, sine = rotary_tables(index_local - earlier)

    wa, gate_full, up_full, down_full, lines, n2, cot, resid_half, query, kv_all, p_soft, attn = front(
        ns, nz, heads, kv, wa_in, small_in, ffn_in, hidden_in, out_cotangent, cosine, sine,
        allowed.astype(F32),
    )
    act, d_gate, d_up, ffn_part, dn2_part = ffn(
        gate_full, up_full, down_full, n2.reshape(group_rows, width), cot.reshape(group_rows, width)
    )
    block_out, input_grad, attn_grad, small, grad_gate, grad_up, grad_down = back(
        ns, nz, heads, kv, wa, n2.reshape(group_rows, width), cot.reshape(group_rows, width), act,
        d_gate, d_up, p_soft, dn2_part, ffn_part, hidden_in, resid_half, out_cotangent, lines, query,
        kv_all, attn, cosine, sine,
    )

    def all_columns(grad):
        return jnp.transpose(grad, (1, 0, 2)).reshape(depth, padded)[:, :hidden_units].astype(F32)

    qkv_cols = q_cols + 2 * k_cols
    return (
        block_out.reshape(rows, width),
        input_grad,
        small[0, :depth],
        attn_grad[:, :qkv_cols],
        small[8:, : qkv_bias.shape[1]],
        attn_grad[:, qkv_cols:].T,
        small[1, :depth],
        all_columns(grad_gate),
        all_columns(grad_up),
        all_columns(grad_down).T,
    )


def general_step(
    hidden_in,
    segment_ids,
    attn_gain,
    qkv_weight,
    qkv_bias,
    out_weight,
    ffn_gain,
    gate_weight,
    up_weight,
    down_weight,
    out_cotangent,
):
    rows, width = hidden_in.shape
    depth = gate_weight.shape[0]
    hidden_units = gate_weight.shape[1]
    parts = lax.axis_size("tensor")
    blocks = lax.axis_size("context")
    heads = H // parts
    kv = KVH // parts
    repeat = H // KVH
    scale = HD ** (-0.5)
    block_index = lax.axis_index("context")
    part_index = lax.axis_index("tensor")
    half_rows = rows // parts
    unit_cols = -(-hidden_units // (blocks * LANES)) * LANES
    padded = unit_cols * blocks

    def spread(weight):
        full = jnp.pad(weight, ((0, 0), (0, padded - hidden_units)))
        mine = lax.all_to_all(full, "context", split_axis=1, concat_axis=0, tiled=True)
        mine = mine.reshape(blocks * depth, unit_cols)
        return lax.all_gather(mine, "shard", axis=0, tiled=True)

    gate_full = spread(gate_weight)
    up_full = spread(up_weight)
    down_full = spread(down_weight.T)
    gain_one = lax.all_gather(attn_gain, OWNERS, axis=0, tiled=True).astype(F32)
    gain_two = lax.all_gather(ffn_gain, OWNERS, axis=0, tiled=True).astype(F32)
    bias = lax.all_gather(qkv_bias, OWNERS, axis=1, tiled=True).reshape(-1).astype(F32)
    qkv_full = lax.all_gather(qkv_weight, OWNERS, axis=0, tiled=True)
    out_full = lax.all_gather(out_weight.T, OWNERS, axis=0, tiled=True)

    seg_all = segment_ids[0]
    group_rows = seg_all.shape[0]
    first_row = block_index * rows
    index_all = jnp.arange(group_rows, dtype=jnp.int32)
    earlier = jnp.sum((seg_all[None, :] < seg_all[:, None]).astype(jnp.int32), axis=1)
    positions = index_all - earlier
    seg_local = lax.dynamic_slice_in_dim(seg_all, first_row, rows)
    index_local = first_row + jnp.arange(rows, dtype=jnp.int32)
    allowed = (seg_local[:, None] == seg_all[None, :]) & (
        index_local[:, None] >= index_all[None, :]
    )
    cosine, sine = rotary_tables(positions)
    cos_local = lax.dynamic_slice_in_dim(cosine, first_row, rows)
    sin_local = lax.dynamic_slice_in_dim(sine, first_row, rows)

    hidden_all = lax.all_gather(hidden_in, "context", axis=0, tiled=True)
    normed_all, _, _ = norm_forward(hidden_all.astype(F32), gain_one)
    hidden_f = hidden_in.astype(F32)
    normed1, unit1, factor1 = norm_forward(hidden_f, gain_one)
    q_cols = heads * HD
    k_cols = kv * HD
    query_f = dot(normed1, qkv_full[:, :q_cols]) + bias[:q_cols]
    kv_f = dot(normed_all, qkv_full[:, q_cols:]) + bias[q_cols:]
    query = jnp.transpose(query_f.reshape(rows, heads, HD), (1, 0, 2))
    query = rotate(query, cos_local, sin_local).astype(BF16)
    keys = jnp.transpose(kv_f[:, :k_cols].reshape(group_rows, kv, HD), (1, 0, 2))
    keys = rotate(keys, cosine, sine).astype(BF16)
    values = jnp.transpose(kv_f[:, k_cols:].reshape(group_rows, kv, HD), (1, 0, 2)).astype(BF16)
    query = query.reshape(kv, repeat * rows, HD)
    mask = jnp.tile(allowed, (repeat, 1))
    scores = jnp.where(mask, batched(query, keys, 2, 2) * scale, -1e30)
    peak = jnp.max(scores, axis=2, keepdims=True)
    lse = peak + jnp.log(jnp.sum(jnp.exp(scores - peak), axis=2, keepdims=True))
    p_soft = jnp.exp(scores - lse)
    probs = p_soft.astype(BF16)
    outs = batched(probs, values, 2, 1).astype(BF16)
    attn = jnp.transpose(outs.reshape(heads, rows, HD), (1, 0, 2)).reshape(rows, q_cols)
    attn_part = contract_last(attn, out_full).astype(BF16)

    mine = part_index * half_rows
    attn_half = lax.psum_scatter(attn_part, "tensor", scatter_dimension=0, tiled=True)
    resid_half = lax.dynamic_slice_in_dim(hidden_f, mine, half_rows) + attn_half.astype(F32)
    normed2_half, unit2, factor2 = norm_forward(resid_half, gain_two)
    normed2 = lax.all_gather(normed2_half, TEAM, axis=0, tiled=True)
    cot_half = lax.dynamic_slice_in_dim(out_cotangent, mine, half_rows)
    cot = lax.all_gather(cot_half, TEAM, axis=0, tiled=True)

    gate = dot(normed2, gate_full)
    up_val = dot(normed2, up_full)
    sigma = jax.nn.sigmoid(gate)
    silu_val = gate * sigma
    act = (silu_val * up_val).astype(BF16)
    ffn_part = contract_last(act, down_full).astype(BF16)
    d_act = dot(cot, down_full)
    d_gate = (d_act * up_val * sigma * (1.0 + gate * (1.0 - sigma))).astype(BF16)
    d_up = (d_act * silu_val).astype(BF16)
    dn2_part = (contract_last(d_gate, gate_full) + contract_last(d_up, up_full)).astype(BF16)
    ffn_half = lax.psum_scatter(ffn_part, TEAM, scatter_dimension=0, tiled=True)
    block_half = (resid_half + ffn_half.astype(F32)).astype(BF16)
    block_out = lax.all_gather(block_half, "tensor", axis=0, tiled=True)
    dn2_half = lax.psum_scatter(dn2_part, TEAM, scatter_dimension=0, tiled=True).astype(F32)
    grad_g2, d_back2 = norm_backward(dn2_half, unit2, factor2, gain_two)
    d_resid_half = cot_half.astype(F32) + d_back2

    def give_back(grad):
        part = lax.psum_scatter(grad.astype(BF16), "shard", scatter_dimension=0, tiled=True)
        part = part.reshape(blocks, depth, unit_cols)
        part = lax.all_to_all(part, "context", split_axis=0, concat_axis=2, tiled=True)
        return part.reshape(depth, padded)[:, :hidden_units].astype(F32)

    sum_gate = give_back(contract_first(normed2, d_gate))
    sum_up = give_back(contract_first(normed2, d_up))
    sum_down = give_back(contract_first(cot, act)).T

    d_resid_b = lax.all_gather(d_resid_half.astype(BF16), "tensor", axis=0, tiled=True)
    grad_out = contract_first(d_resid_b, attn)
    d_attn = dot(d_resid_b, out_full).astype(BF16)
    d_outs = jnp.transpose(d_attn.reshape(rows, heads, HD), (1, 0, 2)).reshape(
        kv, repeat * rows, HD
    )
    d_prob = batched(d_outs, values, 2, 2)
    delta = jnp.sum(d_outs.astype(F32) * outs.astype(F32), axis=2, keepdims=True)
    d_score = (p_soft * (d_prob - delta)).astype(BF16)
    d_query = batched(d_score, keys, 2, 1) * scale
    d_keys = batched(d_score, query, 1, 1) * scale
    d_values = batched(probs, d_outs, 1, 1)
    d_kv = jnp.concatenate([d_keys, d_values], axis=0).astype(BF16)
    d_kv = lax.psum_scatter(d_kv, "context", scatter_dimension=1, tiled=True).astype(F32)
    d_query = unrotate(d_query.reshape(heads, rows, HD), cos_local, sin_local)
    d_keys = unrotate(d_kv[:kv], cos_local, sin_local)
    d_proj = jnp.transpose(jnp.concatenate([d_query, d_keys, d_kv[kv:]], axis=0), (1, 0, 2))
    grad_bias = jnp.sum(d_proj, axis=0)
    d_projb = d_proj.reshape(rows, -1).astype(BF16)
    grad_qkv = contract_first(normed1, d_projb)
    dn1_part = contract_last(d_projb, qkv_full).astype(BF16)
    dn1_half = lax.psum_scatter(dn1_part, "tensor", scatter_dimension=0, tiled=True).astype(F32)
    unit1_half = lax.dynamic_slice_in_dim(unit1, mine, half_rows)
    factor1_half = lax.dynamic_slice_in_dim(factor1, mine, half_rows)
    grad_g1, d_back1 = norm_backward(dn1_half, unit1_half, factor1_half, gain_one)
    input_grad = lax.all_gather(d_resid_half + d_back1, "tensor", axis=0, tiled=True)

    gains = lax.psum(jnp.stack([grad_g1, grad_g2]), "tensor")
    sum_gains = lax.psum_scatter(gains, OWNERS, scatter_dimension=1, tiled=True)
    sum_qkv = lax.psum_scatter(grad_qkv.astype(BF16), OWNERS, scatter_dimension=0, tiled=True)
    sum_bias = lax.psum_scatter(grad_bias, OWNERS, scatter_dimension=1, tiled=True)
    sum_out = lax.psum_scatter(grad_out.astype(BF16), OWNERS, scatter_dimension=0, tiled=True)
    return (
        block_out,
        input_grad,
        sum_gains[0],
        sum_qkv.astype(F32),
        sum_bias,
        sum_out.astype(F32).T,
        sum_gains[1],
        sum_gate,
        sum_up,
        sum_down,
    )


def solution(mesh):
    ns, nz, parts = (mesh.shape[a] for a in ("shard", "context", "tensor"))
    rows = P(OWNERS, None)

    def local(*args):
        depth = args[7].shape[0]
        if depth % SUBLANES == 0 and ns % 2 == 0 and ns > 2 and nz > 1 and parts == 2:
            return fast_step(ns, nz, *args)
        return general_step(*args)

    placed = (
        rows,
        P("shard", None),
        P(OWNERS),
        P(OWNERS, "tensor"),
        P("tensor", OWNERS),
        P("tensor", OWNERS),
        P(OWNERS),
        P(OWNERS, "tensor"),
        P(OWNERS, "tensor"),
        P("tensor", OWNERS),
        rows,
    )
    return jax.shard_map(
        local,
        mesh=mesh,
        in_specs=placed,
        out_specs=(
            rows,
            rows,
            P(OWNERS),
            P(OWNERS, "tensor"),
            P("tensor", OWNERS),
            P("tensor", OWNERS),
            P(OWNERS),
            P(OWNERS, "tensor"),
            P(OWNERS, "tensor"),
            P("tensor", OWNERS),
        ),
        check_vma=False,
    )
```

```python
import functools

import jax
import jax.numpy as jnp
from jax import lax
from jax.experimental import pallas as pl
from jax.experimental.pallas import tpu as pltpu
from jax.sharding import PartitionSpec as P

H = 12
KVH = 2
HD = 128
LANES = 128
SUBLANES = 16
BF16 = jnp.bfloat16
F32 = jnp.float32

EPSILON = 1e-06
THETA = 1000000.0

OWNERS = ("shard", "context")
TEAM = ("context", "tensor")
MESH = pl.DeviceIdType.MESH
VMEM_BYTES = 62 * 1024 * 1024


def dot(left, right):
    return jnp.dot(left, right, preferred_element_type=F32)


def contract_last(left, right):
    return lax.dot_general(left, right, (((1,), (1,)), ((), ())), preferred_element_type=F32)


def contract_first(left, right):
    return lax.dot_general(left, right, (((0,), (0,)), ((), ())), preferred_element_type=F32)


def batched(left, right, left_dim, right_dim):
    return lax.dot_general(
        left, right, (((left_dim,), (right_dim,)), ((0,), (0,))), preferred_element_type=F32
    )


def norm_forward(values, gain):
    factor = lax.rsqrt(jnp.mean(values * values, axis=1, keepdims=True) + EPSILON)
    unit = values * factor
    return ((unit * gain).astype(BF16), unit, factor)


def norm_backward(grad_out, unit, factor, gain):
    gain_grad = jnp.sum(grad_out * unit, axis=0)
    scaled = grad_out * gain
    return (gain_grad, factor * (scaled - unit * jnp.mean(scaled * unit, axis=1, keepdims=True)))


def rotary_tables(positions):
    half = HD // 2
    freqs = THETA ** (-(2.0 * jnp.arange(half, dtype=F32)) / HD)
    angles = positions.astype(F32)[:, None] * freqs[None, :]
    cosine, sine = jnp.cos(angles), jnp.sin(angles)
    return (
        jnp.concatenate([cosine, cosine], axis=1),
        jnp.concatenate([-sine, sine], axis=1),
    )


def swap_halves(values):
    half = values.shape[-1] // 2
    return jnp.concatenate([values[..., half:], values[..., :half]], axis=-1)


def rotate(values, cosine, sine):
    return values * cosine + swap_halves(values) * sine


def unrotate(values, cosine, sine):
    return values * cosine - swap_halves(values) * sine


class Place:
    def __init__(self, ns, nz):
        self.ns, self.nz, self.no = ns, nz, ns // 2
        self.s, self.z, self.y = (lax.axis_index(a) for a in ("shard", "context", "tensor"))
        self.core = lax.rem(self.s, 2)
        self.outer = lax.div(self.s, 2)
        self.mate = self.s + 1 - 2 * self.core
        self.twin = 1 - self.y

    def z_to(self, d):
        return lax.rem(self.z + d, self.nz)

    def z_from(self, d):
        return lax.rem(self.z - d + self.nz, self.nz)

    def s_to(self, o):
        return lax.rem(self.outer + o, self.no) * 2 + self.core

    def s_from(self, o):
        return lax.rem(self.outer - o + self.no, self.no) * 2 + self.core

    def mate_from(self, o):
        return lax.rem(self.outer - o + self.no, self.no) * 2 + 1 - self.core

    def mate_to(self, o):
        return lax.rem(self.outer + o, self.no) * 2 + 1 - self.core

    def greet(self, everyone=False):
        barrier = pltpu.get_barrier_semaphore()
        peers = [{"context": self.z_to(d)} for d in range(1, self.nz)]
        if everyone:
            peers += [{"shard": lax.rem(self.s + k, self.ns)} for k in range(1, self.ns)]
        else:
            peers += [{"shard": self.s_to(o)} for o in range(1, self.no)] + [{"shard": self.mate}]
        peers += [{"tensor": self.twin}]
        for peer in peers:
            pl.semaphore_signal(barrier, inc=1, device_id=peer, device_id_type=MESH)
        pl.semaphore_wait(barrier, len(peers))


class Sends:
    def __init__(self):
        self.remote, self.local = [], []

    def go(self, src, dst, send, recv, only=None, **peer):
        copy = pltpu.make_async_remote_copy(
            src_ref=src, dst_ref=dst, send_sem=send, recv_sem=recv,
            device_id=peer, device_id_type=MESH,
        )
        guarded(only, copy.start)
        self.remote.append((only, copy.wait_send))

    def here(self, src, dst, sem):
        copy = pltpu.make_async_copy(src, dst, sem)
        copy.start()
        self.local.append(copy)

    def drain(self):
        for only, wait in self.remote:
            guarded(only, wait)
        for copy in self.local:
            copy.wait()
        self.remote, self.local = [], []


def guarded(only, action):
    if only is None:
        action()
    else:
        pl.when(only)(action)


def landed(ref, send, recv, only=None, **peer):
    copy = pltpu.make_async_remote_copy(
        src_ref=ref, dst_ref=ref, send_sem=send, recv_sem=recv,
        device_id=peer, device_id_type=MESH,
    )
    guarded(only, copy.wait_recv)


def far_first(n):
    return [n - 1 - i // 2 if i % 2 == 0 else i // 2 for i in range(n)]


class Chain:
    def __init__(self, at, sends, ref, sems):
        self.at, self.sends, self.ref = at, sends, ref
        self.zs, self.zr = sems

    @staticmethod
    def sems(nz):
        dma = pltpu.SemaphoreType.DMA
        return [dma((2, nz)), dma((nz,))]

    def hops(self, steps=None):
        at = self.at
        for k in steps or range(1, at.nz):
            yield (-1, at.z - k >= 0, at.z - k)
            yield (1, at.z + k < at.nz, at.z + k)

    def hand(self, way, origin, src, only):
        at = self.at
        there = at.z + 1 < at.nz if way == 0 else at.z > 0
        self.sends.go(
            src, self.ref(origin), self.zs.at[way, origin], self.zr.at[origin],
            only=there if only is None else there & only, context=at.z + (1 if way == 0 else -1),
        )

    def begin(self, src):
        for way in range(2):
            self.hand(way, self.at.z, src, None)

    def step(self, side, valid, origin):
        ref = self.ref(origin)
        landed(ref, self.zs.at[0, origin], self.zr.at[origin], only=valid, context=self.at.z)
        self.hand(0 if side < 0 else 1, origin, ref, valid)
        return ref


class ChainSum:
    def __init__(self, at, sends, bufs, sems):
        self.at, self.sends = at, sends
        stage, self.land = bufs
        self.stage = stage if callable(stage) else lambda z2: stage.at[z2]
        self.zs, self.zr = sems

    @staticmethod
    def sems(nz):
        dma = pltpu.SemaphoreType.DMA
        return [dma((nz,)), dma((nz + 1,))]

    @staticmethod
    def bufs(nz, shape, dtype=BF16):
        return [pltpu.VMEM((nz, *shape), dtype), pltpu.VMEM((nz + 1, *shape), dtype)]

    def put(self, z2, own):
        at = self.at
        stage, dtype = self.stage(z2), self.land.dtype

        def start(slot, before):
            slot_ref = self.land.at[z2]

            @pl.when(before)
            def _():
                landed(slot_ref, self.zs.at[z2], self.zr.at[z2], context=at.z)
                stage[...] = (own() + self.land[z2].astype(F32)).astype(dtype)

            @pl.when(jnp.logical_not(before))
            def _():
                stage[...] = own().astype(dtype)

            pltpu.make_async_remote_copy(
                src_ref=stage, dst_ref=self.land.at[slot], send_sem=self.zs.at[z2],
                recv_sem=self.zr.at[slot], device_id={"context": at.z + (1 if z2_right else -1)},
                device_id_type=MESH,
            ).start()

        for z2_right in (True, False):
            away = at.z < z2 if z2_right else at.z > z2

            @pl.when(away)
            def _(z2_right=z2_right):
                near = at.z + 1 == z2 if z2_right else at.z - 1 == z2
                slot = z2 if z2_right else z2 + near * (at.nz - z2)
                before = at.z > 0 if z2_right else at.z + 1 < at.nz
                start(slot, before)

        self.sends.remote.append((
            at.z != z2,
            lambda: pltpu.make_async_remote_copy(
                src_ref=stage, dst_ref=self.land.at[z2], send_sem=self.zs.at[z2],
                recv_sem=self.zr.at[z2], device_id={"context": at.z}, device_id_type=MESH,
            ).wait_send(),
        ))

    def total(self, own):
        at = self.at
        total = own
        for slot, there in ((at.z, at.z > 0), (at.nz, at.z + 1 < at.nz)):
            landed(self.land.at[slot], self.zs.at[0], self.zr.at[slot], only=there, context=at.z)
            total = total + jnp.where(there, self.land[slot].astype(F32), 0.0)
        return total


class Spread:
    def __init__(self, at, sends, src, dst, sems, same=False):
        self.at, self.sends, self.src, self.dst = at, sends, src, dst
        self.copy = None
        self.own, self.zs, self.zr, self.xs, self.xr, self.cs, self.cr, *chain = sems
        self.chain = Chain(at, sends, lambda z1: dst(at.s, z1), chain) if same else None

    @staticmethod
    def sems(ns, nz):
        dma, no = pltpu.SemaphoreType.DMA, ns // 2
        return [
            dma, dma((nz,)), dma((nz,)), dma((nz, no)), dma((nz, no)), dma((no, nz)), dma((no, nz)),
        ] + Chain.sems(nz)

    def over_z(self):
        at = self.at
        if self.chain is not None:
            self.chain.begin(self.src(at.z))
            return
        for d in range(1, at.nz):
            z2 = at.z_to(d)
            self.sends.go(
                self.src(z2), self.dst(at.s, at.z), self.zs.at[z2], self.zr.at[at.z], context=z2
            )

    def over_s(self, z1, ref, only=None):
        at = self.at
        for o in range(1, at.no):
            self.sends.go(
                ref, self.dst(at.s, z1), self.xs.at[z1, o], self.xr.at[z1, o], only=only,
                shard=at.s_to(o),
            )
        self.sends.go(
            ref, self.dst(at.s, z1), self.cs.at[0, z1], self.cr.at[0, z1], only=only, shard=at.mate
        )

    def own_block(self):
        at = self.at
        self.over_s(at.z, self.src(at.z))
        self.copy = pltpu.make_async_copy(self.src(at.z), self.dst(at.s, at.z), self.own)
        self.copy.start()

    def pass_z(self):
        at = self.at
        if self.chain is not None:
            for side, valid, z1 in self.chain.hops():
                self.over_s(z1, self.chain.step(side, valid, z1), only=valid)
            return
        for d in range(1, at.nz):
            z1 = at.z_from(d)
            ref = self.dst(at.s, z1)
            landed(ref, self.zs.at[z1], self.zr.at[z1], context=z1)
            self.over_s(z1, ref)

    def pass_s(self):
        at = self.at
        for o in range(1, at.no):
            s1 = at.s_from(o)
            for d in range(at.nz):
                z1 = at.z_from(d)
                ref = self.dst(s1, z1)
                landed(ref, self.xs.at[z1, o], self.xr.at[z1, o], shard=s1)
                self.sends.go(ref, ref, self.cs.at[o, z1], self.cr.at[o, z1], shard=at.mate)

    def finish(self):
        at = self.at
        self.copy.wait()
        for o in range(at.no):
            for z1 in range(at.nz):
                ref = self.dst(at.mate_from(o), z1)
                landed(ref, self.cs.at[o, z1], self.cr.at[o, z1], shard=at.mate)

    def pass_all(self):
        self.pass_z()
        self.pass_s()


class Tokens:
    def __init__(self, at, sends, ref, sems):
        self.at, self.sends, self.ref = at, sends, ref
        self.ys, self.yr, *chain = sems
        self.chain = Chain(at, sends, lambda z1: ref.at[z1, at.y], chain)

    @staticmethod
    def sems(nz):
        dma = pltpu.SemaphoreType.DMA
        return [dma((nz,)), dma((nz,))] + Chain.sems(nz)

    def over_z(self, src):
        self.chain.begin(src)

    def over_y(self, z1, src, only=None):
        at = self.at
        self.sends.go(
            src, self.ref.at[z1, at.y], self.ys.at[z1], self.yr.at[z1], only=only, tensor=at.twin
        )

    def pass_z(self, steps=None):
        for side, valid, z1 in self.chain.hops(steps):
            self.over_y(z1, self.chain.step(side, valid, z1), only=valid)

    def wait_y(self, places, only=None):
        at = self.at
        for z1 in places:
            ref = self.ref.at[z1, at.twin]
            landed(
                ref, self.ys.at[z1], self.yr.at[z1], only=only and only(z1), tensor=at.twin
            )


def whole_lines(small, blocks, depth):
    tiles = []
    for t in range(blocks * depth // LANES):
        tile = jnp.zeros((8, LANES), F32)
        lane = lax.broadcasted_iota(jnp.int32, (8, LANES), 1) + t * LANES
        for b in range(t * LANES // depth, min(blocks, -(-(t + 1) * LANES // depth))):
            line = small[b, :8, :].astype(F32)
            shift = (b * depth - t * LANES) % LANES
            moved = pltpu.roll(line, shift, 1) if shift else line
            tile = jnp.where((lane >= b * depth) & (lane < (b + 1) * depth), moved, tile)
        tiles.append(tile)
    return jnp.concatenate(tiles, axis=1)


def turn_first(left, right):
    return lax.dot_general(left, right, (((0,), (0,)), ((), ())), preferred_element_type=F32)


def turn_last(left, right):
    return lax.dot_general(left, right, (((1,), (1,)), ((), ())), preferred_element_type=F32)


class Return:
    def __init__(self, at, sends, make, room, lands, out, sems):
        self.at, self.sends, self.make, self.out = at, sends, make, out
        self.stage, self.acc = room.at[pl.ds(0, at.no)], room.at[pl.ds(at.no, at.no)]
        self.landc, self.landx = lands
        self.cs, self.cr, self.xs, self.xr, self.zs, self.zr, self.own = sems
        self.chain = None
        self.depth = self.acc.shape[1] // at.nz
        self.copy = None

    @staticmethod
    def sems(ns, nz):
        dma, no = pltpu.SemaphoreType.DMA, ns // 2
        return [
            dma((no,)), dma((no,)), dma((no, nz)), dma((no, nz)), dma((nz,)), dma((nz,)), dma,
        ]

    @staticmethod
    def lands(ns, nz, depth, cols):
        no = ns // 2
        return [pltpu.VMEM((n, nz * depth, cols), BF16) for n in (no, no - 1)]

    def give(self, o):
        at = self.at
        self.stage[o] = self.make(at.mate_to(o)).astype(BF16)
        self.sends.go(
            self.stage.at[o], self.landc.at[o], self.cs.at[o], self.cr.at[o], shard=at.mate
        )
        self.acc[o] = self.make(at.s_to(o)).astype(BF16)

    def give_all(self):
        for o in (*range(1, self.at.no), 0):
            self.give(o)

    def rows(self, z2):
        start = z2 * self.depth
        start = start if isinstance(start, int) else pl.multiple_of(start, SUBLANES)
        return pl.ds(start, self.depth)

    def piece(self, z2):
        return self.acc.at[0, self.rows(z2)]

    def order(self):
        at = self.at
        if self.chain is not None:
            return far_first(at.nz)
        return [at.z_to(d) for d in range(1, at.nz)] + [at.z]

    def add(self, o, z2, others):
        line = self.rows(z2)
        total = self.acc[o, line, :].astype(F32)
        for other, k in others:
            total = total + other[k, line, :].astype(F32)
        self.acc[o, line, :] = total.astype(BF16)

    def over_s(self):
        at = self.at
        for o in range(1, at.no):
            landed(self.landc.at[o], self.cs.at[o], self.cr.at[o], shard=at.mate)
            for z2 in self.order():
                self.add(o, z2, [(self.landc, o)])
                line = self.rows(z2)
                self.sends.go(
                    self.acc.at[o, line], self.landx.at[o - 1, line], self.xs.at[o, z2],
                    self.xr.at[o, z2], shard=at.s_to(o),
                )
        landed(self.landc.at[0], self.cs.at[0], self.cr.at[0], shard=at.mate)

    def over_z(self, i):
        at = self.at
        z2 = self.order()[i]
        line = self.rows(z2)
        for o in range(1, at.no):
            landed(self.landx.at[o - 1, line], self.xs.at[o, z2], self.xr.at[o, z2], shard=at.s_from(o))
        self.add(0, z2, [(self.landc, 0)] + [(self.landx, o - 1) for o in range(1, at.no)])
        if self.chain is not None:
            self.chain.put(z2, lambda: self.piece(z2)[...].astype(F32))
        elif i + 1 < at.nz:
            self.sends.go(
                self.piece(z2), self.out(at.z), self.zs.at[z2], self.zr.at[at.z], context=z2
            )
        else:
            self.copy = pltpu.make_async_copy(self.piece(z2), self.out(z2), self.own)
            self.copy.start()

    def over_z_all(self):
        for i in range(self.at.nz):
            self.over_z(i)

    def finish(self):
        at = self.at
        self.copy.wait()
        for d in range(1, at.nz):
            z1 = at.z_from(d)
            landed(self.out(z1), self.zs.at[z1], self.zr.at[z1], context=z1)


class Reduce:
    def __init__(self, at, sends, parts, bufs, sems):
        self.at, self.sends, self.parts = at, sends, parts
        self.landy, *chain = bufs
        self.ys, self.yr, *chain_sems = sems
        self.chain = ChainSum(at, sends, chain, chain_sems)

    @staticmethod
    def sems(nz):
        dma = pltpu.SemaphoreType.DMA
        return [dma((nz,)), dma((nz,))] + ChainSum.sems(nz)

    @staticmethod
    def bufs(nz, half, width):
        return [pltpu.VMEM((nz, half, width), BF16)] + ChainSum.bufs(nz, (half, width))

    def over_y(self, places):
        at = self.at
        for z2 in places:
            self.sends.go(
                self.parts.at[z2, at.twin], self.landy.at[z2], self.ys.at[z2], self.yr.at[z2],
                tensor=at.twin,
            )

    def own(self, z2):
        return self.parts[z2, self.at.y].astype(F32) + self.landy[z2].astype(F32)

    def pass_y(self):
        at = self.at
        for z2 in far_first(at.nz):
            landed(self.landy.at[z2], self.ys.at[z2], self.yr.at[z2], tensor=at.twin)
            self.chain.put(z2, lambda z2=z2: self.own(z2))

    def total(self):
        return self.chain.total(self.own(self.at.z))


def piece_of_lines(lines, b, depth):
    first, off = divmod(b * depth, LANES)
    tile = lines[:, first * LANES:(first + 1) * LANES]
    if not off:
        return tile
    tile = pltpu.roll(tile, LANES - off, 1)
    if off + depth <= LANES:
        return tile
    after = pltpu.roll(lines[:, (first + 1) * LANES:(first + 2) * LANES], LANES - off, 1)
    lane = lax.broadcasted_iota(jnp.int32, (8, LANES), 1)
    return jnp.where(lane < LANES - off, tile, after)


class Refs:
    def __init__(self, refs):
        self.refs, self.next = refs, 0

    def take(self, n):
        self.next += n
        return self.refs[self.next - n:self.next]


def layer_kernel(ns, nz, heads, kv, *refs):
    refs = Refs(refs)
    (wa_in, small_in, gate_in, up_in, down_in, hidden, cot_in, cosine, sine, mask) = refs.take(10)
    (block_out, input_grad, qkv_grad, out_grad, small_out, *ffn_out) = refs.take(8)
    at = Place(ns, nz)
    w_sends, sends = Sends(), Sends()
    depth = wa_in.shape[0]
    rows, width = hidden.shape
    half = rows // 2
    group_rows = nz * rows
    q_cols = heads * HD
    qkv_cols = q_cols + 2 * kv * HD
    wide = nz * depth
    scale = HD ** (-0.5)
    repeat = heads // kv

    wa, gate_w, up_w, down_w = refs.take(4)
    n_spread, n_tokens, n_ret = len(Spread.sems(ns, nz)), len(Tokens.sems(nz)), len(Return.sems(ns, nz))
    n_red, n_sum = len(Reduce.sems(nz)), len(ChainSum.sems(nz))
    (small, ypart, yland, n2, cot, resid, query, kv_all, probs, attn) = refs.take(10)

    def block(ref):
        return lambda s1, z1: ref.at[s1, pl.ds(pl.multiple_of(z1 * depth, SUBLANES), depth)]

    w_attn = Spread(at, w_sends, lambda z2: wa_in, block(wa), refs.take(n_spread), True)
    w_small = Spread(
        at, w_sends, lambda z2: small_in, lambda s1, z1: small.at[s1 * nz + z1],
        refs.take(n_spread), True,
    )
    ffn = [
        Spread(at, w_sends, lambda z2, src=src: src.at[z2], block(dst), refs.take(n_spread))
        for src, dst in ((gate_in, gate_w), (up_in, up_w), (down_in, down_w))
    ]
    t_cot = Tokens(at, sends, cot, refs.take(n_tokens))
    t_n2 = Tokens(at, sends, n2, refs.take(n_tokens))
    kvs, kvr, yps, ypr, cot_sem = refs.take(5)
    gate, up_val, d_act, act, d_gate, d_up, ffn_part, dn2_part = refs.take(8)
    normed1_b, d_resid_b, d_projb = refs.take(3)

    def columns(ref, s1):
        return ref[..., pl.ds(pl.multiple_of(s1 * wide, LANES), wide)].reshape(-1, wide)

    def out_place(ref):
        unit = ref.shape[1] // nz
        return lambda z1: ref.at[:, pl.ds(pl.multiple_of(z1 * unit, LANES), unit)]

    makers = (
        lambda s1: turn_first(columns(n2, s1), d_gate[...]),
        lambda s1: turn_first(columns(n2, s1), d_up[...]),
        lambda s1: turn_first(columns(cot, s1), act[...]),
    )
    rets = [
        Return(at, sends, makers[i], room, refs.take(2), out_place(ffn_out[i]), refs.take(n_ret))
        for i, room in enumerate((gate_w, up_w, down_w))
    ]

    def summed(make, first, cols):
        room = wa.at[:, :, pl.ds(first, cols)]
        ret = Return(at, sends, make, room, refs.take(2), None, refs.take(n_ret))
        (land,) = refs.take(1)
        ret.chain = ChainSum(at, sends, (ret.piece, land), refs.take(n_sum))
        return ret

    r_qkv = summed(lambda s1: turn_first(columns(normed1_b, s1), d_projb[...]), 0, qkv_cols)
    r_out = summed(lambda s1: turn_first(columns(d_resid_b, s1), attn[...]), qkv_cols, q_cols)
    r_dn2, r_ffn = (
        Reduce(at, sends, parts, refs.take(3), refs.take(n_red)) for parts in (dn2_part, ffn_part)
    )
    (d_resid_f, d_attn, d_score, dkv, dkv_land, dn1_part, dn1_land, small_b, small_land, small_z,
     small_zland, small_y, small_yland, dkvs, dkvr, shs, shr, szs, szr, ysems, yrecv) = refs.take(21)

    at.greet(everyone=True)
    w_small.over_z()
    w_small.own_block()
    w_attn.over_z()
    w_attn.own_block()
    my_half = cot_in.at[pl.ds(pl.multiple_of(at.y * half, SUBLANES), half)]
    sends.here(cot_in.at[pl.ds(0, half)], cot.at[at.z, 0], cot_sem.at[0])
    sends.here(cot_in.at[pl.ds(half, half)], cot.at[at.z, 1], cot_sem.at[1])
    w_small.pass_z()
    w_attn.pass_z()
    ffn[0].over_z()
    for item in ffn:
        item.own_block()

    hidden_f = hidden[...].astype(F32)
    factor1 = lax.rsqrt(jnp.mean(hidden_f * hidden_f, axis=1, keepdims=True) + EPSILON)
    w_small.pass_s()
    w_attn.pass_s()
    w_small.finish()
    gains = whole_lines(small, ns * nz, depth)
    normed1_b[...] = (hidden[...].astype(F32) * factor1 * gains[0:1, :]).astype(BF16)
    width_each = HD // (ns * nz)
    lane = lax.broadcasted_iota(jnp.int32, (8, LANES), 1)
    bias = jnp.zeros((8, LANES), F32)
    for b in range(ns * nz):
        line = small[b, 8:16, :].astype(F32)
        moved = pltpu.roll(line, b * width_each, 1) if b else line
        bias = jnp.where((lane >= b * width_each) & (lane < (b + 1) * width_each), moved, bias)
    w_attn.finish()
    cos_t, sin_t = cosine[...], sine[...]

    def projected(head):
        weight = wa[:, :, head * HD:(head + 1) * HD].reshape(width, HD)
        return jnp.dot(normed1_b[...], weight, preferred_element_type=F32) + bias[head:head + 1, :]

    def rotated(values):
        return values * cos_t + pltpu.roll(values, HD // 2, 1) * sin_t

    for j in range(kv):
        kv_all[at.z, :, j * HD:(j + 1) * HD] = rotated(projected(heads + j)).astype(BF16)
        kv_all[at.z, :, (kv + j) * HD:(kv + j + 1) * HD] = projected(heads + kv + j).astype(BF16)
    for d in range(1, nz):
        z2 = at.z_to(d)
        sends.go(kv_all.at[at.z], kv_all.at[at.z], kvs.at[z2], kvr.at[at.z], context=z2)
    ffn[1].over_z()
    ffn[2].over_z()
    t_cot.over_z(my_half)
    for h in range(heads):
        query[:, h * HD:(h + 1) * HD] = rotated(projected(h)).astype(BF16)
    ffn[0].pass_z()
    for d in range(1, nz):
        z1 = at.z_from(d)
        landed(kv_all.at[z1], kvs.at[z1], kvr.at[z1], context=z1)

    def keys_of(j):
        return kv_all[:, :, j * HD:(j + 1) * HD].reshape(group_rows, HD)

    keep = mask[...] > 0
    for h in range(heads):
        keys, values = keys_of(h // repeat), keys_of(kv + h // repeat)
        scores = turn_last(query[:, h * HD:(h + 1) * HD], keys)
        scores = jnp.where(keep, scores * scale, -1e30)
        peak = jnp.max(scores, axis=1, keepdims=True)
        lse = peak + jnp.log(jnp.sum(jnp.exp(scores - peak), axis=1, keepdims=True))
        p = jnp.exp(scores - lse)
        probs[h * rows:(h + 1) * rows, :] = p
        out = jnp.dot(p.astype(BF16), values, preferred_element_type=F32)
        attn[:, h * HD:(h + 1) * HD] = out.astype(BF16)
    out_w = wa[:, :, qkv_cols:qkv_cols + q_cols].reshape(width, q_cols)
    part = turn_last(attn[...], out_w).astype(BF16)
    ypart[0] = part[:half]
    ypart[1] = part[half:]
    sends.go(ypart.at[at.twin], yland, yps, ypr, tensor=at.twin)
    ffn[0].pass_s()

    landed(yland, yps, ypr, tensor=at.twin)
    base = pl.multiple_of(at.y * half, SUBLANES)
    total = ypart[at.y].astype(F32) + yland[...].astype(F32)
    res = hidden[pl.ds(base, half), :].astype(F32) + total
    resid[...] = res
    factor2 = lax.rsqrt(jnp.mean(res * res, axis=1, keepdims=True) + EPSILON)
    n2[at.z, at.y] = (res * factor2 * gains[1:2, :]).astype(BF16)
    t_n2.over_z(n2.at[at.z, at.y])
    t_n2.over_y(at.z, n2.at[at.z, at.y])
    ffn[1].pass_z()
    ffn[1].pass_s()
    ffn[2].pass_z()
    t_cot.pass_z()
    t_n2.pass_z()
    ffn[2].pass_s()
    t_cot.wait_y(range(nz), lambda z1: at.z != z1)
    for item in ffn:
        item.finish()
    for copy in sends.local:
        copy.wait()
    sends.local = []

    def weight(ref):
        return ref[...].reshape(width, -1)

    d_act[...] = jnp.dot(cot[...].reshape(group_rows, width), weight(down_w), preferred_element_type=F32)
    few, tall = nz // 2, 32
    chunk = few * rows

    def half_block(first):
        t_n2.wait_y([first * few + i for i in range(few)])
        start = pl.multiple_of(first * chunk, chunk)
        mine = n2[pl.ds(first * few, few)].reshape(chunk, width)
        gate[...] = jnp.dot(mine, weight(gate_w), preferred_element_type=F32)
        up_val[...] = jnp.dot(mine, weight(up_w), preferred_element_type=F32)

        @pl.loop(0, chunk // tall)
        def _(i):
            line = pl.ds(pl.multiple_of(i * tall, tall), tall)
            whole = pl.ds(pl.multiple_of(start + i * tall, tall), tall)
            g, u, d = gate[line, :], up_val[line, :], d_act[whole, :]
            sigma = jax.nn.sigmoid(g)
            silu_val = g * sigma
            act[whole, :] = (silu_val * u).astype(BF16)
            d_gate[whole, :] = (d * u * sigma * (1.0 + g * (1.0 - sigma))).astype(BF16)
            d_up[whole, :] = (d * silu_val).astype(BF16)

        span = pl.ds(start, chunk)
        dn2_part[pl.ds(first * few, few)] = (
            turn_last(d_gate[span, :], weight(gate_w)) + turn_last(d_up[span, :], weight(up_w))
        ).astype(BF16).reshape(few, 2, half, width)
        r_dn2.over_y([first * few + i for i in range(few)])

    nearer = lax.div(at.z, few)
    half_block(nearer)
    half_block(1 - nearer)
    w_sends.drain()

    rets[0].give_all()
    rets[0].over_s()
    r_dn2.pass_y()
    rets[1].give_all()
    rets[1].over_s()
    res = resid[...]
    factor2 = lax.rsqrt(jnp.mean(res * res, axis=1, keepdims=True) + EPSILON)
    unit2 = res * factor2
    dn2 = r_dn2.total()
    grad_g2 = jnp.sum(dn2 * unit2, axis=0, keepdims=True)
    scaled = dn2 * gains[1:2, :]
    back2 = factor2 * (scaled - unit2 * jnp.mean(scaled * unit2, axis=1, keepdims=True))
    d_res = cot[at.z, at.y].astype(F32) + back2
    d_resid_f[at.y] = d_res
    d_resid_b[at.y] = d_res.astype(BF16)
    mine_b, mine_f = d_resid_b.at[at.y], d_resid_f.at[at.y]
    sends.go(mine_b, mine_b, ysems.at[0], yrecv.at[0], tensor=at.twin)
    ffn_part[...] = turn_last(act[...], weight(down_w)).astype(BF16).reshape(nz, 2, half, width)
    rets[2].give_all()
    rets[0].over_z_all()
    landed(d_resid_b.at[at.twin], ysems.at[0], yrecv.at[0], tensor=at.twin)
    r_ffn.over_y(far_first(nz))
    sends.go(mine_f, mine_f, ysems.at[1], yrecv.at[1], tensor=at.twin)

    d_resid_all = d_resid_b[...].reshape(rows, width)
    out_w = wa[:, :, qkv_cols:qkv_cols + q_cols].reshape(width, q_cols)
    d_attn[...] = jnp.dot(d_resid_all, out_w, preferred_element_type=F32).astype(BF16)
    r_out.give_all()
    r_out.over_s()

    def unrotated(values):
        return values * cos_t - pltpu.roll(values, HD // 2, 1) * sin_t

    bias_rows = [None] * (heads + 2 * kv)

    def place(head, grad):
        bias_rows[head] = jnp.sum(grad, axis=0, keepdims=True)
        d_projb[:, head * HD:(head + 1) * HD] = grad.astype(BF16)

    for j in range(kv):
        keys, values = keys_of(j), keys_of(kv + j)
        d_values = jnp.zeros((group_rows, HD), F32)
        d_keys = jnp.zeros((group_rows, HD), F32)
        for h in range(j * repeat, (j + 1) * repeat):
            d_out = d_attn[:, h * HD:(h + 1) * HD]
            p = probs[h * rows:(h + 1) * rows, :]
            d_prob = turn_last(d_out, values)
            delta = jnp.sum(
                d_out.astype(F32) * attn[:, h * HD:(h + 1) * HD].astype(F32), axis=1, keepdims=True
            )
            d_score[...] = (p * (d_prob - delta)).astype(BF16)
            d_query = jnp.dot(d_score[...], keys, preferred_element_type=F32)
            place(h, unrotated(d_query * scale))
            d_keys = d_keys + turn_first(d_score[...], query[:, h * HD:(h + 1) * HD])
            d_values = d_values + turn_first(p.astype(BF16), d_out)
        for i, grad in ((j, d_keys * scale), (kv + j, d_values)):
            dkv[:, :, i * HD:(i + 1) * HD] = grad.astype(BF16).reshape(nz, rows, HD)
    for d in range(1, nz):
        z2 = at.z_to(d)
        sends.go(dkv.at[z2], dkv_land.at[at.z], dkvs.at[z2], dkvr.at[at.z], context=z2)
    rets[1].over_z_all()
    d_own = dkv[at.z].astype(F32)
    for d in range(1, nz):
        z1 = at.z_from(d)
        landed(dkv_land.at[z1], dkvs.at[z1], dkvr.at[z1], context=z1)
        d_own = d_own + dkv_land[z1].astype(F32)
    for j in range(kv):
        place(heads + j, unrotated(d_own[:, j * HD:(j + 1) * HD]))
        place(heads + kv + j, d_own[:, (kv + j) * HD:(kv + j + 1) * HD])
    qkv_w = wa[:, :, :qkv_cols].reshape(width, qkv_cols)
    dn1_part[...] = turn_last(d_projb[...], qkv_w).astype(BF16)
    sends.go(dn1_part, dn1_land, ysems.at[2], yrecv.at[2], tensor=at.twin)
    r_qkv.give_all()
    r_qkv.over_s()
    rets[2].over_s()
    r_ffn.pass_y()
    r_out.over_z_all()

    block_out[at.y] = (r_ffn.total() + resid[...]).astype(BF16)
    sends.go(block_out.at[at.y], block_out.at[at.y], ysems.at[3], yrecv.at[3], tensor=at.twin)

    landed(dn1_land, ysems.at[2], yrecv.at[2], tensor=at.twin)
    landed(d_resid_f.at[at.twin], ysems.at[1], yrecv.at[1], tensor=at.twin)
    dn1 = dn1_part[...].astype(F32) + dn1_land[...].astype(F32)
    hidden_f = hidden[...].astype(F32)
    factor1 = lax.rsqrt(jnp.mean(hidden_f * hidden_f, axis=1, keepdims=True) + EPSILON)
    unit1 = hidden_f * factor1
    row = lax.broadcasted_iota(jnp.int32, (rows, 1), 0)
    my_row = (row >= at.y * half) & (row < (at.y + 1) * half)
    grad_g1 = jnp.sum(jnp.where(my_row, dn1 * unit1, 0.0), axis=0, keepdims=True)
    scaled = dn1 * gains[0:1, :]
    back1 = factor1 * (scaled - unit1 * jnp.mean(scaled * unit1, axis=1, keepdims=True))
    input_grad[...] = d_resid_f[...].reshape(rows, width) + back1

    both = jnp.concatenate([grad_g1, grad_g2, jnp.zeros((6, width), F32)], axis=0)
    bias = jnp.concatenate(bias_rows, axis=0)
    for b in range(ns * nz):
        moved = pltpu.roll(bias, LANES - b * width_each, 1) if b else bias
        small_b[b // nz, b % nz] = jnp.concatenate([piece_of_lines(both, b, depth), moved], axis=0)
    for k in range(1, ns):
        s2 = lax.rem(at.s + k, ns)
        sends.go(small_b.at[s2], small_land.at[k], shs.at[k], shr.at[k], shard=s2)
    r_qkv.over_z_all()
    total = small_b[at.s]
    for k in range(1, ns):
        s1 = lax.rem(at.s - k + ns, ns)
        landed(small_land.at[k], shs.at[k], shr.at[k], shard=s1)
        total = total + small_land[k]
    small_z[...] = total
    for d in range(1, nz):
        sends.go(small_z.at[at.z_to(d)], small_zland.at[d], szs.at[d], szr.at[d], context=at.z_to(d))
    rets[2].over_z_all()
    total = small_z[at.z]
    for d in range(1, nz):
        landed(small_zland.at[d], szs.at[d], szr.at[d], context=at.z_from(d))
        total = total + small_zland[d]
    small_y[...] = total
    sends.go(small_y, small_yland, ysems.at[4], yrecv.at[4], tensor=at.twin)
    out_grad[...] = r_out.chain.total(r_out.piece(at.z)[...].astype(F32))
    qkv_grad[...] = r_qkv.chain.total(r_qkv.piece(at.z)[...].astype(F32))
    landed(small_yland, ysems.at[4], yrecv.at[4], tensor=at.twin)
    small_out[:8, :] = small_y[:8, :] + small_yland[:8, :]
    small_out[8:, :] = small_y[8:, :]
    landed(block_out.at[at.twin], ysems.at[3], yrecv.at[3], tensor=at.twin)
    for ret in rets:
        ret.finish()
    sends.drain()


def layer(ns, nz, heads, kv, wa_in, small_in, ffn_in, hidden, cot, cosine, sine, mask):
    rows, width = hidden.shape
    owners, half, group_rows = ns * nz, rows // 2, nz * rows
    depth, cols = wa_in.shape
    unit = ffn_in[0].shape[2]
    q_cols, kv_cols = heads * HD, 2 * kv * HD
    qkv_cols = q_cols + kv_cols
    dma = pltpu.SemaphoreType.DMA
    shape = jax.ShapeDtypeStruct
    room = pltpu.VMEM
    vmem = pl.BlockSpec(memory_space=pltpu.VMEM)
    anyspace = pl.BlockSpec(memory_space=pl.ANY)
    scratch = [room((ns, nz * depth, cols), BF16)] + [room((ns, nz * depth, unit), BF16)] * 3
    scratch += [
        room((owners, 16, LANES), BF16),
        room((2, half, width), BF16),
        room((half, width), BF16),
        room((nz, 2, half, width), BF16),
        room((nz, 2, half, width), BF16),
        room((half, width), F32),
        room((rows, q_cols), BF16),
        room((nz, rows, kv_cols), BF16),
        room((heads * rows, group_rows), F32),
        room((rows, q_cols), BF16),
    ]
    scratch += Spread.sems(ns, nz) * 5 + Tokens.sems(nz) * 2
    scratch += [dma((nz,)), dma((nz,)), dma, dma, dma((2,))]
    scratch += [room((group_rows // 2, unit), F32)] * 2 + [room((group_rows, unit), F32)]
    scratch += [room((group_rows, unit), BF16)] * 3 + [room((nz, 2, half, width), BF16)] * 2
    scratch += [
        room((rows, width), BF16), room((2, half, width), BF16), room((rows, qkv_cols), BF16),
    ]
    for _ in range(3):
        scratch += Return.lands(ns, nz, depth, unit) + Return.sems(ns, nz)
    for n in (qkv_cols, q_cols):
        scratch += Return.lands(ns, nz, depth, n) + Return.sems(ns, nz)
        scratch += ChainSum.bufs(nz, (depth, n))[1:] + ChainSum.sems(nz)
    for _ in range(2):
        scratch += Reduce.bufs(nz, half, width) + Reduce.sems(nz)
    scratch += [
        room((2, half, width), F32),
        room((rows, q_cols), BF16),
        room((rows, group_rows), BF16),
        room((nz, rows, kv_cols), BF16),
        room((nz, rows, kv_cols), BF16),
        room((rows, width), BF16),
        room((rows, width), BF16),
        room((ns, nz, 16, LANES), F32),
        room((ns, nz, 16, LANES), F32),
        room((nz, 16, LANES), F32),
        room((nz, 16, LANES), F32),
        room((16, LANES), F32),
        room((16, LANES), F32),
        dma((nz,)), dma((nz,)), dma((ns,)), dma((ns,)), dma((nz,)), dma((nz,)), dma((5,)), dma((5,)),
    ]
    return pl.pallas_call(
        functools.partial(layer_kernel, ns, nz, heads, kv),
        out_shape=[
            shape((2, half, width), BF16),
            shape((rows, width), F32),
            shape((depth, qkv_cols), F32),
            shape((depth, q_cols), F32),
            shape((16, LANES), F32),
            *[shape((depth, nz * unit), BF16)] * 3,
        ],
        in_specs=[anyspace] * 5 + [vmem, anyspace] + [vmem] * 3,
        out_specs=[vmem] * 5 + [anyspace] * 3,
        scratch_shapes=scratch,
        compiler_params=pltpu.CompilerParams(
            collective_id=0, has_side_effects=True, vmem_limit_bytes=VMEM_BYTES
        ),
    )(wa_in, small_in, *ffn_in, hidden, cot, cosine, sine, mask)


def fast_step(
    ns,
    nz,
    hidden_in,
    segment_ids,
    attn_gain,
    qkv_weight,
    qkv_bias,
    out_weight,
    ffn_gain,
    gate_weight,
    up_weight,
    down_weight,
    out_cotangent,
):
    rows, width = hidden_in.shape
    depth, hidden_units = gate_weight.shape
    parts = 2
    heads = H // parts
    kv = KVH // parts
    block_index = lax.axis_index("context")
    unit_cols = -(-hidden_units // (nz * LANES)) * LANES
    padded = unit_cols * nz

    def by_place(weight):
        full = jnp.pad(weight, ((0, 0), (0, padded - hidden_units)))
        return jnp.transpose(full.reshape(depth, nz, unit_cols), (1, 0, 2))

    ffn_in = [by_place(w) for w in (gate_weight, up_weight, down_weight.T)]
    wa_in = jnp.concatenate([qkv_weight, out_weight.T], axis=1)
    gains_in = jnp.pad(jnp.stack([attn_gain, ffn_gain]), ((0, 6), (0, LANES - depth)))
    bias_in = jnp.pad(qkv_bias, ((0, 0), (0, LANES - qkv_bias.shape[1])))
    small_in = jnp.concatenate([gains_in, bias_in], axis=0)

    seg_all = segment_ids[0]
    group_rows = seg_all.shape[0]
    first_row = block_index * rows
    index_all = jnp.arange(group_rows, dtype=jnp.int32)
    seg_local = lax.dynamic_slice_in_dim(seg_all, first_row, rows)
    index_local = first_row + jnp.arange(rows, dtype=jnp.int32)
    earlier = jnp.sum((seg_all[None, :] < seg_local[:, None]).astype(jnp.int32), axis=1)
    allowed = (seg_local[:, None] == seg_all[None, :]) & (
        index_local[:, None] >= index_all[None, :]
    )
    cosine, sine = rotary_tables(index_local - earlier)

    block_out, input_grad, grad_qkv, grad_out, small, grad_gate, grad_up, grad_down = layer(
        ns, nz, heads, kv, wa_in, small_in, ffn_in, hidden_in, out_cotangent, cosine, sine,
        allowed.astype(F32),
    )

    def all_columns(grad):
        return grad[:, :hidden_units].astype(F32)

    return (
        block_out.reshape(rows, width),
        input_grad,
        small[0, :depth],
        grad_qkv,
        small[8:, : qkv_bias.shape[1]],
        grad_out.T,
        small[1, :depth],
        all_columns(grad_gate),
        all_columns(grad_up),
        all_columns(grad_down).T,
    )


def general_step(
    hidden_in,
    segment_ids,
    attn_gain,
    qkv_weight,
    qkv_bias,
    out_weight,
    ffn_gain,
    gate_weight,
    up_weight,
    down_weight,
    out_cotangent,
):
    rows, width = hidden_in.shape
    depth = gate_weight.shape[0]
    hidden_units = gate_weight.shape[1]
    parts = lax.axis_size("tensor")
    blocks = lax.axis_size("context")
    heads = H // parts
    kv = KVH // parts
    repeat = H // KVH
    scale = HD ** (-0.5)
    block_index = lax.axis_index("context")
    part_index = lax.axis_index("tensor")
    half_rows = rows // parts
    unit_cols = -(-hidden_units // (blocks * LANES)) * LANES
    padded = unit_cols * blocks

    def spread(weight):
        full = jnp.pad(weight, ((0, 0), (0, padded - hidden_units)))
        mine = lax.all_to_all(full, "context", split_axis=1, concat_axis=0, tiled=True)
        mine = mine.reshape(blocks * depth, unit_cols)
        return lax.all_gather(mine, "shard", axis=0, tiled=True)

    gate_full = spread(gate_weight)
    up_full = spread(up_weight)
    down_full = spread(down_weight.T)
    gain_one = lax.all_gather(attn_gain, OWNERS, axis=0, tiled=True).astype(F32)
    gain_two = lax.all_gather(ffn_gain, OWNERS, axis=0, tiled=True).astype(F32)
    bias = lax.all_gather(qkv_bias, OWNERS, axis=1, tiled=True).reshape(-1).astype(F32)
    qkv_full = lax.all_gather(qkv_weight, OWNERS, axis=0, tiled=True)
    out_full = lax.all_gather(out_weight.T, OWNERS, axis=0, tiled=True)

    seg_all = segment_ids[0]
    group_rows = seg_all.shape[0]
    first_row = block_index * rows
    index_all = jnp.arange(group_rows, dtype=jnp.int32)
    earlier = jnp.sum((seg_all[None, :] < seg_all[:, None]).astype(jnp.int32), axis=1)
    positions = index_all - earlier
    seg_local = lax.dynamic_slice_in_dim(seg_all, first_row, rows)
    index_local = first_row + jnp.arange(rows, dtype=jnp.int32)
    allowed = (seg_local[:, None] == seg_all[None, :]) & (
        index_local[:, None] >= index_all[None, :]
    )
    cosine, sine = rotary_tables(positions)
    cos_local = lax.dynamic_slice_in_dim(cosine, first_row, rows)
    sin_local = lax.dynamic_slice_in_dim(sine, first_row, rows)

    hidden_all = lax.all_gather(hidden_in, "context", axis=0, tiled=True)
    normed_all, _, _ = norm_forward(hidden_all.astype(F32), gain_one)
    hidden_f = hidden_in.astype(F32)
    normed1, unit1, factor1 = norm_forward(hidden_f, gain_one)
    q_cols = heads * HD
    k_cols = kv * HD
    query_f = dot(normed1, qkv_full[:, :q_cols]) + bias[:q_cols]
    kv_f = dot(normed_all, qkv_full[:, q_cols:]) + bias[q_cols:]
    query = jnp.transpose(query_f.reshape(rows, heads, HD), (1, 0, 2))
    query = rotate(query, cos_local, sin_local).astype(BF16)
    keys = jnp.transpose(kv_f[:, :k_cols].reshape(group_rows, kv, HD), (1, 0, 2))
    keys = rotate(keys, cosine, sine).astype(BF16)
    values = jnp.transpose(kv_f[:, k_cols:].reshape(group_rows, kv, HD), (1, 0, 2)).astype(BF16)
    query = query.reshape(kv, repeat * rows, HD)
    mask = jnp.tile(allowed, (repeat, 1))
    scores = jnp.where(mask, batched(query, keys, 2, 2) * scale, -1e30)
    peak = jnp.max(scores, axis=2, keepdims=True)
    lse = peak + jnp.log(jnp.sum(jnp.exp(scores - peak), axis=2, keepdims=True))
    p_soft = jnp.exp(scores - lse)
    probs = p_soft.astype(BF16)
    outs = batched(probs, values, 2, 1).astype(BF16)
    attn = jnp.transpose(outs.reshape(heads, rows, HD), (1, 0, 2)).reshape(rows, q_cols)
    attn_part = contract_last(attn, out_full).astype(BF16)

    mine = part_index * half_rows
    attn_half = lax.psum_scatter(attn_part, "tensor", scatter_dimension=0, tiled=True)
    resid_half = lax.dynamic_slice_in_dim(hidden_f, mine, half_rows) + attn_half.astype(F32)
    normed2_half, unit2, factor2 = norm_forward(resid_half, gain_two)
    normed2 = lax.all_gather(normed2_half, TEAM, axis=0, tiled=True)
    cot_half = lax.dynamic_slice_in_dim(out_cotangent, mine, half_rows)
    cot = lax.all_gather(cot_half, TEAM, axis=0, tiled=True)

    gate = dot(normed2, gate_full)
    up_val = dot(normed2, up_full)
    sigma = jax.nn.sigmoid(gate)
    silu_val = gate * sigma
    act = (silu_val * up_val).astype(BF16)
    ffn_part = contract_last(act, down_full).astype(BF16)
    d_act = dot(cot, down_full)
    d_gate = (d_act * up_val * sigma * (1.0 + gate * (1.0 - sigma))).astype(BF16)
    d_up = (d_act * silu_val).astype(BF16)
    dn2_part = (contract_last(d_gate, gate_full) + contract_last(d_up, up_full)).astype(BF16)
    ffn_half = lax.psum_scatter(ffn_part, TEAM, scatter_dimension=0, tiled=True)
    block_half = (resid_half + ffn_half.astype(F32)).astype(BF16)
    block_out = lax.all_gather(block_half, "tensor", axis=0, tiled=True)
    dn2_half = lax.psum_scatter(dn2_part, TEAM, scatter_dimension=0, tiled=True).astype(F32)
    grad_g2, d_back2 = norm_backward(dn2_half, unit2, factor2, gain_two)
    d_resid_half = cot_half.astype(F32) + d_back2

    def give_back(grad):
        part = lax.psum_scatter(grad.astype(BF16), "shard", scatter_dimension=0, tiled=True)
        part = part.reshape(blocks, depth, unit_cols)
        part = lax.all_to_all(part, "context", split_axis=0, concat_axis=2, tiled=True)
        return part.reshape(depth, padded)[:, :hidden_units].astype(F32)

    sum_gate = give_back(contract_first(normed2, d_gate))
    sum_up = give_back(contract_first(normed2, d_up))
    sum_down = give_back(contract_first(cot, act)).T

    d_resid_b = lax.all_gather(d_resid_half.astype(BF16), "tensor", axis=0, tiled=True)
    grad_out = contract_first(d_resid_b, attn)
    d_attn = dot(d_resid_b, out_full).astype(BF16)
    d_outs = jnp.transpose(d_attn.reshape(rows, heads, HD), (1, 0, 2)).reshape(
        kv, repeat * rows, HD
    )
    d_prob = batched(d_outs, values, 2, 2)
    delta = jnp.sum(d_outs.astype(F32) * outs.astype(F32), axis=2, keepdims=True)
    d_score = (p_soft * (d_prob - delta)).astype(BF16)
    d_query = batched(d_score, keys, 2, 1) * scale
    d_keys = batched(d_score, query, 1, 1) * scale
    d_values = batched(probs, d_outs, 1, 1)
    d_kv = jnp.concatenate([d_keys, d_values], axis=0).astype(BF16)
    d_kv = lax.psum_scatter(d_kv, "context", scatter_dimension=1, tiled=True).astype(F32)
    d_query = unrotate(d_query.reshape(heads, rows, HD), cos_local, sin_local)
    d_keys = unrotate(d_kv[:kv], cos_local, sin_local)
    d_proj = jnp.transpose(jnp.concatenate([d_query, d_keys, d_kv[kv:]], axis=0), (1, 0, 2))
    grad_bias = jnp.sum(d_proj, axis=0)
    d_projb = d_proj.reshape(rows, -1).astype(BF16)
    grad_qkv = contract_first(normed1, d_projb)
    dn1_part = contract_last(d_projb, qkv_full).astype(BF16)
    dn1_half = lax.psum_scatter(dn1_part, "tensor", scatter_dimension=0, tiled=True).astype(F32)
    unit1_half = lax.dynamic_slice_in_dim(unit1, mine, half_rows)
    factor1_half = lax.dynamic_slice_in_dim(factor1, mine, half_rows)
    grad_g1, d_back1 = norm_backward(dn1_half, unit1_half, factor1_half, gain_one)
    input_grad = lax.all_gather(d_resid_half + d_back1, "tensor", axis=0, tiled=True)

    gains = lax.psum(jnp.stack([grad_g1, grad_g2]), "tensor")
    sum_gains = lax.psum_scatter(gains, OWNERS, scatter_dimension=1, tiled=True)
    sum_qkv = lax.psum_scatter(grad_qkv.astype(BF16), OWNERS, scatter_dimension=0, tiled=True)
    sum_bias = lax.psum_scatter(grad_bias, OWNERS, scatter_dimension=1, tiled=True)
    sum_out = lax.psum_scatter(grad_out.astype(BF16), OWNERS, scatter_dimension=0, tiled=True)
    return (
        block_out,
        input_grad,
        sum_gains[0],
        sum_qkv.astype(F32),
        sum_bias,
        sum_out.astype(F32).T,
        sum_gains[1],
        sum_gate,
        sum_up,
        sum_down,
    )


def solution(mesh):
    ns, nz, parts = (mesh.shape[a] for a in ("shard", "context", "tensor"))
    rows = P(OWNERS, None)

    def local(*args):
        depth = args[7].shape[0]
        if depth % SUBLANES == 0 and ns % 2 == 0 and ns > 2 and nz % 2 == 0 and parts == 2:
            return fast_step(ns, nz, *args)
        return general_step(*args)

    placed = (
        rows,
        P("shard", None),
        P(OWNERS),
        P(OWNERS, "tensor"),
        P("tensor", OWNERS),
        P("tensor", OWNERS),
        P(OWNERS),
        P(OWNERS, "tensor"),
        P(OWNERS, "tensor"),
        P("tensor", OWNERS),
        rows,
    )
    return jax.shard_map(
        local,
        mesh=mesh,
        in_specs=placed,
        out_specs=(
            rows,
            rows,
            P(OWNERS),
            P(OWNERS, "tensor"),
            P("tensor", OWNERS),
            P("tensor", OWNERS),
            P(OWNERS),
            P(OWNERS, "tensor"),
            P(OWNERS, "tensor"),
            P("tensor", OWNERS),
        ),
        check_vma=False,
    )
```

```python
import functools
import math

import jax
import jax.numpy as jnp
from jax import lax
from jax.experimental import pallas as pl
from jax.experimental.pallas import tpu as pltpu
from jax.sharding import PartitionSpec as P

H = 12
KVH = 2
HD = 128
LANES = 128
SUBLANES = 16
BF16 = jnp.bfloat16
F32 = jnp.float32

EPSILON = 1e-06
THETA = 1000000.0

OWNERS = ("shard", "context")
TEAM = ("context", "tensor")
MESH = pl.DeviceIdType.MESH
VMEM_BYTES = 62 * 1024 * 1024


def dot(left, right):
    return jnp.dot(left, right, preferred_element_type=F32)


def contract_last(left, right):
    return lax.dot_general(left, right, (((1,), (1,)), ((), ())), preferred_element_type=F32)


def contract_first(left, right):
    return lax.dot_general(left, right, (((0,), (0,)), ((), ())), preferred_element_type=F32)


def batched(left, right, left_dim, right_dim):
    return lax.dot_general(
        left, right, (((left_dim,), (right_dim,)), ((0,), (0,))), preferred_element_type=F32
    )


def norm_forward(values, gain):
    factor = lax.rsqrt(jnp.mean(values * values, axis=1, keepdims=True) + EPSILON)
    unit = values * factor
    return ((unit * gain).astype(BF16), unit, factor)


def norm_backward(grad_out, unit, factor, gain):
    gain_grad = jnp.sum(grad_out * unit, axis=0)
    scaled = grad_out * gain
    return (gain_grad, factor * (scaled - unit * jnp.mean(scaled * unit, axis=1, keepdims=True)))


def rotary_tables(positions):
    half = HD // 2
    freqs = THETA ** (-(2.0 * jnp.arange(half, dtype=F32)) / HD)
    angles = positions.astype(F32)[:, None] * freqs[None, :]
    cosine, sine = jnp.cos(angles), jnp.sin(angles)
    return (
        jnp.concatenate([cosine, cosine], axis=1),
        jnp.concatenate([-sine, sine], axis=1),
    )


def swap_halves(values):
    half = values.shape[-1] // 2
    return jnp.concatenate([values[..., half:], values[..., :half]], axis=-1)


def rotate(values, cosine, sine):
    return values * cosine + swap_halves(values) * sine


def unrotate(values, cosine, sine):
    return values * cosine - swap_halves(values) * sine


class Place:
    def __init__(self, ns, nz):
        self.ns, self.nz, self.no = ns, nz, ns // 2
        self.s, self.z, self.y = (lax.axis_index(a) for a in ("shard", "context", "tensor"))
        self.core = lax.rem(self.s, 2)
        self.outer = lax.div(self.s, 2)
        self.mate = self.s + 1 - 2 * self.core
        self.twin = 1 - self.y

    def z_to(self, d):
        return lax.rem(self.z + d, self.nz)

    def z_from(self, d):
        return lax.rem(self.z - d + self.nz, self.nz)

    def near(self):
        for k in range(1, self.nz):
            yield (self.z + k < self.nz, lax.rem(self.z + k, self.nz))
            yield (self.z >= k, lax.rem(self.z - k + self.nz, self.nz))

    def s_to(self, o):
        return lax.rem(self.outer + o, self.no) * 2 + self.core

    def s_from(self, o):
        return lax.rem(self.outer - o + self.no, self.no) * 2 + self.core

    def mate_from(self, o):
        return lax.rem(self.outer - o + self.no, self.no) * 2 + 1 - self.core

    def mate_to(self, o):
        return lax.rem(self.outer + o, self.no) * 2 + 1 - self.core

    def greet(self, everyone=False):
        barrier = pltpu.get_barrier_semaphore()
        peers = [{"context": self.z_to(d)} for d in range(1, self.nz)]
        if everyone:
            peers += [{"shard": lax.rem(self.s + k, self.ns)} for k in range(1, self.ns)]
        else:
            peers += [{"shard": self.s_to(o)} for o in range(1, self.no)] + [{"shard": self.mate}]
        peers += [{"tensor": self.twin}]
        for peer in peers:
            pl.semaphore_signal(barrier, inc=1, device_id=peer, device_id_type=MESH)
        pl.semaphore_wait(barrier, len(peers))


class Sends:
    def __init__(self):
        self.remote, self.local = [], []

    def go(self, src, dst, send, recv, only=None, **peer):
        copy = pltpu.make_async_remote_copy(
            src_ref=src, dst_ref=dst, send_sem=send, recv_sem=recv,
            device_id=peer, device_id_type=MESH,
        )
        guarded(only, copy.start)
        self.remote.append((only, copy.wait_send))

    def here(self, src, dst, sem):
        copy = pltpu.make_async_copy(src, dst, sem)
        copy.start()
        self.local.append(copy)

    def drain(self):
        for only, wait in self.remote:
            guarded(only, wait)
        for copy in self.local:
            copy.wait()
        self.remote, self.local = [], []


def both(one, other):
    return other if one is None else one & other


def guarded(only, action):
    if only is None:
        action()
    else:
        pl.when(only)(action)


def landed(ref, send, recv, only=None, **peer):
    copy = pltpu.make_async_remote_copy(
        src_ref=ref, dst_ref=ref, send_sem=send, recv_sem=recv,
        device_id=peer, device_id_type=MESH,
    )
    guarded(only, copy.wait_recv)


def far_first(n):
    return [n - 1 - i // 2 if i % 2 == 0 else i // 2 for i in range(n)]


class Chain:
    def __init__(self, at, sends, ref, sems):
        self.at, self.sends, self.ref = at, sends, ref
        self.zs, self.zr = sems

    @staticmethod
    def sems(nz):
        dma = pltpu.SemaphoreType.DMA
        return [dma((2, nz)), dma((nz,))]

    def hops(self, steps=None):
        at = self.at
        for k in steps or range(1, at.nz):
            yield (-1, at.z - k >= 0, at.z - k)
            yield (1, at.z + k < at.nz, at.z + k)

    def hand(self, way, origin, src, only):
        at = self.at
        there = at.z + 1 < at.nz if way == 0 else at.z > 0
        self.sends.go(
            src, self.ref(origin), self.zs.at[way, origin], self.zr.at[origin],
            only=there if only is None else there & only, context=at.z + (1 if way == 0 else -1),
        )

    def begin(self, src):
        for way in range(2):
            self.hand(way, self.at.z, src, None)

    def step(self, side, valid, origin):
        ref = self.ref(origin)
        landed(ref, self.zs.at[0, origin], self.zr.at[origin], only=valid, context=self.at.z)
        self.hand(0 if side < 0 else 1, origin, ref, valid)
        return ref


class ChainSum:
    def __init__(self, at, sends, bufs, sems):
        self.at, self.sends = at, sends
        stage, self.land = bufs
        self.stage = stage if callable(stage) else lambda z2: stage.at[z2]
        self.zs, self.zr = sems

    @staticmethod
    def sems(nz):
        dma = pltpu.SemaphoreType.DMA
        return [dma((nz,)), dma((nz + 1,))]

    @staticmethod
    def bufs(nz, shape, dtype=BF16):
        return [pltpu.VMEM((nz, *shape), dtype), pltpu.VMEM((nz + 1, *shape), dtype)]

    def put(self, z2, own):
        at = self.at
        stage, dtype = self.stage(z2), self.land.dtype

        def start(slot, before):
            slot_ref = self.land.at[z2]

            @pl.when(before)
            def _():
                landed(slot_ref, self.zs.at[z2], self.zr.at[z2], context=at.z)
                stage[...] = (own() + self.land[z2].astype(F32)).astype(dtype)

            @pl.when(jnp.logical_not(before))
            def _():
                stage[...] = own().astype(dtype)

            pltpu.make_async_remote_copy(
                src_ref=stage, dst_ref=self.land.at[slot], send_sem=self.zs.at[z2],
                recv_sem=self.zr.at[slot], device_id={"context": at.z + (1 if z2_right else -1)},
                device_id_type=MESH,
            ).start()

        for z2_right in (True, False):
            away = at.z < z2 if z2_right else at.z > z2

            @pl.when(away)
            def _(z2_right=z2_right):
                near = at.z + 1 == z2 if z2_right else at.z - 1 == z2
                slot = z2 if z2_right else z2 + near * (at.nz - z2)
                before = at.z > 0 if z2_right else at.z + 1 < at.nz
                start(slot, before)

        self.sends.remote.append((
            at.z != z2,
            lambda: pltpu.make_async_remote_copy(
                src_ref=stage, dst_ref=self.land.at[z2], send_sem=self.zs.at[z2],
                recv_sem=self.zr.at[z2], device_id={"context": at.z}, device_id_type=MESH,
            ).wait_send(),
        ))

    def total(self, own):
        at = self.at
        total = own
        for slot, there in ((at.z, at.z > 0), (at.nz, at.z + 1 < at.nz)):
            landed(self.land.at[slot], self.zs.at[0], self.zr.at[slot], only=there, context=at.z)
            total = total + jnp.where(there, self.land[slot].astype(F32), 0.0)
        return total


class Spread:
    def __init__(self, at, sends, src, dst, sems, same=False):
        self.at, self.sends, self.src, self.dst = at, sends, src, dst
        self.copy = None
        self.own, self.zs, self.zr, self.xs, self.xr, self.cs, self.cr, *chain = sems
        self.chain = Chain(at, sends, lambda z1: dst(at.s, z1), chain) if same else None

    @staticmethod
    def sems(ns, nz):
        dma, no = pltpu.SemaphoreType.DMA, ns // 2
        return [
            dma, dma((nz,)), dma((nz,)), dma((nz, no)), dma((nz, no)), dma((no, nz)), dma((no, nz)),
        ] + Chain.sems(nz)

    def over_z(self):
        at = self.at
        if self.chain is not None:
            self.chain.begin(self.src(at.z))
            return
        for there, z2 in at.near():
            self.sends.go(
                self.src(z2), self.dst(at.s, at.z), self.zs.at[z2], self.zr.at[at.z], only=there,
                context=z2,
            )

    def over_s(self, z1, ref, only=None):
        at = self.at
        for o in range(1, at.no):
            self.sends.go(
                ref, self.dst(at.s, z1), self.xs.at[z1, o], self.xr.at[z1, o], only=only,
                shard=at.s_to(o),
            )
        self.sends.go(
            ref, self.dst(at.s, z1), self.cs.at[0, z1], self.cr.at[0, z1], only=only, shard=at.mate
        )

    def own_block(self):
        at = self.at
        self.over_s(at.z, self.src(at.z))
        self.copy = pltpu.make_async_copy(self.src(at.z), self.dst(at.s, at.z), self.own)
        self.copy.start()

    def pass_z(self, steps=None):
        at = self.at
        if self.chain is not None:
            for side, valid, z1 in self.chain.hops(steps):
                self.over_s(z1, self.chain.step(side, valid, z1), only=valid)
            return
        for there, z1 in at.near():
            ref = self.dst(at.s, z1)
            landed(ref, self.zs.at[z1], self.zr.at[z1], only=there, context=z1)
            self.over_s(z1, ref, only=there)

    def pass_s(self):
        at = self.at
        for o in range(1, at.no):
            s1 = at.s_from(o)
            for d in range(at.nz):
                z1 = at.z_from(d)
                ref = self.dst(s1, z1)
                landed(ref, self.xs.at[z1, o], self.xr.at[z1, o], shard=s1)
                self.sends.go(ref, ref, self.cs.at[o, z1], self.cr.at[o, z1], shard=at.mate)

    def finish(self):
        at = self.at
        self.copy.wait()
        for o in range(at.no):
            for z1 in range(at.nz):
                ref = self.dst(at.mate_from(o), z1)
                landed(ref, self.cs.at[o, z1], self.cr.at[o, z1], shard=at.mate)

    def pass_all(self):
        self.pass_z()
        self.pass_s()


class Tokens:
    def __init__(self, at, sends, ref, sems):
        self.at, self.sends, self.ref = at, sends, ref
        self.ys, self.yr, *chain = sems
        self.chain = Chain(at, sends, lambda z1: ref.at[z1, at.y], chain)

    @staticmethod
    def sems(nz):
        dma = pltpu.SemaphoreType.DMA
        return [dma((nz,)), dma((nz,))] + Chain.sems(nz)

    def over_z(self, src):
        self.chain.begin(src)

    def over_y(self, z1, src, only=None):
        at = self.at
        self.sends.go(
            src, self.ref.at[z1, at.y], self.ys.at[z1], self.yr.at[z1], only=only, tensor=at.twin
        )

    def pass_z(self, steps=None):
        for side, valid, z1 in self.chain.hops(steps):
            self.over_y(z1, self.chain.step(side, valid, z1), only=valid)

    def wait_y(self, places, only=None):
        at = self.at
        for z1 in places:
            ref = self.ref.at[z1, at.twin]
            landed(
                ref, self.ys.at[z1], self.yr.at[z1], only=only and only(z1), tensor=at.twin
            )


def whole_lines(small, blocks, depth):
    tiles = []
    for t in range(blocks * depth // LANES):
        tile = jnp.zeros((8, LANES), F32)
        lane = lax.broadcasted_iota(jnp.int32, (8, LANES), 1) + t * LANES
        for b in range(t * LANES // depth, min(blocks, -(-(t + 1) * LANES // depth))):
            line = small[b, :8, :].astype(F32)
            shift = (b * depth - t * LANES) % LANES
            moved = pltpu.roll(line, shift, 1) if shift else line
            tile = jnp.where((lane >= b * depth) & (lane < (b + 1) * depth), moved, tile)
        tiles.append(tile)
    return jnp.concatenate(tiles, axis=1)


def turn_first(left, right):
    return lax.dot_general(left, right, (((0,), (0,)), ((), ())), preferred_element_type=F32)


def turn_last(left, right):
    return lax.dot_general(left, right, (((1,), (1,)), ((), ())), preferred_element_type=F32)


class Return:
    def __init__(self, at, sends, make, room, lands, out, sems):
        self.at, self.sends, self.make, self.out = at, sends, make, out
        self.stage, self.acc = room.at[pl.ds(0, at.no)], room.at[pl.ds(at.no, at.no)]
        self.landc, self.landx = lands
        self.cs, self.cr, self.xs, self.xr, self.zs, self.zr, self.own = sems
        self.chain, self.short = None, 0
        self.depth = self.acc.shape[1] // at.nz

    @staticmethod
    def sems(ns, nz):
        dma, no = pltpu.SemaphoreType.DMA, ns // 2
        return [
            dma((no,)), dma((no,)), dma((no, nz)), dma((no, nz)), dma((2, nz)), dma((2, nz)), dma((2,)),
        ]

    @staticmethod
    def lands(ns, nz, depth, cols):
        no = ns // 2
        return [pltpu.VMEM((n, nz * depth, cols), BF16) for n in (no, no - 1)]

    def give(self, o):
        at = self.at
        self.stage[o] = self.make(at.mate_to(o)).astype(BF16)
        self.sends.go(
            self.stage.at[o], self.landc.at[o], self.cs.at[o], self.cr.at[o], shard=at.mate
        )
        self.acc[o] = self.make(at.s_to(o)).astype(BF16)

    def give_all(self):
        for o in (*range(1, self.at.no), 0):
            self.give(o)

    def rows(self, z2):
        start = z2 * self.depth
        start = start if isinstance(start, int) else pl.multiple_of(start, SUBLANES)
        return pl.ds(start, self.depth)

    def piece(self, z2):
        return self.acc.at[0, self.rows(z2)]

    def slots(self):
        if self.chain is not None:
            return [(None, z2) for z2 in far_first(self.at.nz)]
        return [*self.at.near(), (None, self.at.z)]

    def add(self, o, z2, others):
        line = self.rows(z2)
        total = self.acc[o, line, :].astype(F32)
        for other, k in others:
            total = total + other[k, line, :].astype(F32)
        self.acc[o, line, :] = total.astype(BF16)

    def over_s(self, first=True, last=True):
        at = self.at
        slots = self.slots()
        middle = len(slots) // 2
        slots = (slots[:middle] if first else []) + (slots[middle:] if last else [])
        for o in range(1, at.no):
            if first:
                landed(self.landc.at[o], self.cs.at[o], self.cr.at[o], shard=at.mate)
            for there, z2 in slots:
                line = self.rows(z2)
                guarded(there, lambda: self.add(o, z2, [(self.landc, o)]))
                self.sends.go(
                    self.acc.at[o, line], self.landx.at[o - 1, line], self.xs.at[o, z2],
                    self.xr.at[o, z2], only=there, shard=at.s_to(o),
                )
        if first:
            landed(self.landc.at[0], self.cs.at[0], self.cr.at[0], shard=at.mate)

    def over_z(self, first=True, last=True):
        at = self.at
        slots = self.slots()
        middle = len(slots) // 2
        slots = (slots[:middle] if first else []) + (slots[middle:] if last else [])
        for there, z2 in slots:
            line = self.rows(z2)
            for o in range(1, at.no):
                landed(
                    self.landx.at[o - 1, line], self.xs.at[o, z2], self.xr.at[o, z2], only=there,
                    shard=at.s_from(o),
                )
            terms = [(self.landc, 0)] + [(self.landx, o - 1) for o in range(1, at.no)]
            guarded(there, lambda: self.add(0, z2, terms))
            if self.chain is not None:
                self.chain.put(z2, lambda: self.piece(z2)[...].astype(F32))
                continue
            for w, (cols, whole) in enumerate(self.wings(at.z)):
                src, dst = self.piece(z2).at[:, cols], self.out(at.z, cols)
                if there is not None:
                    self.sends.go(
                        src, dst, self.zs.at[w, z2], self.zr.at[w, at.z], only=both(whole, there),
                        context=z2,
                    )
                else:
                    copy = pltpu.make_async_copy(src, dst, self.own.at[w])
                    guarded(whole, copy.start)

    def wings(self, z1):
        unit, short = self.acc.shape[2], self.short
        yield (pl.ds(0, unit - short), None)
        if short:
            yield (pl.ds(unit - short, short), z1 + 1 < self.at.nz)

    def finish(self):
        at = self.at
        for w, (cols, whole) in enumerate(self.wings(at.z)):
            copy = pltpu.make_async_copy(
                self.piece(at.z).at[:, cols], self.out(at.z, cols), self.own.at[w]
            )
            guarded(whole, copy.wait)
        for there, z1 in at.near():
            for w, (cols, whole) in enumerate(self.wings(z1)):
                landed(
                    self.out(z1, cols), self.zs.at[w, z1], self.zr.at[w, z1],
                    only=both(whole, there), context=z1,
                )


class Reduce:
    def __init__(self, at, sends, parts, bufs, sems):
        self.at, self.sends, self.parts = at, sends, parts
        self.landy, *chain = bufs
        self.ys, self.yr, *chain_sems = sems
        self.chain = ChainSum(at, sends, chain, chain_sems)

    @staticmethod
    def sems(nz):
        dma = pltpu.SemaphoreType.DMA
        return [dma((nz,)), dma((nz,))] + ChainSum.sems(nz)

    @staticmethod
    def bufs(nz, half, width):
        return [pltpu.VMEM((nz, half, width), BF16)] + ChainSum.bufs(nz, (half, width))

    def over_y(self, places):
        at = self.at
        for z2 in places:
            self.sends.go(
                self.parts.at[z2, at.twin], self.landy.at[z2], self.ys.at[z2], self.yr.at[z2],
                tensor=at.twin,
            )

    def own(self, z2):
        return self.parts[z2, self.at.y].astype(F32) + self.landy[z2].astype(F32)

    def pass_y(self, places):
        at = self.at
        for z2 in places:
            landed(self.landy.at[z2], self.ys.at[z2], self.yr.at[z2], tensor=at.twin)
            self.chain.put(z2, lambda z2=z2: self.own(z2))

    def total(self):
        return self.chain.total(self.own(self.at.z))


def piece_of_lines(lines, b, depth):
    first, off = divmod(b * depth, LANES)
    tile = lines[:, first * LANES:(first + 1) * LANES]
    if not off:
        return tile
    tile = pltpu.roll(tile, LANES - off, 1)
    if off + depth <= LANES:
        return tile
    after = pltpu.roll(lines[:, (first + 1) * LANES:(first + 2) * LANES], LANES - off, 1)
    lane = lax.broadcasted_iota(jnp.int32, (8, LANES), 1)
    return jnp.where(lane < LANES - off, tile, after)


class Refs:
    def __init__(self, refs):
        self.refs, self.next = refs, 0

    def take(self, n):
        self.next += n
        return self.refs[self.next - n:self.next]


def layer_kernel(ns, nz, heads, kv, *refs):
    refs = Refs(refs)
    (qkv_in, out_in, small_in, gate_in, up_in, down_in, hidden, cot_in, segments) = refs.take(9)
    (block_out, input_grad, qkv_grad, out_grad, small_out, *ffn_out) = refs.take(8)
    at = Place(ns, nz)
    w_sends, sends = Sends(), Sends()
    depth = qkv_in.shape[0]
    rows, width = hidden.shape
    half = rows // 2
    group_rows = nz * rows
    q_cols = heads * HD
    qkv_cols = q_cols + 2 * kv * HD
    wide = nz * depth
    scale = HD ** (-0.5)
    repeat = heads // kv

    wa, gate_w, up_w, down_w = refs.take(4)
    n_spread, n_tokens, n_ret = len(Spread.sems(ns, nz)), len(Tokens.sems(nz)), len(Return.sems(ns, nz))
    n_red, n_sum = len(Reduce.sems(nz)), len(ChainSum.sems(nz))
    (small, ypart, yland, n2, cot, resid, query, kv_all, probs, attn) = refs.take(10)

    def block(ref):
        return lambda s1, z1: ref.at[s1, pl.ds(pl.multiple_of(z1 * depth, SUBLANES), depth)]

    w_qkv, w_out = (
        Spread(at, w_sends, lambda z2, src=src: src, block(dst), refs.take(n_spread), True)
        for src, dst in (
            (qkv_in, wa.at[:, :, pl.ds(0, qkv_cols)]), (out_in, wa.at[:, :, pl.ds(qkv_cols, q_cols)]),
        )
    )
    w_small = Spread(
        at, w_sends, lambda z2: small_in, lambda s1, z1: small.at[s1 * nz + z1],
        refs.take(n_spread), True,
    )
    ffn = [
        Spread(at, w_sends, lambda z2, src=src: src.at[z2], block(dst), refs.take(n_spread))
        for src, dst in ((gate_in, gate_w), (up_in, up_w), (down_in, down_w))
    ]
    t_cot = Tokens(at, sends, cot, refs.take(n_tokens))
    t_n2 = Tokens(at, sends, n2, refs.take(n_tokens))
    kvs, kvr, yps, ypr, cot_sem = refs.take(5)
    gate, up_val, d_act, act, d_gate, d_up, ffn_part, dn2_part = refs.take(8)
    normed1_b, d_resid_b, d_projb = refs.take(3)

    def columns(ref, s1):
        return ref[..., pl.ds(pl.multiple_of(s1 * wide, LANES), wide)].reshape(-1, wide)

    unit = gate_w.shape[2]

    def out_place(ref):
        return lambda z1, cols: ref.at[
            :, pl.ds(pl.multiple_of(z1 * unit + cols.start, LANES), cols.size)
        ]

    makers = (
        lambda s1: turn_first(columns(n2, s1), d_gate[...]),
        lambda s1: turn_first(columns(n2, s1), d_up[...]),
        lambda s1: turn_first(columns(cot, s1), act[...]),
    )
    rets = [
        Return(at, sends, makers[i], room, refs.take(2), out_place(ffn_out[i]), refs.take(n_ret))
        for i, room in enumerate((gate_w, up_w, down_w))
    ]
    for ret, out in zip(rets, ffn_out):
        ret.short = nz * unit - out.shape[1]

    def summed(make, first, cols):
        room = wa.at[:, :, pl.ds(first, cols)]
        ret = Return(at, sends, make, room, refs.take(2), None, refs.take(n_ret))
        (land,) = refs.take(1)
        ret.chain = ChainSum(at, sends, (ret.piece, land), refs.take(n_sum))
        return ret

    r_qkv = summed(lambda s1: turn_first(columns(normed1_b, s1), d_projb[...]), 0, qkv_cols)
    r_out = summed(lambda s1: turn_first(columns(d_resid_b, s1), attn[...]), qkv_cols, q_cols)
    r_dn2, r_ffn = (
        Reduce(at, sends, parts, refs.take(3), refs.take(n_red)) for parts in (dn2_part, ffn_part)
    )
    (d_resid_f, d_attn, d_score, dkv, dkv_land, dn1_part, dn1_land, small_b, small_land, small_z,
     small_zland, small_y, small_yland, cosine, sine, mask, dkvs, dkvr, shs, shr, szs, szr, ysems,
     yrecv) = refs.take(24)

    at.greet(everyone=True)
    w_small.over_z()
    w_small.own_block()
    for item in (w_qkv, w_out):
        item.over_z()
        item.own_block()
    my_half = cot_in.at[pl.ds(pl.multiple_of(at.y * half, SUBLANES), half)]
    sends.here(cot_in.at[pl.ds(0, half)], cot.at[at.z, 0], cot_sem.at[0])
    sends.here(cot_in.at[pl.ds(half, half)], cot.at[at.z, 1], cot_sem.at[1])
    w_small.pass_z()
    w_qkv.pass_z()
    w_out.pass_z()
    ffn[0].over_z()
    ffn[1].over_z()
    for item in ffn:
        item.own_block()

    hidden_f = hidden[...].astype(F32)
    factor1 = lax.rsqrt(jnp.mean(hidden_f * hidden_f, axis=1, keepdims=True) + EPSILON)
    seg = segments[...].astype(F32)
    row = lax.broadcasted_iota(jnp.int32, (rows, group_rows), 0) + at.z * rows
    col = lax.broadcasted_iota(jnp.int32, (rows, group_rows), 1)
    seg_row = jnp.sum(jnp.where(row == col, seg, 0.0), axis=1, keepdims=True)
    earlier = jnp.sum(jnp.where(seg < seg_row, 1.0, 0.0), axis=1, keepdims=True)
    mask[...] = jnp.where((seg == seg_row) & (col <= row), 1.0, 0.0)
    position = row[:, :1].astype(F32) - earlier
    lane = lax.broadcasted_iota(jnp.int32, (1, HD), 1)
    pair = lax.rem(lane, HD // 2).astype(F32)
    angle = position * jnp.exp(pair * (-2.0 * math.log(THETA) / HD))
    cosine[...] = jnp.cos(angle)
    sine[...] = jnp.sin(angle) * jnp.where(lane < HD // 2, -1.0, 1.0)
    w_small.pass_s()
    w_qkv.pass_s()
    w_out.pass_s()
    w_small.finish()
    gains = whole_lines(small, ns * nz, depth)
    normed1_b[...] = (hidden[...].astype(F32) * factor1 * gains[0:1, :]).astype(BF16)
    width_each = HD // (ns * nz)
    lane = lax.broadcasted_iota(jnp.int32, (8, LANES), 1)
    bias = jnp.zeros((8, LANES), F32)
    for b in range(ns * nz):
        line = small[b, 8:16, :].astype(F32)
        moved = pltpu.roll(line, b * width_each, 1) if b else line
        bias = jnp.where((lane >= b * width_each) & (lane < (b + 1) * width_each), moved, bias)
    w_qkv.finish()
    cos_t, sin_t = cosine[...], sine[...]

    def projected(head):
        weight = wa[:, :, head * HD:(head + 1) * HD].reshape(width, HD)
        return jnp.dot(normed1_b[...], weight, preferred_element_type=F32) + bias[head:head + 1, :]

    def rotated(values):
        return values * cos_t + pltpu.roll(values, HD // 2, 1) * sin_t

    for j in range(kv):
        kv_all[at.z, :, j * HD:(j + 1) * HD] = rotated(projected(heads + j)).astype(BF16)
        kv_all[at.z, :, (kv + j) * HD:(kv + j + 1) * HD] = projected(heads + kv + j).astype(BF16)
    for there, z2 in at.near():
        sends.go(
            kv_all.at[at.z], kv_all.at[at.z], kvs.at[z2], kvr.at[at.z], only=there, context=z2
        )
    ffn[2].over_z()
    t_cot.over_z(my_half)
    for h in range(heads):
        query[:, h * HD:(h + 1) * HD] = rotated(projected(h)).astype(BF16)
    ffn[0].pass_z()
    ffn[1].pass_z()
    for d in range(1, nz):
        z1 = at.z_from(d)
        landed(kv_all.at[z1], kvs.at[z1], kvr.at[z1], context=z1)

    def keys_of(j):
        return kv_all[:, :, j * HD:(j + 1) * HD].reshape(group_rows, HD)

    keep = mask[...] > 0
    for h in range(heads):
        keys, values = keys_of(h // repeat), keys_of(kv + h // repeat)
        scores = turn_last(query[:, h * HD:(h + 1) * HD], keys)
        scores = jnp.where(keep, scores * scale, -1e30)
        peak = jnp.max(scores, axis=1, keepdims=True)
        lse = peak + jnp.log(jnp.sum(jnp.exp(scores - peak), axis=1, keepdims=True))
        p = jnp.exp(scores - lse)
        probs[h * rows:(h + 1) * rows, :] = p
        out = jnp.dot(p.astype(BF16), values, preferred_element_type=F32)
        attn[:, h * HD:(h + 1) * HD] = out.astype(BF16)
    w_out.finish()
    out_w = wa[:, :, qkv_cols:qkv_cols + q_cols].reshape(width, q_cols)
    part = turn_last(attn[...], out_w).astype(BF16)
    ypart[0] = part[:half]
    ypart[1] = part[half:]
    sends.go(ypart.at[at.twin], yland, yps, ypr, tensor=at.twin)
    ffn[0].pass_s()

    landed(yland, yps, ypr, tensor=at.twin)
    base = pl.multiple_of(at.y * half, SUBLANES)
    total = ypart[at.y].astype(F32) + yland[...].astype(F32)
    res = hidden[pl.ds(base, half), :].astype(F32) + total
    resid[...] = res
    factor2 = lax.rsqrt(jnp.mean(res * res, axis=1, keepdims=True) + EPSILON)
    n2[at.z, at.y] = (res * factor2 * gains[1:2, :]).astype(BF16)
    t_n2.over_z(n2.at[at.z, at.y])
    t_n2.over_y(at.z, n2.at[at.z, at.y])
    ffn[1].pass_s()
    ffn[2].pass_z()
    t_cot.pass_z()
    t_n2.pass_z([1])
    ffn[2].pass_s()
    t_cot.wait_y(range(nz), lambda z1: at.z != z1)
    for item in ffn:
        item.finish()
    for copy in sends.local:
        copy.wait()
    sends.local = []

    def weight(ref):
        return ref[...].reshape(width, -1)

    d_act[...] = jnp.dot(cot[...].reshape(group_rows, width), weight(down_w), preferred_element_type=F32)
    few, tall = nz // 2, 32
    chunk = few * rows

    def half_block(first):
        t_n2.wait_y([first * few + i for i in range(few)])
        start = pl.multiple_of(first * chunk, chunk)
        mine = n2[pl.ds(first * few, few)].reshape(chunk, width)
        gate[...] = jnp.dot(mine, weight(gate_w), preferred_element_type=F32)
        up_val[...] = jnp.dot(mine, weight(up_w), preferred_element_type=F32)

        @pl.loop(0, chunk // tall)
        def _(i):
            line = pl.ds(pl.multiple_of(i * tall, tall), tall)
            whole = pl.ds(pl.multiple_of(start + i * tall, tall), tall)
            g, u, d = gate[line, :], up_val[line, :], d_act[whole, :]
            sigma = jax.nn.sigmoid(g)
            silu_val = g * sigma
            act[whole, :] = (silu_val * u).astype(BF16)
            d_gate[whole, :] = (d * u * sigma * (1.0 + g * (1.0 - sigma))).astype(BF16)
            d_up[whole, :] = (d * silu_val).astype(BF16)

        span = pl.ds(start, chunk)
        dn2_part[pl.ds(first * few, few)] = (
            turn_last(d_gate[span, :], weight(gate_w)) + turn_last(d_up[span, :], weight(up_w))
        ).astype(BF16).reshape(few, 2, half, width)
        r_dn2.over_y([first * few + i for i in range(few)])

    nearer = lax.div(at.z, few)
    t_n2.pass_z(range(2, nz - 1))
    half_block(nearer)
    t_n2.pass_z([nz - 1])
    half_block(1 - nearer)
    w_sends.drain()

    rets[0].give_all()
    rets[0].over_s()
    r_dn2.pass_y(far_first(nz))
    rets[0].over_z(last=False)
    rets[1].give_all()
    rets[1].over_s()
    res = resid[...]
    factor2 = lax.rsqrt(jnp.mean(res * res, axis=1, keepdims=True) + EPSILON)
    unit2 = res * factor2
    dn2 = r_dn2.total()
    grad_g2 = jnp.sum(dn2 * unit2, axis=0, keepdims=True)
    scaled = dn2 * gains[1:2, :]
    back2 = factor2 * (scaled - unit2 * jnp.mean(scaled * unit2, axis=1, keepdims=True))
    d_res = cot[at.z, at.y].astype(F32) + back2
    d_resid_f[at.y] = d_res
    d_resid_b[at.y] = d_res.astype(BF16)
    mine_b, mine_f = d_resid_b.at[at.y], d_resid_f.at[at.y]
    sends.go(mine_b, mine_b, ysems.at[0], yrecv.at[0], tensor=at.twin)
    ffn_part[...] = turn_last(act[...], weight(down_w)).astype(BF16).reshape(nz, 2, half, width)
    rets[2].give_all()
    rets[2].over_s()
    landed(d_resid_b.at[at.twin], ysems.at[0], yrecv.at[0], tensor=at.twin)
    r_ffn.over_y(far_first(nz))
    sends.go(mine_f, mine_f, ysems.at[1], yrecv.at[1], tensor=at.twin)

    d_resid_all = d_resid_b[...].reshape(rows, width)
    out_w = wa[:, :, qkv_cols:qkv_cols + q_cols].reshape(width, q_cols)
    d_attn[...] = jnp.dot(d_resid_all, out_w, preferred_element_type=F32).astype(BF16)
    r_out.give_all()
    r_out.over_s()

    def unrotated(values):
        return values * cos_t - pltpu.roll(values, HD // 2, 1) * sin_t

    bias_rows = [None] * (heads + 2 * kv)

    def place(head, grad):
        bias_rows[head] = jnp.sum(grad, axis=0, keepdims=True)
        d_projb[:, head * HD:(head + 1) * HD] = grad.astype(BF16)

    for j in range(kv):
        keys, values = keys_of(j), keys_of(kv + j)
        d_values = jnp.zeros((group_rows, HD), F32)
        d_keys = jnp.zeros((group_rows, HD), F32)
        for h in range(j * repeat, (j + 1) * repeat):
            d_out = d_attn[:, h * HD:(h + 1) * HD]
            p = probs[h * rows:(h + 1) * rows, :]
            d_prob = turn_last(d_out, values)
            delta = jnp.sum(
                d_out.astype(F32) * attn[:, h * HD:(h + 1) * HD].astype(F32), axis=1, keepdims=True
            )
            d_score[...] = (p * (d_prob - delta)).astype(BF16)
            d_query = jnp.dot(d_score[...], keys, preferred_element_type=F32)
            place(h, unrotated(d_query * scale))
            d_keys = d_keys + turn_first(d_score[...], query[:, h * HD:(h + 1) * HD])
            d_values = d_values + turn_first(p.astype(BF16), d_out)
        for i, grad in ((j, d_keys * scale), (kv + j, d_values)):
            dkv[:, :, i * HD:(i + 1) * HD] = grad.astype(BF16).reshape(nz, rows, HD)
    for there, z2 in at.near():
        sends.go(dkv.at[z2], dkv_land.at[at.z], dkvs.at[z2], dkvr.at[at.z], only=there, context=z2)
    rets[0].over_z(first=False)
    rets[1].over_z(last=False)
    d_own = dkv[at.z].astype(F32)
    for d in range(1, nz):
        z1 = at.z_from(d)
        landed(dkv_land.at[z1], dkvs.at[z1], dkvr.at[z1], context=z1)
        d_own = d_own + dkv_land[z1].astype(F32)
    for j in range(kv):
        place(heads + j, unrotated(d_own[:, j * HD:(j + 1) * HD]))
        place(heads + kv + j, d_own[:, (kv + j) * HD:(kv + j + 1) * HD])
    qkv_w = wa[:, :, :qkv_cols].reshape(width, qkv_cols)
    dn1_part[...] = turn_last(d_projb[...], qkv_w).astype(BF16)
    sends.go(dn1_part, dn1_land, ysems.at[2], yrecv.at[2], tensor=at.twin)
    r_qkv.give_all()
    r_qkv.over_s()
    rets[1].over_z(first=False)
    r_ffn.pass_y(far_first(nz))
    rets[2].over_z(last=False)
    r_out.over_z()

    block_out[at.y] = (r_ffn.total() + resid[...]).astype(BF16)
    sends.go(block_out.at[at.y], block_out.at[at.y], ysems.at[3], yrecv.at[3], tensor=at.twin)

    landed(dn1_land, ysems.at[2], yrecv.at[2], tensor=at.twin)
    landed(d_resid_f.at[at.twin], ysems.at[1], yrecv.at[1], tensor=at.twin)
    dn1 = dn1_part[...].astype(F32) + dn1_land[...].astype(F32)
    hidden_f = hidden[...].astype(F32)
    factor1 = lax.rsqrt(jnp.mean(hidden_f * hidden_f, axis=1, keepdims=True) + EPSILON)
    unit1 = hidden_f * factor1
    row = lax.broadcasted_iota(jnp.int32, (rows, 1), 0)
    my_row = (row >= at.y * half) & (row < (at.y + 1) * half)
    grad_g1 = jnp.sum(jnp.where(my_row, dn1 * unit1, 0.0), axis=0, keepdims=True)
    scaled = dn1 * gains[0:1, :]
    back1 = factor1 * (scaled - unit1 * jnp.mean(scaled * unit1, axis=1, keepdims=True))
    input_grad[...] = d_resid_f[...].reshape(rows, width) + back1

    both = jnp.concatenate([grad_g1, grad_g2, jnp.zeros((6, width), F32)], axis=0)
    bias = jnp.concatenate(bias_rows, axis=0)
    for b in range(ns * nz):
        moved = pltpu.roll(bias, LANES - b * width_each, 1) if b else bias
        small_b[b // nz, b % nz] = jnp.concatenate([piece_of_lines(both, b, depth), moved], axis=0)
    for k in range(1, ns):
        s2 = lax.rem(at.s + k, ns)
        sends.go(small_b.at[s2], small_land.at[k], shs.at[k], shr.at[k], shard=s2)
    rets[2].over_z(first=False)
    total = small_b[at.s]
    for k in range(1, ns):
        s1 = lax.rem(at.s - k + ns, ns)
        landed(small_land.at[k], shs.at[k], shr.at[k], shard=s1)
        total = total + small_land[k]
    small_z[...] = total
    for d in range(1, nz):
        sends.go(small_z.at[at.z_to(d)], small_zland.at[d], szs.at[d], szr.at[d], context=at.z_to(d))
    r_qkv.over_z()
    total = small_z[at.z]
    for d in range(1, nz):
        landed(small_zland.at[d], szs.at[d], szr.at[d], context=at.z_from(d))
        total = total + small_zland[d]
    small_y[...] = total
    sends.go(small_y, small_yland, ysems.at[4], yrecv.at[4], tensor=at.twin)
    out_grad[...] = r_out.chain.total(r_out.piece(at.z)[...].astype(F32))
    qkv_grad[...] = r_qkv.chain.total(r_qkv.piece(at.z)[...].astype(F32))
    landed(small_yland, ysems.at[4], yrecv.at[4], tensor=at.twin)
    small_out[:8, :] = small_y[:8, :] + small_yland[:8, :]
    small_out[8:, :] = small_y[8:, :]
    landed(block_out.at[at.twin], ysems.at[3], yrecv.at[3], tensor=at.twin)
    for ret in rets:
        ret.finish()
    sends.drain()


def layer(ns, nz, heads, kv, hidden_units, qkv_in, out_in, small_in, ffn_in, hidden, cot, segments):
    rows, width = hidden.shape
    owners, half, group_rows = ns * nz, rows // 2, nz * rows
    depth, cols = qkv_in.shape[0], qkv_in.shape[1] + out_in.shape[1]
    unit = ffn_in[0].shape[2]
    q_cols, kv_cols = heads * HD, 2 * kv * HD
    qkv_cols = q_cols + kv_cols
    dma = pltpu.SemaphoreType.DMA
    shape = jax.ShapeDtypeStruct
    room = pltpu.VMEM
    vmem = pl.BlockSpec(memory_space=pltpu.VMEM)
    anyspace = pl.BlockSpec(memory_space=pl.ANY)
    scratch = [room((ns, nz * depth, cols), BF16)] + [room((ns, nz * depth, unit), BF16)] * 3
    scratch += [
        room((owners, 16, LANES), BF16),
        room((2, half, width), BF16),
        room((half, width), BF16),
        room((nz, 2, half, width), BF16),
        room((nz, 2, half, width), BF16),
        room((half, width), F32),
        room((rows, q_cols), BF16),
        room((nz, rows, kv_cols), BF16),
        room((heads * rows, group_rows), F32),
        room((rows, q_cols), BF16),
    ]
    scratch += Spread.sems(ns, nz) * 6 + Tokens.sems(nz) * 2
    scratch += [dma((nz,)), dma((nz,)), dma, dma, dma((2,))]
    scratch += [room((group_rows // 2, unit), F32)] * 2 + [room((group_rows, unit), F32)]
    scratch += [room((group_rows, unit), BF16)] * 3 + [room((nz, 2, half, width), BF16)] * 2
    scratch += [
        room((rows, width), BF16), room((2, half, width), BF16), room((rows, qkv_cols), BF16),
    ]
    for _ in range(3):
        scratch += Return.lands(ns, nz, depth, unit) + Return.sems(ns, nz)
    for n in (qkv_cols, q_cols):
        scratch += Return.lands(ns, nz, depth, n) + Return.sems(ns, nz)
        scratch += ChainSum.bufs(nz, (depth, n))[1:] + ChainSum.sems(nz)
    for _ in range(2):
        scratch += Reduce.bufs(nz, half, width) + Reduce.sems(nz)
    scratch += [
        room((2, half, width), F32),
        room((rows, q_cols), BF16),
        room((rows, group_rows), BF16),
        room((nz, rows, kv_cols), BF16),
        room((nz, rows, kv_cols), BF16),
        room((rows, width), BF16),
        room((rows, width), BF16),
        room((ns, nz, 16, LANES), F32),
        room((ns, nz, 16, LANES), F32),
        room((nz, 16, LANES), F32),
        room((nz, 16, LANES), F32),
        room((16, LANES), F32),
        room((16, LANES), F32),
        room((rows, HD), F32),
        room((rows, HD), F32),
        room((rows, group_rows), F32),
        dma((nz,)), dma((nz,)), dma((ns,)), dma((ns,)), dma((nz,)), dma((nz,)), dma((5,)), dma((5,)),
    ]
    return pl.pallas_call(
        functools.partial(layer_kernel, ns, nz, heads, kv),
        out_shape=[
            shape((2, half, width), BF16),
            shape((rows, width), F32),
            shape((depth, qkv_cols), F32),
            shape((depth, q_cols), F32),
            shape((16, LANES), F32),
            *[shape((depth, hidden_units), BF16)] * 3,
        ],
        in_specs=[anyspace] * 6 + [vmem, anyspace, vmem],
        out_specs=[vmem] * 5 + [anyspace] * 3,
        scratch_shapes=scratch,
        compiler_params=pltpu.CompilerParams(
            collective_id=0, has_side_effects=True, vmem_limit_bytes=VMEM_BYTES
        ),
    )(qkv_in, out_in, small_in, *ffn_in, hidden, cot, segments)


def fast_step(
    ns,
    nz,
    hidden_in,
    segment_ids,
    attn_gain,
    qkv_weight,
    qkv_bias,
    out_weight,
    ffn_gain,
    gate_weight,
    up_weight,
    down_weight,
    out_cotangent,
):
    rows, width = hidden_in.shape
    depth, hidden_units = gate_weight.shape
    parts = 2
    heads = H // parts
    kv = KVH // parts
    unit_cols = -(-hidden_units // (nz * LANES)) * LANES
    padded = unit_cols * nz

    def by_place(weight):
        full = jnp.pad(weight, ((0, 0), (0, padded - hidden_units)))
        return jnp.transpose(full.reshape(depth, nz, unit_cols), (1, 0, 2))

    ffn_in = [by_place(w) for w in (gate_weight, up_weight, down_weight.T)]
    gains_in = jnp.pad(jnp.stack([attn_gain, ffn_gain]), ((0, 6), (0, LANES - depth)))
    bias_in = jnp.pad(qkv_bias, ((0, 0), (0, LANES - qkv_bias.shape[1])))
    small_in = jnp.concatenate([gains_in, bias_in], axis=0)

    block_out, input_grad, grad_qkv, grad_out, small, grad_gate, grad_up, grad_down = layer(
        ns, nz, heads, kv, hidden_units, qkv_weight, out_weight.T, small_in, ffn_in, hidden_in,
        out_cotangent, segment_ids,
    )

    return (
        block_out.reshape(rows, width),
        input_grad,
        small[0, :depth],
        grad_qkv,
        small[8:, : qkv_bias.shape[1]],
        grad_out.T,
        small[1, :depth],
        grad_gate.astype(F32),
        grad_up.astype(F32),
        grad_down.astype(F32).T,
    )


def general_step(
    hidden_in,
    segment_ids,
    attn_gain,
    qkv_weight,
    qkv_bias,
    out_weight,
    ffn_gain,
    gate_weight,
    up_weight,
    down_weight,
    out_cotangent,
):
    rows, width = hidden_in.shape
    depth = gate_weight.shape[0]
    hidden_units = gate_weight.shape[1]
    parts = lax.axis_size("tensor")
    blocks = lax.axis_size("context")
    heads = H // parts
    kv = KVH // parts
    repeat = H // KVH
    scale = HD ** (-0.5)
    block_index = lax.axis_index("context")
    part_index = lax.axis_index("tensor")
    half_rows = rows // parts
    unit_cols = -(-hidden_units // (blocks * LANES)) * LANES
    padded = unit_cols * blocks

    def spread(weight):
        full = jnp.pad(weight, ((0, 0), (0, padded - hidden_units)))
        mine = lax.all_to_all(full, "context", split_axis=1, concat_axis=0, tiled=True)
        mine = mine.reshape(blocks * depth, unit_cols)
        return lax.all_gather(mine, "shard", axis=0, tiled=True)

    gate_full = spread(gate_weight)
    up_full = spread(up_weight)
    down_full = spread(down_weight.T)
    gain_one = lax.all_gather(attn_gain, OWNERS, axis=0, tiled=True).astype(F32)
    gain_two = lax.all_gather(ffn_gain, OWNERS, axis=0, tiled=True).astype(F32)
    bias = lax.all_gather(qkv_bias, OWNERS, axis=1, tiled=True).reshape(-1).astype(F32)
    qkv_full = lax.all_gather(qkv_weight, OWNERS, axis=0, tiled=True)
    out_full = lax.all_gather(out_weight.T, OWNERS, axis=0, tiled=True)

    seg_all = segment_ids[0]
    group_rows = seg_all.shape[0]
    first_row = block_index * rows
    index_all = jnp.arange(group_rows, dtype=jnp.int32)
    earlier = jnp.sum((seg_all[None, :] < seg_all[:, None]).astype(jnp.int32), axis=1)
    positions = index_all - earlier
    seg_local = lax.dynamic_slice_in_dim(seg_all, first_row, rows)
    index_local = first_row + jnp.arange(rows, dtype=jnp.int32)
    allowed = (seg_local[:, None] == seg_all[None, :]) & (
        index_local[:, None] >= index_all[None, :]
    )
    cosine, sine = rotary_tables(positions)
    cos_local = lax.dynamic_slice_in_dim(cosine, first_row, rows)
    sin_local = lax.dynamic_slice_in_dim(sine, first_row, rows)

    hidden_all = lax.all_gather(hidden_in, "context", axis=0, tiled=True)
    normed_all, _, _ = norm_forward(hidden_all.astype(F32), gain_one)
    hidden_f = hidden_in.astype(F32)
    normed1, unit1, factor1 = norm_forward(hidden_f, gain_one)
    q_cols = heads * HD
    k_cols = kv * HD
    query_f = dot(normed1, qkv_full[:, :q_cols]) + bias[:q_cols]
    kv_f = dot(normed_all, qkv_full[:, q_cols:]) + bias[q_cols:]
    query = jnp.transpose(query_f.reshape(rows, heads, HD), (1, 0, 2))
    query = rotate(query, cos_local, sin_local).astype(BF16)
    keys = jnp.transpose(kv_f[:, :k_cols].reshape(group_rows, kv, HD), (1, 0, 2))
    keys = rotate(keys, cosine, sine).astype(BF16)
    values = jnp.transpose(kv_f[:, k_cols:].reshape(group_rows, kv, HD), (1, 0, 2)).astype(BF16)
    query = query.reshape(kv, repeat * rows, HD)
    mask = jnp.tile(allowed, (repeat, 1))
    scores = jnp.where(mask, batched(query, keys, 2, 2) * scale, -1e30)
    peak = jnp.max(scores, axis=2, keepdims=True)
    lse = peak + jnp.log(jnp.sum(jnp.exp(scores - peak), axis=2, keepdims=True))
    p_soft = jnp.exp(scores - lse)
    probs = p_soft.astype(BF16)
    outs = batched(probs, values, 2, 1).astype(BF16)
    attn = jnp.transpose(outs.reshape(heads, rows, HD), (1, 0, 2)).reshape(rows, q_cols)
    attn_part = contract_last(attn, out_full).astype(BF16)

    mine = part_index * half_rows
    attn_half = lax.psum_scatter(attn_part, "tensor", scatter_dimension=0, tiled=True)
    resid_half = lax.dynamic_slice_in_dim(hidden_f, mine, half_rows) + attn_half.astype(F32)
    normed2_half, unit2, factor2 = norm_forward(resid_half, gain_two)
    normed2 = lax.all_gather(normed2_half, TEAM, axis=0, tiled=True)
    cot_half = lax.dynamic_slice_in_dim(out_cotangent, mine, half_rows)
    cot = lax.all_gather(cot_half, TEAM, axis=0, tiled=True)

    gate = dot(normed2, gate_full)
    up_val = dot(normed2, up_full)
    sigma = jax.nn.sigmoid(gate)
    silu_val = gate * sigma
    act = (silu_val * up_val).astype(BF16)
    ffn_part = contract_last(act, down_full).astype(BF16)
    d_act = dot(cot, down_full)
    d_gate = (d_act * up_val * sigma * (1.0 + gate * (1.0 - sigma))).astype(BF16)
    d_up = (d_act * silu_val).astype(BF16)
    dn2_part = (contract_last(d_gate, gate_full) + contract_last(d_up, up_full)).astype(BF16)
    ffn_half = lax.psum_scatter(ffn_part, TEAM, scatter_dimension=0, tiled=True)
    block_half = (resid_half + ffn_half.astype(F32)).astype(BF16)
    block_out = lax.all_gather(block_half, "tensor", axis=0, tiled=True)
    dn2_half = lax.psum_scatter(dn2_part, TEAM, scatter_dimension=0, tiled=True).astype(F32)
    grad_g2, d_back2 = norm_backward(dn2_half, unit2, factor2, gain_two)
    d_resid_half = cot_half.astype(F32) + d_back2

    def give_back(grad):
        part = lax.psum_scatter(grad.astype(BF16), "shard", scatter_dimension=0, tiled=True)
        part = part.reshape(blocks, depth, unit_cols)
        part = lax.all_to_all(part, "context", split_axis=0, concat_axis=2, tiled=True)
        return part.reshape(depth, padded)[:, :hidden_units].astype(F32)

    sum_gate = give_back(contract_first(normed2, d_gate))
    sum_up = give_back(contract_first(normed2, d_up))
    sum_down = give_back(contract_first(cot, act)).T

    d_resid_b = lax.all_gather(d_resid_half.astype(BF16), "tensor", axis=0, tiled=True)
    grad_out = contract_first(d_resid_b, attn)
    d_attn = dot(d_resid_b, out_full).astype(BF16)
    d_outs = jnp.transpose(d_attn.reshape(rows, heads, HD), (1, 0, 2)).reshape(
        kv, repeat * rows, HD
    )
    d_prob = batched(d_outs, values, 2, 2)
    delta = jnp.sum(d_outs.astype(F32) * outs.astype(F32), axis=2, keepdims=True)
    d_score = (p_soft * (d_prob - delta)).astype(BF16)
    d_query = batched(d_score, keys, 2, 1) * scale
    d_keys = batched(d_score, query, 1, 1) * scale
    d_values = batched(probs, d_outs, 1, 1)
    d_kv = jnp.concatenate([d_keys, d_values], axis=0).astype(BF16)
    d_kv = lax.psum_scatter(d_kv, "context", scatter_dimension=1, tiled=True).astype(F32)
    d_query = unrotate(d_query.reshape(heads, rows, HD), cos_local, sin_local)
    d_keys = unrotate(d_kv[:kv], cos_local, sin_local)
    d_proj = jnp.transpose(jnp.concatenate([d_query, d_keys, d_kv[kv:]], axis=0), (1, 0, 2))
    grad_bias = jnp.sum(d_proj, axis=0)
    d_projb = d_proj.reshape(rows, -1).astype(BF16)
    grad_qkv = contract_first(normed1, d_projb)
    dn1_part = contract_last(d_projb, qkv_full).astype(BF16)
    dn1_half = lax.psum_scatter(dn1_part, "tensor", scatter_dimension=0, tiled=True).astype(F32)
    unit1_half = lax.dynamic_slice_in_dim(unit1, mine, half_rows)
    factor1_half = lax.dynamic_slice_in_dim(factor1, mine, half_rows)
    grad_g1, d_back1 = norm_backward(dn1_half, unit1_half, factor1_half, gain_one)
    input_grad = lax.all_gather(d_resid_half + d_back1, "tensor", axis=0, tiled=True)

    gains = lax.psum(jnp.stack([grad_g1, grad_g2]), "tensor")
    sum_gains = lax.psum_scatter(gains, OWNERS, scatter_dimension=1, tiled=True)
    sum_qkv = lax.psum_scatter(grad_qkv.astype(BF16), OWNERS, scatter_dimension=0, tiled=True)
    sum_bias = lax.psum_scatter(grad_bias, OWNERS, scatter_dimension=1, tiled=True)
    sum_out = lax.psum_scatter(grad_out.astype(BF16), OWNERS, scatter_dimension=0, tiled=True)
    return (
        block_out,
        input_grad,
        sum_gains[0],
        sum_qkv.astype(F32),
        sum_bias,
        sum_out.astype(F32).T,
        sum_gains[1],
        sum_gate,
        sum_up,
        sum_down,
    )


def solution(mesh):
    ns, nz, parts = (mesh.shape[a] for a in ("shard", "context", "tensor"))
    rows = P(OWNERS, None)

    def local(*args):
        depth = args[7].shape[0]
        if depth % SUBLANES == 0 and ns % 2 == 0 and ns > 2 and nz % 2 == 0 and parts == 2:
            return fast_step(ns, nz, *args)
        return general_step(*args)

    placed = (
        rows,
        P("shard", None),
        P(OWNERS),
        P(OWNERS, "tensor"),
        P("tensor", OWNERS),
        P("tensor", OWNERS),
        P(OWNERS),
        P(OWNERS, "tensor"),
        P(OWNERS, "tensor"),
        P("tensor", OWNERS),
        rows,
    )
    return jax.shard_map(
        local,
        mesh=mesh,
        in_specs=placed,
        out_specs=(
            rows,
            rows,
            P(OWNERS),
            P(OWNERS, "tensor"),
            P("tensor", OWNERS),
            P("tensor", OWNERS),
            P(OWNERS),
            P(OWNERS, "tensor"),
            P(OWNERS, "tensor"),
            P("tensor", OWNERS),
        ),
        check_vma=False,
    )
```

```python
import functools
import math

import jax
import jax.numpy as jnp
from jax import lax
from jax.experimental import pallas as pl
from jax.experimental.pallas import tpu as pltpu
from jax.sharding import PartitionSpec as P

H = 12
KVH = 2
HD = 128
LANES = 128
SUBLANES = 16
BF16 = jnp.bfloat16
F32 = jnp.float32

EPSILON = 1e-06
THETA = 1000000.0

OWNERS = ("shard", "context")
TEAM = ("context", "tensor")
MESH = pl.DeviceIdType.MESH
VMEM_BYTES = 62 * 1024 * 1024


def dot(left, right):
    return jnp.dot(left, right, preferred_element_type=F32)


def contract_last(left, right):
    return lax.dot_general(left, right, (((1,), (1,)), ((), ())), preferred_element_type=F32)


def contract_first(left, right):
    return lax.dot_general(left, right, (((0,), (0,)), ((), ())), preferred_element_type=F32)


def batched(left, right, left_dim, right_dim):
    return lax.dot_general(
        left, right, (((left_dim,), (right_dim,)), ((0,), (0,))), preferred_element_type=F32
    )


def norm_forward(values, gain):
    factor = lax.rsqrt(jnp.mean(values * values, axis=1, keepdims=True) + EPSILON)
    unit = values * factor
    return ((unit * gain).astype(BF16), unit, factor)


def norm_backward(grad_out, unit, factor, gain):
    gain_grad = jnp.sum(grad_out * unit, axis=0)
    scaled = grad_out * gain
    return (gain_grad, factor * (scaled - unit * jnp.mean(scaled * unit, axis=1, keepdims=True)))


def rotary_tables(positions):
    half = HD // 2
    freqs = THETA ** (-(2.0 * jnp.arange(half, dtype=F32)) / HD)
    angles = positions.astype(F32)[:, None] * freqs[None, :]
    cosine, sine = jnp.cos(angles), jnp.sin(angles)
    return (
        jnp.concatenate([cosine, cosine], axis=1),
        jnp.concatenate([-sine, sine], axis=1),
    )


def swap_halves(values):
    half = values.shape[-1] // 2
    return jnp.concatenate([values[..., half:], values[..., :half]], axis=-1)


def rotate(values, cosine, sine):
    return values * cosine + swap_halves(values) * sine


def unrotate(values, cosine, sine):
    return values * cosine - swap_halves(values) * sine


class Place:
    def __init__(self, ns, nz):
        self.ns, self.nz, self.no = ns, nz, ns // 2
        self.s, self.z, self.y = (lax.axis_index(a) for a in ("shard", "context", "tensor"))
        self.core = lax.rem(self.s, 2)
        self.outer = lax.div(self.s, 2)
        self.mate = self.s + 1 - 2 * self.core
        self.twin = 1 - self.y

    def z_to(self, d):
        return lax.rem(self.z + d, self.nz)

    def z_from(self, d):
        return lax.rem(self.z - d + self.nz, self.nz)

    def near(self):
        for k in range(1, self.nz):
            yield (self.z + k < self.nz, lax.rem(self.z + k, self.nz))
            yield (self.z >= k, lax.rem(self.z - k + self.nz, self.nz))

    def s_to(self, o):
        return lax.rem(self.outer + o, self.no) * 2 + self.core

    def s_from(self, o):
        return lax.rem(self.outer - o + self.no, self.no) * 2 + self.core

    def mate_from(self, o):
        return lax.rem(self.outer - o + self.no, self.no) * 2 + 1 - self.core

    def mate_to(self, o):
        return lax.rem(self.outer + o, self.no) * 2 + 1 - self.core

    def greet(self, everyone=False):
        barrier = pltpu.get_barrier_semaphore()
        peers = [{"context": self.z_to(d)} for d in range(1, self.nz)]
        if everyone:
            peers += [{"shard": lax.rem(self.s + k, self.ns)} for k in range(1, self.ns)]
        else:
            peers += [{"shard": self.s_to(o)} for o in range(1, self.no)] + [{"shard": self.mate}]
        peers += [{"tensor": self.twin}]
        for peer in peers:
            pl.semaphore_signal(barrier, inc=1, device_id=peer, device_id_type=MESH)
        pl.semaphore_wait(barrier, len(peers))


class Sends:
    def __init__(self):
        self.remote, self.local = [], []

    def go(self, src, dst, send, recv, only=None, **peer):
        copy = pltpu.make_async_remote_copy(
            src_ref=src, dst_ref=dst, send_sem=send, recv_sem=recv,
            device_id=peer, device_id_type=MESH,
        )
        guarded(only, copy.start)
        self.remote.append((only, copy.wait_send))

    def here(self, src, dst, sem):
        copy = pltpu.make_async_copy(src, dst, sem)
        copy.start()
        self.local.append(copy)

    def drain(self):
        for only, wait in self.remote:
            guarded(only, wait)
        for copy in self.local:
            copy.wait()
        self.remote, self.local = [], []


def both(one, other):
    return other if one is None else one & other


def guarded(only, action):
    if only is None:
        action()
    else:
        pl.when(only)(action)


def landed(ref, send, recv, only=None, **peer):
    copy = pltpu.make_async_remote_copy(
        src_ref=ref, dst_ref=ref, send_sem=send, recv_sem=recv,
        device_id=peer, device_id_type=MESH,
    )
    guarded(only, copy.wait_recv)


def far_first(n):
    return [n - 1 - i // 2 if i % 2 == 0 else i // 2 for i in range(n)]


class Chain:
    def __init__(self, at, sends, ref, sems):
        self.at, self.sends, self.ref = at, sends, ref
        self.zs, self.zr = sems

    @staticmethod
    def sems(nz):
        dma = pltpu.SemaphoreType.DMA
        return [dma((2, nz)), dma((nz,))]

    def hops(self, steps=None):
        at = self.at
        for k in steps or range(1, at.nz):
            yield (-1, at.z - k >= 0, at.z - k)
            yield (1, at.z + k < at.nz, at.z + k)

    def hand(self, way, origin, src, only):
        at = self.at
        there = at.z + 1 < at.nz if way == 0 else at.z > 0
        self.sends.go(
            src, self.ref(origin), self.zs.at[way, origin], self.zr.at[origin],
            only=there if only is None else there & only, context=at.z + (1 if way == 0 else -1),
        )

    def begin(self, src):
        for way in range(2):
            self.hand(way, self.at.z, src, None)

    def step(self, side, valid, origin):
        ref = self.ref(origin)
        landed(ref, self.zs.at[0, origin], self.zr.at[origin], only=valid, context=self.at.z)
        self.hand(0 if side < 0 else 1, origin, ref, valid)
        return ref


class ChainSum:
    def __init__(self, at, sends, bufs, sems):
        self.at, self.sends = at, sends
        stage, self.land = bufs
        self.stage = stage if callable(stage) else lambda z2: stage.at[z2]
        self.zs, self.zr = sems

    @staticmethod
    def sems(nz):
        dma = pltpu.SemaphoreType.DMA
        return [dma((nz,)), dma((nz + 1,))]

    @staticmethod
    def bufs(nz, shape, dtype=BF16):
        return [pltpu.VMEM((nz, *shape), dtype), pltpu.VMEM((nz + 1, *shape), dtype)]

    def put(self, z2, own):
        at = self.at
        stage, dtype = self.stage(z2), self.land.dtype

        def start(slot, before):
            slot_ref = self.land.at[z2]

            @pl.when(before)
            def _():
                landed(slot_ref, self.zs.at[z2], self.zr.at[z2], context=at.z)
                stage[...] = (own() + self.land[z2].astype(F32)).astype(dtype)

            @pl.when(jnp.logical_not(before))
            def _():
                stage[...] = own().astype(dtype)

            pltpu.make_async_remote_copy(
                src_ref=stage, dst_ref=self.land.at[slot], send_sem=self.zs.at[z2],
                recv_sem=self.zr.at[slot], device_id={"context": at.z + (1 if z2_right else -1)},
                device_id_type=MESH,
            ).start()

        for z2_right in (True, False):
            away = at.z < z2 if z2_right else at.z > z2

            @pl.when(away)
            def _(z2_right=z2_right):
                near = at.z + 1 == z2 if z2_right else at.z - 1 == z2
                slot = z2 if z2_right else z2 + near * (at.nz - z2)
                before = at.z > 0 if z2_right else at.z + 1 < at.nz
                start(slot, before)

        self.sends.remote.append((
            at.z != z2,
            lambda: pltpu.make_async_remote_copy(
                src_ref=stage, dst_ref=self.land.at[z2], send_sem=self.zs.at[z2],
                recv_sem=self.zr.at[z2], device_id={"context": at.z}, device_id_type=MESH,
            ).wait_send(),
        ))

    def total(self, own):
        at = self.at
        total = own
        for slot, there in ((at.z, at.z > 0), (at.nz, at.z + 1 < at.nz)):
            landed(self.land.at[slot], self.zs.at[0], self.zr.at[slot], only=there, context=at.z)
            total = total + jnp.where(there, self.land[slot].astype(F32), 0.0)
        return total


class Spread:
    def __init__(self, at, sends, src, dst, sems, same=False):
        self.at, self.sends, self.src, self.dst = at, sends, src, dst
        self.copy = None
        self.own, self.zs, self.zr, self.xs, self.xr, self.cs, self.cr, *chain = sems
        self.chain = Chain(at, sends, lambda z1: dst(at.s, z1), chain) if same else None

    @staticmethod
    def sems(ns, nz):
        dma, no = pltpu.SemaphoreType.DMA, ns // 2
        return [
            dma, dma((nz,)), dma((nz,)), dma((nz, no)), dma((nz, no)), dma((no, nz)), dma((no, nz)),
        ] + Chain.sems(nz)

    def over_z(self):
        at = self.at
        if self.chain is not None:
            self.chain.begin(self.src(at.z))
            return
        for there, z2 in at.near():
            self.sends.go(
                self.src(z2), self.dst(at.s, at.z), self.zs.at[z2], self.zr.at[at.z], only=there,
                context=z2,
            )

    def over_s(self, z1, ref, only=None):
        at = self.at
        for o in range(1, at.no):
            self.sends.go(
                ref, self.dst(at.s, z1), self.xs.at[z1, o], self.xr.at[z1, o], only=only,
                shard=at.s_to(o),
            )
        self.sends.go(
            ref, self.dst(at.s, z1), self.cs.at[0, z1], self.cr.at[0, z1], only=only, shard=at.mate
        )

    def own_block(self):
        at = self.at
        self.over_s(at.z, self.src(at.z))
        self.copy = pltpu.make_async_copy(self.src(at.z), self.dst(at.s, at.z), self.own)
        self.copy.start()

    def pass_z(self, steps=None):
        at = self.at
        if self.chain is not None:
            for side, valid, z1 in self.chain.hops(steps):
                self.over_s(z1, self.chain.step(side, valid, z1), only=valid)
            return
        for there, z1 in at.near():
            ref = self.dst(at.s, z1)
            landed(ref, self.zs.at[z1], self.zr.at[z1], only=there, context=z1)
            self.over_s(z1, ref, only=there)

    def pass_s(self):
        at = self.at
        for o in range(1, at.no):
            s1 = at.s_from(o)
            for d in range(at.nz):
                z1 = at.z_from(d)
                ref = self.dst(s1, z1)
                landed(ref, self.xs.at[z1, o], self.xr.at[z1, o], shard=s1)
                self.sends.go(ref, ref, self.cs.at[o, z1], self.cr.at[o, z1], shard=at.mate)

    def finish(self):
        at = self.at
        self.copy.wait()
        for o in range(at.no):
            for z1 in range(at.nz):
                ref = self.dst(at.mate_from(o), z1)
                landed(ref, self.cs.at[o, z1], self.cr.at[o, z1], shard=at.mate)

    def pass_all(self):
        self.pass_z()
        self.pass_s()


class Tokens:
    def __init__(self, at, sends, ref, sems):
        self.at, self.sends, self.ref = at, sends, ref
        self.ys, self.yr, *chain = sems
        self.chain = Chain(at, sends, lambda z1: ref.at[z1, at.y], chain)

    @staticmethod
    def sems(nz):
        dma = pltpu.SemaphoreType.DMA
        return [dma((nz,)), dma((nz,))] + Chain.sems(nz)

    def over_z(self, src):
        self.chain.begin(src)

    def over_y(self, z1, src, only=None):
        at = self.at
        self.sends.go(
            src, self.ref.at[z1, at.y], self.ys.at[z1], self.yr.at[z1], only=only, tensor=at.twin
        )

    def pass_z(self, steps=None):
        for side, valid, z1 in self.chain.hops(steps):
            self.over_y(z1, self.chain.step(side, valid, z1), only=valid)

    def wait_y(self, places, only=None):
        at = self.at
        for z1 in places:
            ref = self.ref.at[z1, at.twin]
            landed(
                ref, self.ys.at[z1], self.yr.at[z1], only=only and only(z1), tensor=at.twin
            )


def whole_lines(small, blocks, depth):
    tiles = []
    for t in range(blocks * depth // LANES):
        tile = jnp.zeros((8, LANES), F32)
        lane = lax.broadcasted_iota(jnp.int32, (8, LANES), 1) + t * LANES
        for b in range(t * LANES // depth, min(blocks, -(-(t + 1) * LANES // depth))):
            line = small[b, :8, :].astype(F32)
            shift = (b * depth - t * LANES) % LANES
            moved = pltpu.roll(line, shift, 1) if shift else line
            tile = jnp.where((lane >= b * depth) & (lane < (b + 1) * depth), moved, tile)
        tiles.append(tile)
    return jnp.concatenate(tiles, axis=1)


def turn_first(left, right):
    return lax.dot_general(left, right, (((0,), (0,)), ((), ())), preferred_element_type=F32)


def turn_last(left, right):
    return lax.dot_general(left, right, (((1,), (1,)), ((), ())), preferred_element_type=F32)


class Return:
    def __init__(self, at, sends, make, room, lands, out, sems):
        self.at, self.sends, self.make, self.out = at, sends, make, out
        self.stage, self.acc = room.at[pl.ds(0, at.no)], room.at[pl.ds(at.no, at.no)]
        self.landc, self.landx = lands
        self.cs, self.cr, self.xs, self.xr, self.zs, self.zr, self.own = sems
        self.chain, self.short = None, 0
        self.depth = self.acc.shape[1] // at.nz

    @staticmethod
    def sems(ns, nz):
        dma, no = pltpu.SemaphoreType.DMA, ns // 2
        return [
            dma((no,)), dma((no,)), dma((no, nz)), dma((no, nz)), dma((2, nz)), dma((2, nz)), dma((2,)),
        ]

    @staticmethod
    def lands(ns, nz, depth, cols):
        no = ns // 2
        return [pltpu.VMEM((n, nz * depth, cols), BF16) for n in (no, no - 1)]

    def to_mate(self, o):
        return pltpu.make_async_remote_copy(
            src_ref=self.stage.at[o], dst_ref=self.landc.at[o], send_sem=self.cs.at[o],
            recv_sem=self.cr.at[o], device_id={"shard": self.at.mate}, device_id_type=MESH,
        )

    def give_all(self):
        at = self.at

        @pl.loop(0, at.no)
        def _(i):
            o = at.no - 1 - i
            self.stage[o] = self.make(at.mate_to(o)).astype(BF16)
            self.to_mate(o).start()
            self.acc[o] = self.make(at.s_to(o)).astype(BF16)

        self.sends.remote += [(None, self.to_mate(o).wait_send) for o in range(at.no)]

    def rows(self, z2):
        start = z2 * self.depth
        start = start if isinstance(start, int) else pl.multiple_of(start, SUBLANES)
        return pl.ds(start, self.depth)

    def piece(self, z2):
        return self.acc.at[0, self.rows(z2)]

    def slots(self):
        if self.chain is not None:
            return [(None, z2) for z2 in far_first(self.at.nz)]
        return [*self.at.near(), (None, self.at.z)]

    def add(self, o, z2, others):
        line = self.rows(z2)
        total = self.acc[o, line, :].astype(F32)
        for other, k in others:
            total = total + other[k, line, :].astype(F32)
        self.acc[o, line, :] = total.astype(BF16)

    def over_s(self, first=True, last=True):
        at = self.at
        slots = self.slots()
        middle = len(slots) // 2
        slots = (slots[:middle] if first else []) + (slots[middle:] if last else [])
        for o in range(1, at.no):
            if first:
                landed(self.landc.at[o], self.cs.at[o], self.cr.at[o], shard=at.mate)
            for there, z2 in slots:
                line = self.rows(z2)
                guarded(there, lambda: self.add(o, z2, [(self.landc, o)]))
                self.sends.go(
                    self.acc.at[o, line], self.landx.at[o - 1, line], self.xs.at[o, z2],
                    self.xr.at[o, z2], only=there, shard=at.s_to(o),
                )
        if first:
            landed(self.landc.at[0], self.cs.at[0], self.cr.at[0], shard=at.mate)

    def over_z(self, first=True, last=True):
        at = self.at
        slots = self.slots()
        middle = len(slots) // 2
        slots = (slots[:middle] if first else []) + (slots[middle:] if last else [])
        for there, z2 in slots:
            line = self.rows(z2)
            for o in range(1, at.no):
                landed(
                    self.landx.at[o - 1, line], self.xs.at[o, z2], self.xr.at[o, z2], only=there,
                    shard=at.s_from(o),
                )
            terms = [(self.landc, 0)] + [(self.landx, o - 1) for o in range(1, at.no)]
            guarded(there, lambda: self.add(0, z2, terms))
            if self.chain is not None:
                self.chain.put(z2, lambda: self.piece(z2)[...].astype(F32))
                continue
            for w, (cols, whole) in enumerate(self.wings(at.z)):
                src, dst = self.piece(z2).at[:, cols], self.out(at.z, cols)
                if there is not None:
                    self.sends.go(
                        src, dst, self.zs.at[w, z2], self.zr.at[w, at.z], only=both(whole, there),
                        context=z2,
                    )
                else:
                    copy = pltpu.make_async_copy(src, dst, self.own.at[w])
                    guarded(whole, copy.start)

    def wings(self, z1):
        unit, short = self.acc.shape[2], self.short
        yield (pl.ds(0, unit - short), None)
        if short:
            yield (pl.ds(unit - short, short), z1 + 1 < self.at.nz)

    def finish(self):
        at = self.at
        for w, (cols, whole) in enumerate(self.wings(at.z)):
            copy = pltpu.make_async_copy(
                self.piece(at.z).at[:, cols], self.out(at.z, cols), self.own.at[w]
            )
            guarded(whole, copy.wait)
        for there, z1 in at.near():
            for w, (cols, whole) in enumerate(self.wings(z1)):
                landed(
                    self.out(z1, cols), self.zs.at[w, z1], self.zr.at[w, z1],
                    only=both(whole, there), context=z1,
                )


class Reduce:
    def __init__(self, at, sends, parts, bufs, sems):
        self.at, self.sends, self.parts = at, sends, parts
        self.landy, *chain = bufs
        self.ys, self.yr, *chain_sems = sems
        self.chain = ChainSum(at, sends, chain, chain_sems)

    @staticmethod
    def sems(nz):
        dma = pltpu.SemaphoreType.DMA
        return [dma((nz,)), dma((nz,))] + ChainSum.sems(nz)

    @staticmethod
    def bufs(nz, half, width):
        return [pltpu.VMEM((nz, half, width), BF16)] + ChainSum.bufs(nz, (half, width))

    def over_y(self, places):
        at = self.at
        for z2 in places:
            self.sends.go(
                self.parts.at[z2, at.twin], self.landy.at[z2], self.ys.at[z2], self.yr.at[z2],
                tensor=at.twin,
            )

    def own(self, z2):
        return self.parts[z2, self.at.y].astype(F32) + self.landy[z2].astype(F32)

    def pass_y(self, places):
        at = self.at
        for z2 in places:
            landed(self.landy.at[z2], self.ys.at[z2], self.yr.at[z2], tensor=at.twin)
            self.chain.put(z2, lambda z2=z2: self.own(z2))

    def total(self):
        return self.chain.total(self.own(self.at.z))


def piece_of_lines(lines, b, depth):
    first, off = divmod(b * depth, LANES)
    tile = lines[:, first * LANES:(first + 1) * LANES]
    if not off:
        return tile
    tile = pltpu.roll(tile, LANES - off, 1)
    if off + depth <= LANES:
        return tile
    after = pltpu.roll(lines[:, (first + 1) * LANES:(first + 2) * LANES], LANES - off, 1)
    lane = lax.broadcasted_iota(jnp.int32, (8, LANES), 1)
    return jnp.where(lane < LANES - off, tile, after)


class Refs:
    def __init__(self, refs):
        self.refs, self.next = refs, 0

    def take(self, n):
        self.next += n
        return self.refs[self.next - n:self.next]


def layer_kernel(ns, nz, heads, kv, *refs):
    refs = Refs(refs)
    (qkv_in, out_in, small_in, gate_in, up_in, down_in, hidden, cot_in, segments) = refs.take(9)
    (block_out, input_grad, qkv_grad, out_grad, small_out, *ffn_out) = refs.take(8)
    at = Place(ns, nz)
    w_sends, sends = Sends(), Sends()
    depth = qkv_in.shape[0]
    rows, width = hidden.shape
    half = rows // 2
    group_rows = nz * rows
    q_cols = heads * HD
    qkv_cols = q_cols + 2 * kv * HD
    wide = nz * depth
    scale = HD ** (-0.5)
    repeat = heads // kv

    wa, gate_w, up_w, down_w = refs.take(4)
    n_spread, n_tokens, n_ret = len(Spread.sems(ns, nz)), len(Tokens.sems(nz)), len(Return.sems(ns, nz))
    n_red, n_sum = len(Reduce.sems(nz)), len(ChainSum.sems(nz))
    (small, ypart, yland, n2, cot, resid, query, kv_all, probs, attn) = refs.take(10)

    def block(ref):
        return lambda s1, z1: ref.at[s1, pl.ds(pl.multiple_of(z1 * depth, SUBLANES), depth)]

    w_qkv, w_out = (
        Spread(at, w_sends, lambda z2, src=src: src, block(dst), refs.take(n_spread), True)
        for src, dst in (
            (qkv_in, wa.at[:, :, pl.ds(0, qkv_cols)]), (out_in, wa.at[:, :, pl.ds(qkv_cols, q_cols)]),
        )
    )
    w_small = Spread(
        at, w_sends, lambda z2: small_in, lambda s1, z1: small.at[s1 * nz + z1],
        refs.take(n_spread), True,
    )
    ffn = [
        Spread(at, w_sends, lambda z2, src=src: src.at[z2], block(dst), refs.take(n_spread))
        for src, dst in ((gate_in, gate_w), (up_in, up_w), (down_in, down_w))
    ]
    t_cot = Tokens(at, sends, cot, refs.take(n_tokens))
    t_n2 = Tokens(at, sends, n2, refs.take(n_tokens))
    kvs, kvr, yps, ypr, cot_sem = refs.take(5)
    gate, up_val, d_act, act, d_gate, d_up, ffn_part, dn2_part = refs.take(8)
    normed1_b, d_resid_b, d_projb = refs.take(3)

    def columns(ref, s1):
        return ref[..., pl.ds(pl.multiple_of(s1 * wide, LANES), wide)].reshape(-1, wide)

    unit = gate_w.shape[2]

    def out_place(ref):
        return lambda z1, cols: ref.at[
            :, pl.ds(pl.multiple_of(z1 * unit + cols.start, LANES), cols.size)
        ]

    makers = (
        lambda s1: turn_first(columns(n2, s1), d_gate[...]),
        lambda s1: turn_first(columns(n2, s1), d_up[...]),
        lambda s1: turn_first(columns(cot, s1), act[...]),
    )
    rets = [
        Return(at, sends, makers[i], room, refs.take(2), out_place(ffn_out[i]), refs.take(n_ret))
        for i, room in enumerate((gate_w, up_w, down_w))
    ]
    for ret, out in zip(rets, ffn_out):
        ret.short = nz * unit - out.shape[1]

    def summed(make, first, cols):
        room = wa.at[:, :, pl.ds(first, cols)]
        ret = Return(at, sends, make, room, refs.take(2), None, refs.take(n_ret))
        (land,) = refs.take(1)
        ret.chain = ChainSum(at, sends, (ret.piece, land), refs.take(n_sum))
        return ret

    r_qkv = summed(lambda s1: turn_first(columns(normed1_b, s1), d_projb[...]), 0, qkv_cols)
    r_out = summed(lambda s1: turn_first(columns(d_resid_b, s1), attn[...]), qkv_cols, q_cols)
    r_dn2, r_ffn = (
        Reduce(at, sends, parts, refs.take(3), refs.take(n_red)) for parts in (dn2_part, ffn_part)
    )
    (d_resid_f, d_attn, d_score, dkv, dkv_land, dn1_part, dn1_land, small_b, small_land, small_z,
     small_zland, small_y, small_yland, cosine, sine, mask, dkvs, dkvr, shs, shr, szs, szr, ysems,
     yrecv) = refs.take(24)

    at.greet(everyone=True)
    w_small.over_z()
    w_small.own_block()
    for item in (w_qkv, w_out):
        item.over_z()
        item.own_block()
    my_half = cot_in.at[pl.ds(pl.multiple_of(at.y * half, SUBLANES), half)]
    sends.here(cot_in.at[pl.ds(0, half)], cot.at[at.z, 0], cot_sem.at[0])
    sends.here(cot_in.at[pl.ds(half, half)], cot.at[at.z, 1], cot_sem.at[1])
    w_small.pass_z()
    w_qkv.pass_z()
    w_out.pass_z()
    ffn[0].over_z()
    ffn[1].over_z()
    for item in ffn:
        item.own_block()

    hidden_f = hidden[...].astype(F32)
    factor1 = lax.rsqrt(jnp.mean(hidden_f * hidden_f, axis=1, keepdims=True) + EPSILON)
    seg = segments[...].astype(F32)
    row = lax.broadcasted_iota(jnp.int32, (rows, group_rows), 0) + at.z * rows
    col = lax.broadcasted_iota(jnp.int32, (rows, group_rows), 1)
    seg_row = jnp.sum(jnp.where(row == col, seg, 0.0), axis=1, keepdims=True)
    earlier = jnp.sum(jnp.where(seg < seg_row, 1.0, 0.0), axis=1, keepdims=True)
    mask[...] = jnp.where((seg == seg_row) & (col <= row), 1.0, 0.0)
    position = row[:, :1].astype(F32) - earlier
    lane = lax.broadcasted_iota(jnp.int32, (1, HD), 1)
    pair = lax.rem(lane, HD // 2).astype(F32)
    angle = position * jnp.exp(pair * (-2.0 * math.log(THETA) / HD))
    cosine[...] = jnp.cos(angle)
    sine[...] = jnp.sin(angle) * jnp.where(lane < HD // 2, -1.0, 1.0)
    w_small.pass_s()
    w_qkv.pass_s()
    w_out.pass_s()
    w_small.finish()
    gains = whole_lines(small, ns * nz, depth)
    normed1_b[...] = (hidden[...].astype(F32) * factor1 * gains[0:1, :]).astype(BF16)
    width_each = HD // (ns * nz)
    lane = lax.broadcasted_iota(jnp.int32, (8, LANES), 1)
    bias = jnp.zeros((8, LANES), F32)
    for b in range(ns * nz):
        line = small[b, 8:16, :].astype(F32)
        moved = pltpu.roll(line, b * width_each, 1) if b else line
        bias = jnp.where((lane >= b * width_each) & (lane < (b + 1) * width_each), moved, bias)
    w_qkv.finish()
    cos_t, sin_t = cosine[...], sine[...]

    def projected(head):
        weight = wa[:, :, head * HD:(head + 1) * HD].reshape(width, HD)
        return jnp.dot(normed1_b[...], weight, preferred_element_type=F32) + bias[head:head + 1, :]

    def rotated(values):
        return values * cos_t + pltpu.roll(values, HD // 2, 1) * sin_t

    for j in range(kv):
        kv_all[at.z, :, j * HD:(j + 1) * HD] = rotated(projected(heads + j)).astype(BF16)
        kv_all[at.z, :, (kv + j) * HD:(kv + j + 1) * HD] = projected(heads + kv + j).astype(BF16)
    for there, z2 in at.near():
        sends.go(
            kv_all.at[at.z], kv_all.at[at.z], kvs.at[z2], kvr.at[at.z], only=there, context=z2
        )
    ffn[2].over_z()
    t_cot.over_z(my_half)
    for h in range(heads):
        query[:, h * HD:(h + 1) * HD] = rotated(projected(h)).astype(BF16)
    ffn[0].pass_z()
    ffn[1].pass_z()
    for d in range(1, nz):
        z1 = at.z_from(d)
        landed(kv_all.at[z1], kvs.at[z1], kvr.at[z1], context=z1)

    def keys_of(j):
        return kv_all[:, :, j * HD:(j + 1) * HD].reshape(group_rows, HD)

    keep = mask[...] > 0
    for h in range(heads):
        keys, values = keys_of(h // repeat), keys_of(kv + h // repeat)
        scores = turn_last(query[:, h * HD:(h + 1) * HD], keys)
        scores = jnp.where(keep, scores * scale, -1e30)
        peak = jnp.max(scores, axis=1, keepdims=True)
        lse = peak + jnp.log(jnp.sum(jnp.exp(scores - peak), axis=1, keepdims=True))
        p = jnp.exp(scores - lse)
        probs[h * rows:(h + 1) * rows, :] = p
        out = jnp.dot(p.astype(BF16), values, preferred_element_type=F32)
        attn[:, h * HD:(h + 1) * HD] = out.astype(BF16)
    w_out.finish()
    out_w = wa[:, :, qkv_cols:qkv_cols + q_cols].reshape(width, q_cols)
    part = turn_last(attn[...], out_w).astype(BF16)
    ypart[0] = part[:half]
    ypart[1] = part[half:]
    sends.go(ypart.at[at.twin], yland, yps, ypr, tensor=at.twin)
    ffn[0].pass_s()

    landed(yland, yps, ypr, tensor=at.twin)
    base = pl.multiple_of(at.y * half, SUBLANES)
    total = ypart[at.y].astype(F32) + yland[...].astype(F32)
    res = hidden[pl.ds(base, half), :].astype(F32) + total
    resid[...] = res
    factor2 = lax.rsqrt(jnp.mean(res * res, axis=1, keepdims=True) + EPSILON)
    n2[at.z, at.y] = (res * factor2 * gains[1:2, :]).astype(BF16)
    t_n2.over_z(n2.at[at.z, at.y])
    t_n2.over_y(at.z, n2.at[at.z, at.y])
    ffn[1].pass_s()
    ffn[2].pass_z()
    t_cot.pass_z()
    t_n2.pass_z([1])
    ffn[2].pass_s()
    t_cot.wait_y(range(nz), lambda z1: at.z != z1)
    for item in ffn:
        item.finish()
    for copy in sends.local:
        copy.wait()
    sends.local = []

    def weight(ref):
        return ref[...].reshape(width, -1)

    d_act[...] = jnp.dot(cot[...].reshape(group_rows, width), weight(down_w), preferred_element_type=F32)
    few, tall = nz // 2, 32
    chunk = few * rows

    def half_block(first):
        t_n2.wait_y([first * few + i for i in range(few)])
        start = pl.multiple_of(first * chunk, chunk)
        mine = n2[pl.ds(first * few, few)].reshape(chunk, width)
        gate[...] = jnp.dot(mine, weight(gate_w), preferred_element_type=F32)
        up_val[...] = jnp.dot(mine, weight(up_w), preferred_element_type=F32)

        @pl.loop(0, chunk // tall)
        def _(i):
            line = pl.ds(pl.multiple_of(i * tall, tall), tall)
            whole = pl.ds(pl.multiple_of(start + i * tall, tall), tall)
            g, u, d = gate[line, :], up_val[line, :], d_act[whole, :]
            sigma = jax.nn.sigmoid(g)
            silu_val = g * sigma
            act[whole, :] = (silu_val * u).astype(BF16)
            d_gate[whole, :] = (d * u * sigma * (1.0 + g * (1.0 - sigma))).astype(BF16)
            d_up[whole, :] = (d * silu_val).astype(BF16)

        span = pl.ds(start, chunk)
        dn2_part[pl.ds(first * few, few)] = (
            turn_last(d_gate[span, :], weight(gate_w)) + turn_last(d_up[span, :], weight(up_w))
        ).astype(BF16).reshape(few, 2, half, width)
        r_dn2.over_y([first * few + i for i in range(few)])

    nearer = lax.div(at.z, few)
    t_n2.pass_z(range(2, nz - 1))
    half_block(nearer)
    t_n2.pass_z([nz - 1])
    half_block(1 - nearer)
    w_sends.drain()

    rets[0].give_all()
    rets[0].over_s()
    r_dn2.pass_y(far_first(nz))
    rets[0].over_z(last=False)
    rets[1].give_all()
    rets[1].over_s()
    res = resid[...]
    factor2 = lax.rsqrt(jnp.mean(res * res, axis=1, keepdims=True) + EPSILON)
    unit2 = res * factor2
    dn2 = r_dn2.total()
    grad_g2 = jnp.sum(dn2 * unit2, axis=0, keepdims=True)
    scaled = dn2 * gains[1:2, :]
    back2 = factor2 * (scaled - unit2 * jnp.mean(scaled * unit2, axis=1, keepdims=True))
    d_res = cot[at.z, at.y].astype(F32) + back2
    d_resid_f[at.y] = d_res
    d_resid_b[at.y] = d_res.astype(BF16)
    mine_b, mine_f = d_resid_b.at[at.y], d_resid_f.at[at.y]
    sends.go(mine_b, mine_b, ysems.at[0], yrecv.at[0], tensor=at.twin)
    ffn_part[...] = turn_last(act[...], weight(down_w)).astype(BF16).reshape(nz, 2, half, width)
    rets[2].give_all()
    rets[2].over_s()
    landed(d_resid_b.at[at.twin], ysems.at[0], yrecv.at[0], tensor=at.twin)
    r_ffn.over_y(far_first(nz))
    sends.go(mine_f, mine_f, ysems.at[1], yrecv.at[1], tensor=at.twin)

    d_resid_all = d_resid_b[...].reshape(rows, width)
    out_w = wa[:, :, qkv_cols:qkv_cols + q_cols].reshape(width, q_cols)
    d_attn[...] = jnp.dot(d_resid_all, out_w, preferred_element_type=F32).astype(BF16)
    r_out.give_all()
    r_out.over_s()

    def unrotated(values):
        return values * cos_t - pltpu.roll(values, HD // 2, 1) * sin_t

    bias_rows = [None] * (heads + 2 * kv)

    def place(head, grad):
        bias_rows[head] = jnp.sum(grad, axis=0, keepdims=True)
        d_projb[:, head * HD:(head + 1) * HD] = grad.astype(BF16)

    for j in range(kv):
        keys, values = keys_of(j), keys_of(kv + j)
        d_values = jnp.zeros((group_rows, HD), F32)
        d_keys = jnp.zeros((group_rows, HD), F32)
        for h in range(j * repeat, (j + 1) * repeat):
            d_out = d_attn[:, h * HD:(h + 1) * HD]
            p = probs[h * rows:(h + 1) * rows, :]
            d_prob = turn_last(d_out, values)
            delta = jnp.sum(
                d_out.astype(F32) * attn[:, h * HD:(h + 1) * HD].astype(F32), axis=1, keepdims=True
            )
            d_score[...] = (p * (d_prob - delta)).astype(BF16)
            d_query = jnp.dot(d_score[...], keys, preferred_element_type=F32)
            place(h, unrotated(d_query * scale))
            d_keys = d_keys + turn_first(d_score[...], query[:, h * HD:(h + 1) * HD])
            d_values = d_values + turn_first(p.astype(BF16), d_out)
        for i, grad in ((j, d_keys * scale), (kv + j, d_values)):
            dkv[:, :, i * HD:(i + 1) * HD] = grad.astype(BF16).reshape(nz, rows, HD)
    for there, z2 in at.near():
        sends.go(dkv.at[z2], dkv_land.at[at.z], dkvs.at[z2], dkvr.at[at.z], only=there, context=z2)
    rets[0].over_z(first=False)
    rets[1].over_z(last=False)
    d_own = dkv[at.z].astype(F32)
    for d in range(1, nz):
        z1 = at.z_from(d)
        landed(dkv_land.at[z1], dkvs.at[z1], dkvr.at[z1], context=z1)
        d_own = d_own + dkv_land[z1].astype(F32)
    for j in range(kv):
        place(heads + j, unrotated(d_own[:, j * HD:(j + 1) * HD]))
        place(heads + kv + j, d_own[:, (kv + j) * HD:(kv + j + 1) * HD])
    qkv_w = wa[:, :, :qkv_cols].reshape(width, qkv_cols)
    dn1_part[...] = turn_last(d_projb[...], qkv_w).astype(BF16)
    sends.go(dn1_part, dn1_land, ysems.at[2], yrecv.at[2], tensor=at.twin)
    r_qkv.give_all()
    r_qkv.over_s()
    rets[1].over_z(first=False)
    r_ffn.pass_y(far_first(nz))
    rets[2].over_z(last=False)
    r_out.over_z()

    block_out[at.y] = (r_ffn.total() + resid[...]).astype(BF16)
    sends.go(block_out.at[at.y], block_out.at[at.y], ysems.at[3], yrecv.at[3], tensor=at.twin)

    landed(dn1_land, ysems.at[2], yrecv.at[2], tensor=at.twin)
    landed(d_resid_f.at[at.twin], ysems.at[1], yrecv.at[1], tensor=at.twin)
    dn1 = dn1_part[...].astype(F32) + dn1_land[...].astype(F32)
    hidden_f = hidden[...].astype(F32)
    factor1 = lax.rsqrt(jnp.mean(hidden_f * hidden_f, axis=1, keepdims=True) + EPSILON)
    unit1 = hidden_f * factor1
    row = lax.broadcasted_iota(jnp.int32, (rows, 1), 0)
    my_row = (row >= at.y * half) & (row < (at.y + 1) * half)
    grad_g1 = jnp.sum(jnp.where(my_row, dn1 * unit1, 0.0), axis=0, keepdims=True)
    scaled = dn1 * gains[0:1, :]
    back1 = factor1 * (scaled - unit1 * jnp.mean(scaled * unit1, axis=1, keepdims=True))
    input_grad[...] = d_resid_f[...].reshape(rows, width) + back1

    both = jnp.concatenate([grad_g1, grad_g2, jnp.zeros((6, width), F32)], axis=0)
    bias = jnp.concatenate(bias_rows, axis=0)
    for b in range(ns * nz):
        moved = pltpu.roll(bias, LANES - b * width_each, 1) if b else bias
        small_b[b // nz, b % nz] = jnp.concatenate([piece_of_lines(both, b, depth), moved], axis=0)
    for k in range(1, ns):
        s2 = lax.rem(at.s + k, ns)
        sends.go(small_b.at[s2], small_land.at[k], shs.at[k], shr.at[k], shard=s2)
    rets[2].over_z(first=False)
    total = small_b[at.s]
    for k in range(1, ns):
        s1 = lax.rem(at.s - k + ns, ns)
        landed(small_land.at[k], shs.at[k], shr.at[k], shard=s1)
        total = total + small_land[k]
    small_z[...] = total
    for d in range(1, nz):
        sends.go(small_z.at[at.z_to(d)], small_zland.at[d], szs.at[d], szr.at[d], context=at.z_to(d))
    r_qkv.over_z()
    total = small_z[at.z]
    for d in range(1, nz):
        landed(small_zland.at[d], szs.at[d], szr.at[d], context=at.z_from(d))
        total = total + small_zland[d]
    small_y[...] = total
    sends.go(small_y, small_yland, ysems.at[4], yrecv.at[4], tensor=at.twin)
    out_grad[...] = r_out.chain.total(r_out.piece(at.z)[...].astype(F32))
    qkv_grad[...] = r_qkv.chain.total(r_qkv.piece(at.z)[...].astype(F32))
    landed(small_yland, ysems.at[4], yrecv.at[4], tensor=at.twin)
    small_out[:8, :] = small_y[:8, :] + small_yland[:8, :]
    small_out[8:, :] = small_y[8:, :]
    landed(block_out.at[at.twin], ysems.at[3], yrecv.at[3], tensor=at.twin)
    for ret in rets:
        ret.finish()
    sends.drain()


def layer(ns, nz, heads, kv, hidden_units, qkv_in, out_in, small_in, ffn_in, hidden, cot, segments):
    rows, width = hidden.shape
    owners, half, group_rows = ns * nz, rows // 2, nz * rows
    depth, cols = qkv_in.shape[0], qkv_in.shape[1] + out_in.shape[1]
    unit = ffn_in[0].shape[2]
    q_cols, kv_cols = heads * HD, 2 * kv * HD
    qkv_cols = q_cols + kv_cols
    dma = pltpu.SemaphoreType.DMA
    shape = jax.ShapeDtypeStruct
    room = pltpu.VMEM
    vmem = pl.BlockSpec(memory_space=pltpu.VMEM)
    anyspace = pl.BlockSpec(memory_space=pl.ANY)
    scratch = [room((ns, nz * depth, cols), BF16)] + [room((ns, nz * depth, unit), BF16)] * 3
    scratch += [
        room((owners, 16, LANES), BF16),
        room((2, half, width), BF16),
        room((half, width), BF16),
        room((nz, 2, half, width), BF16),
        room((nz, 2, half, width), BF16),
        room((half, width), F32),
        room((rows, q_cols), BF16),
        room((nz, rows, kv_cols), BF16),
        room((heads * rows, group_rows), F32),
        room((rows, q_cols), BF16),
    ]
    scratch += Spread.sems(ns, nz) * 6 + Tokens.sems(nz) * 2
    scratch += [dma((nz,)), dma((nz,)), dma, dma, dma((2,))]
    scratch += [room((group_rows // 2, unit), F32)] * 2 + [room((group_rows, unit), F32)]
    scratch += [room((group_rows, unit), BF16)] * 3 + [room((nz, 2, half, width), BF16)] * 2
    scratch += [
        room((rows, width), BF16), room((2, half, width), BF16), room((rows, qkv_cols), BF16),
    ]
    for _ in range(3):
        scratch += Return.lands(ns, nz, depth, unit) + Return.sems(ns, nz)
    for n in (qkv_cols, q_cols):
        scratch += Return.lands(ns, nz, depth, n) + Return.sems(ns, nz)
        scratch += ChainSum.bufs(nz, (depth, n))[1:] + ChainSum.sems(nz)
    for _ in range(2):
        scratch += Reduce.bufs(nz, half, width) + Reduce.sems(nz)
    scratch += [
        room((2, half, width), F32),
        room((rows, q_cols), BF16),
        room((rows, group_rows), BF16),
        room((nz, rows, kv_cols), BF16),
        room((nz, rows, kv_cols), BF16),
        room((rows, width), BF16),
        room((rows, width), BF16),
        room((ns, nz, 16, LANES), F32),
        room((ns, nz, 16, LANES), F32),
        room((nz, 16, LANES), F32),
        room((nz, 16, LANES), F32),
        room((16, LANES), F32),
        room((16, LANES), F32),
        room((rows, HD), F32),
        room((rows, HD), F32),
        room((rows, group_rows), F32),
        dma((nz,)), dma((nz,)), dma((ns,)), dma((ns,)), dma((nz,)), dma((nz,)), dma((5,)), dma((5,)),
    ]
    return pl.pallas_call(
        functools.partial(layer_kernel, ns, nz, heads, kv),
        out_shape=[
            shape((2, half, width), BF16),
            shape((rows, width), F32),
            shape((depth, qkv_cols), F32),
            shape((depth, q_cols), F32),
            shape((16, LANES), F32),
            *[shape((depth, hidden_units), BF16)] * 3,
        ],
        in_specs=[anyspace] * 6 + [vmem, anyspace, vmem],
        out_specs=[vmem] * 5 + [anyspace] * 3,
        scratch_shapes=scratch,
        compiler_params=pltpu.CompilerParams(
            collective_id=0, has_side_effects=True, vmem_limit_bytes=VMEM_BYTES
        ),
    )(qkv_in, out_in, small_in, *ffn_in, hidden, cot, segments)


def fast_step(
    ns,
    nz,
    hidden_in,
    segment_ids,
    attn_gain,
    qkv_weight,
    qkv_bias,
    out_weight,
    ffn_gain,
    gate_weight,
    up_weight,
    down_weight,
    out_cotangent,
):
    rows, width = hidden_in.shape
    depth, hidden_units = gate_weight.shape
    parts = 2
    heads = H // parts
    kv = KVH // parts
    unit_cols = -(-hidden_units // (nz * LANES)) * LANES
    padded = unit_cols * nz

    def by_place(weight):
        full = jnp.pad(weight, ((0, 0), (0, padded - hidden_units)))
        return jnp.transpose(full.reshape(depth, nz, unit_cols), (1, 0, 2))

    ffn_in = [by_place(w) for w in (gate_weight, up_weight, down_weight.T)]
    gains_in = jnp.pad(jnp.stack([attn_gain, ffn_gain]), ((0, 6), (0, LANES - depth)))
    bias_in = jnp.pad(qkv_bias, ((0, 0), (0, LANES - qkv_bias.shape[1])))
    small_in = jnp.concatenate([gains_in, bias_in], axis=0)

    block_out, input_grad, grad_qkv, grad_out, small, grad_gate, grad_up, grad_down = layer(
        ns, nz, heads, kv, hidden_units, qkv_weight, out_weight.T, small_in, ffn_in, hidden_in,
        out_cotangent, segment_ids,
    )

    return (
        block_out.reshape(rows, width),
        input_grad,
        small[0, :depth],
        grad_qkv,
        small[8:, : qkv_bias.shape[1]],
        grad_out.T,
        small[1, :depth],
        grad_gate.astype(F32),
        grad_up.astype(F32),
        grad_down.astype(F32).T,
    )


def general_step(
    hidden_in,
    segment_ids,
    attn_gain,
    qkv_weight,
    qkv_bias,
    out_weight,
    ffn_gain,
    gate_weight,
    up_weight,
    down_weight,
    out_cotangent,
):
    rows, width = hidden_in.shape
    depth = gate_weight.shape[0]
    hidden_units = gate_weight.shape[1]
    parts = lax.axis_size("tensor")
    blocks = lax.axis_size("context")
    heads = H // parts
    kv = KVH // parts
    repeat = H // KVH
    scale = HD ** (-0.5)
    block_index = lax.axis_index("context")
    part_index = lax.axis_index("tensor")
    half_rows = rows // parts
    unit_cols = -(-hidden_units // (blocks * LANES)) * LANES
    padded = unit_cols * blocks

    def spread(weight):
        full = jnp.pad(weight, ((0, 0), (0, padded - hidden_units)))
        mine = lax.all_to_all(full, "context", split_axis=1, concat_axis=0, tiled=True)
        mine = mine.reshape(blocks * depth, unit_cols)
        return lax.all_gather(mine, "shard", axis=0, tiled=True)

    gate_full = spread(gate_weight)
    up_full = spread(up_weight)
    down_full = spread(down_weight.T)
    gain_one = lax.all_gather(attn_gain, OWNERS, axis=0, tiled=True).astype(F32)
    gain_two = lax.all_gather(ffn_gain, OWNERS, axis=0, tiled=True).astype(F32)
    bias = lax.all_gather(qkv_bias, OWNERS, axis=1, tiled=True).reshape(-1).astype(F32)
    qkv_full = lax.all_gather(qkv_weight, OWNERS, axis=0, tiled=True)
    out_full = lax.all_gather(out_weight.T, OWNERS, axis=0, tiled=True)

    seg_all = segment_ids[0]
    group_rows = seg_all.shape[0]
    first_row = block_index * rows
    index_all = jnp.arange(group_rows, dtype=jnp.int32)
    earlier = jnp.sum((seg_all[None, :] < seg_all[:, None]).astype(jnp.int32), axis=1)
    positions = index_all - earlier
    seg_local = lax.dynamic_slice_in_dim(seg_all, first_row, rows)
    index_local = first_row + jnp.arange(rows, dtype=jnp.int32)
    allowed = (seg_local[:, None] == seg_all[None, :]) & (
        index_local[:, None] >= index_all[None, :]
    )
    cosine, sine = rotary_tables(positions)
    cos_local = lax.dynamic_slice_in_dim(cosine, first_row, rows)
    sin_local = lax.dynamic_slice_in_dim(sine, first_row, rows)

    hidden_all = lax.all_gather(hidden_in, "context", axis=0, tiled=True)
    normed_all, _, _ = norm_forward(hidden_all.astype(F32), gain_one)
    hidden_f = hidden_in.astype(F32)
    normed1, unit1, factor1 = norm_forward(hidden_f, gain_one)
    q_cols = heads * HD
    k_cols = kv * HD
    query_f = dot(normed1, qkv_full[:, :q_cols]) + bias[:q_cols]
    kv_f = dot(normed_all, qkv_full[:, q_cols:]) + bias[q_cols:]
    query = jnp.transpose(query_f.reshape(rows, heads, HD), (1, 0, 2))
    query = rotate(query, cos_local, sin_local).astype(BF16)
    keys = jnp.transpose(kv_f[:, :k_cols].reshape(group_rows, kv, HD), (1, 0, 2))
    keys = rotate(keys, cosine, sine).astype(BF16)
    values = jnp.transpose(kv_f[:, k_cols:].reshape(group_rows, kv, HD), (1, 0, 2)).astype(BF16)
    query = query.reshape(kv, repeat * rows, HD)
    mask = jnp.tile(allowed, (repeat, 1))
    scores = jnp.where(mask, batched(query, keys, 2, 2) * scale, -1e30)
    peak = jnp.max(scores, axis=2, keepdims=True)
    lse = peak + jnp.log(jnp.sum(jnp.exp(scores - peak), axis=2, keepdims=True))
    p_soft = jnp.exp(scores - lse)
    probs = p_soft.astype(BF16)
    outs = batched(probs, values, 2, 1).astype(BF16)
    attn = jnp.transpose(outs.reshape(heads, rows, HD), (1, 0, 2)).reshape(rows, q_cols)
    attn_part = contract_last(attn, out_full).astype(BF16)

    mine = part_index * half_rows
    attn_half = lax.psum_scatter(attn_part, "tensor", scatter_dimension=0, tiled=True)
    resid_half = lax.dynamic_slice_in_dim(hidden_f, mine, half_rows) + attn_half.astype(F32)
    normed2_half, unit2, factor2 = norm_forward(resid_half, gain_two)
    normed2 = lax.all_gather(normed2_half, TEAM, axis=0, tiled=True)
    cot_half = lax.dynamic_slice_in_dim(out_cotangent, mine, half_rows)
    cot = lax.all_gather(cot_half, TEAM, axis=0, tiled=True)

    gate = dot(normed2, gate_full)
    up_val = dot(normed2, up_full)
    sigma = jax.nn.sigmoid(gate)
    silu_val = gate * sigma
    act = (silu_val * up_val).astype(BF16)
    ffn_part = contract_last(act, down_full).astype(BF16)
    d_act = dot(cot, down_full)
    d_gate = (d_act * up_val * sigma * (1.0 + gate * (1.0 - sigma))).astype(BF16)
    d_up = (d_act * silu_val).astype(BF16)
    dn2_part = (contract_last(d_gate, gate_full) + contract_last(d_up, up_full)).astype(BF16)
    ffn_half = lax.psum_scatter(ffn_part, TEAM, scatter_dimension=0, tiled=True)
    block_half = (resid_half + ffn_half.astype(F32)).astype(BF16)
    block_out = lax.all_gather(block_half, "tensor", axis=0, tiled=True)
    dn2_half = lax.psum_scatter(dn2_part, TEAM, scatter_dimension=0, tiled=True).astype(F32)
    grad_g2, d_back2 = norm_backward(dn2_half, unit2, factor2, gain_two)
    d_resid_half = cot_half.astype(F32) + d_back2

    def give_back(grad):
        part = lax.psum_scatter(grad.astype(BF16), "shard", scatter_dimension=0, tiled=True)
        part = part.reshape(blocks, depth, unit_cols)
        part = lax.all_to_all(part, "context", split_axis=0, concat_axis=2, tiled=True)
        return part.reshape(depth, padded)[:, :hidden_units].astype(F32)

    sum_gate = give_back(contract_first(normed2, d_gate))
    sum_up = give_back(contract_first(normed2, d_up))
    sum_down = give_back(contract_first(cot, act)).T

    d_resid_b = lax.all_gather(d_resid_half.astype(BF16), "tensor", axis=0, tiled=True)
    grad_out = contract_first(d_resid_b, attn)
    d_attn = dot(d_resid_b, out_full).astype(BF16)
    d_outs = jnp.transpose(d_attn.reshape(rows, heads, HD), (1, 0, 2)).reshape(
        kv, repeat * rows, HD
    )
    d_prob = batched(d_outs, values, 2, 2)
    delta = jnp.sum(d_outs.astype(F32) * outs.astype(F32), axis=2, keepdims=True)
    d_score = (p_soft * (d_prob - delta)).astype(BF16)
    d_query = batched(d_score, keys, 2, 1) * scale
    d_keys = batched(d_score, query, 1, 1) * scale
    d_values = batched(probs, d_outs, 1, 1)
    d_kv = jnp.concatenate([d_keys, d_values], axis=0).astype(BF16)
    d_kv = lax.psum_scatter(d_kv, "context", scatter_dimension=1, tiled=True).astype(F32)
    d_query = unrotate(d_query.reshape(heads, rows, HD), cos_local, sin_local)
    d_keys = unrotate(d_kv[:kv], cos_local, sin_local)
    d_proj = jnp.transpose(jnp.concatenate([d_query, d_keys, d_kv[kv:]], axis=0), (1, 0, 2))
    grad_bias = jnp.sum(d_proj, axis=0)
    d_projb = d_proj.reshape(rows, -1).astype(BF16)
    grad_qkv = contract_first(normed1, d_projb)
    dn1_part = contract_last(d_projb, qkv_full).astype(BF16)
    dn1_half = lax.psum_scatter(dn1_part, "tensor", scatter_dimension=0, tiled=True).astype(F32)
    unit1_half = lax.dynamic_slice_in_dim(unit1, mine, half_rows)
    factor1_half = lax.dynamic_slice_in_dim(factor1, mine, half_rows)
    grad_g1, d_back1 = norm_backward(dn1_half, unit1_half, factor1_half, gain_one)
    input_grad = lax.all_gather(d_resid_half + d_back1, "tensor", axis=0, tiled=True)

    gains = lax.psum(jnp.stack([grad_g1, grad_g2]), "tensor")
    sum_gains = lax.psum_scatter(gains, OWNERS, scatter_dimension=1, tiled=True)
    sum_qkv = lax.psum_scatter(grad_qkv.astype(BF16), OWNERS, scatter_dimension=0, tiled=True)
    sum_bias = lax.psum_scatter(grad_bias, OWNERS, scatter_dimension=1, tiled=True)
    sum_out = lax.psum_scatter(grad_out.astype(BF16), OWNERS, scatter_dimension=0, tiled=True)
    return (
        block_out,
        input_grad,
        sum_gains[0],
        sum_qkv.astype(F32),
        sum_bias,
        sum_out.astype(F32).T,
        sum_gains[1],
        sum_gate,
        sum_up,
        sum_down,
    )


def solution(mesh):
    ns, nz, parts = (mesh.shape[a] for a in ("shard", "context", "tensor"))
    rows = P(OWNERS, None)

    def local(*args):
        depth = args[7].shape[0]
        if depth % SUBLANES == 0 and ns % 2 == 0 and ns > 2 and nz % 2 == 0 and parts == 2:
            return fast_step(ns, nz, *args)
        return general_step(*args)

    placed = (
        rows,
        P("shard", None),
        P(OWNERS),
        P(OWNERS, "tensor"),
        P("tensor", OWNERS),
        P("tensor", OWNERS),
        P(OWNERS),
        P(OWNERS, "tensor"),
        P(OWNERS, "tensor"),
        P("tensor", OWNERS),
        rows,
    )
    return jax.shard_map(
        local,
        mesh=mesh,
        in_specs=placed,
        out_specs=(
            rows,
            rows,
            P(OWNERS),
            P(OWNERS, "tensor"),
            P("tensor", OWNERS),
            P("tensor", OWNERS),
            P(OWNERS),
            P(OWNERS, "tensor"),
            P(OWNERS, "tensor"),
            P("tensor", OWNERS),
        ),
        check_vma=False,
    )
```

```python
import functools
import math

import jax
import jax.numpy as jnp
from jax import lax
from jax.experimental import pallas as pl
from jax.experimental.pallas import tpu as pltpu
from jax.sharding import PartitionSpec as P

H = 12
KVH = 2
HD = 128
LANES = 128
SUBLANES = 16
BF16 = jnp.bfloat16
F32 = jnp.float32

EPSILON = 1e-06
THETA = 1000000.0

OWNERS = ("shard", "context")
TEAM = ("context", "tensor")
MESH = pl.DeviceIdType.MESH
VMEM_BYTES = 62 * 1024 * 1024


def dot(left, right):
    return jnp.dot(left, right, preferred_element_type=F32)


def contract_last(left, right):
    return lax.dot_general(left, right, (((1,), (1,)), ((), ())), preferred_element_type=F32)


def contract_first(left, right):
    return lax.dot_general(left, right, (((0,), (0,)), ((), ())), preferred_element_type=F32)


def batched(left, right, left_dim, right_dim):
    return lax.dot_general(
        left, right, (((left_dim,), (right_dim,)), ((0,), (0,))), preferred_element_type=F32
    )


def norm_forward(values, gain):
    factor = lax.rsqrt(jnp.mean(values * values, axis=1, keepdims=True) + EPSILON)
    unit = values * factor
    return ((unit * gain).astype(BF16), unit, factor)


def norm_backward(grad_out, unit, factor, gain):
    gain_grad = jnp.sum(grad_out * unit, axis=0)
    scaled = grad_out * gain
    return (gain_grad, factor * (scaled - unit * jnp.mean(scaled * unit, axis=1, keepdims=True)))


def rotary_tables(positions):
    half = HD // 2
    freqs = THETA ** (-(2.0 * jnp.arange(half, dtype=F32)) / HD)
    angles = positions.astype(F32)[:, None] * freqs[None, :]
    cosine, sine = jnp.cos(angles), jnp.sin(angles)
    return (
        jnp.concatenate([cosine, cosine], axis=1),
        jnp.concatenate([-sine, sine], axis=1),
    )


def swap_halves(values):
    half = values.shape[-1] // 2
    return jnp.concatenate([values[..., half:], values[..., :half]], axis=-1)


def rotate(values, cosine, sine):
    return values * cosine + swap_halves(values) * sine


def unrotate(values, cosine, sine):
    return values * cosine - swap_halves(values) * sine


class Place:
    def __init__(self, ns, nz):
        self.ns, self.nz, self.no = ns, nz, ns // 2
        self.s, self.z, self.y = (lax.axis_index(a) for a in ("shard", "context", "tensor"))
        self.core = lax.rem(self.s, 2)
        self.outer = lax.div(self.s, 2)
        self.mate = self.s + 1 - 2 * self.core
        self.twin = 1 - self.y

    def z_to(self, d):
        return lax.rem(self.z + d, self.nz)

    def z_from(self, d):
        return lax.rem(self.z - d + self.nz, self.nz)

    def near(self):
        for k in range(1, self.nz):
            yield (self.z + k < self.nz, lax.rem(self.z + k, self.nz))
            yield (self.z >= k, lax.rem(self.z - k + self.nz, self.nz))

    def s_to(self, o):
        return lax.rem(self.outer + o, self.no) * 2 + self.core

    def s_from(self, o):
        return lax.rem(self.outer - o + self.no, self.no) * 2 + self.core

    def mate_from(self, o):
        return lax.rem(self.outer - o + self.no, self.no) * 2 + 1 - self.core

    def mate_to(self, o):
        return lax.rem(self.outer + o, self.no) * 2 + 1 - self.core

    def greet(self, everyone=False):
        barrier = pltpu.get_barrier_semaphore()
        peers = [{"context": self.z_to(d)} for d in range(1, self.nz)]
        if everyone:
            peers += [{"shard": lax.rem(self.s + k, self.ns)} for k in range(1, self.ns)]
        else:
            peers += [{"shard": self.s_to(o)} for o in range(1, self.no)] + [{"shard": self.mate}]
        peers += [{"tensor": self.twin}]
        for peer in peers:
            pl.semaphore_signal(barrier, inc=1, device_id=peer, device_id_type=MESH)
        pl.semaphore_wait(barrier, len(peers))


class Sends:
    def __init__(self):
        self.remote, self.local = [], []

    def go(self, src, dst, send, recv, only=None, **peer):
        copy = pltpu.make_async_remote_copy(
            src_ref=src, dst_ref=dst, send_sem=send, recv_sem=recv,
            device_id=peer, device_id_type=MESH,
        )
        guarded(only, copy.start)
        self.remote.append((only, copy.wait_send))

    def here(self, src, dst, sem):
        copy = pltpu.make_async_copy(src, dst, sem)
        copy.start()
        self.local.append(copy)

    def drain(self):
        for only, wait in self.remote:
            guarded(only, wait)
        for copy in self.local:
            copy.wait()
        self.remote, self.local = [], []


def both(one, other):
    return other if one is None else one & other


def guarded(only, action):
    if only is None:
        action()
    else:
        pl.when(only)(action)


def landed(ref, send, recv, only=None, **peer):
    copy = pltpu.make_async_remote_copy(
        src_ref=ref, dst_ref=ref, send_sem=send, recv_sem=recv,
        device_id=peer, device_id_type=MESH,
    )
    guarded(only, copy.wait_recv)


def far_first(n):
    return [n - 1 - i // 2 if i % 2 == 0 else i // 2 for i in range(n)]


class Chain:
    def __init__(self, at, sends, ref, sems):
        self.at, self.sends, self.ref = at, sends, ref
        self.zs, self.zr = sems

    @staticmethod
    def sems(nz):
        dma = pltpu.SemaphoreType.DMA
        return [dma((2, nz)), dma((nz,))]

    def hops(self, steps=None):
        at = self.at
        for k in steps or range(1, at.nz):
            yield (-1, at.z - k >= 0, at.z - k)
            yield (1, at.z + k < at.nz, at.z + k)

    def hand(self, way, origin, src, only):
        at = self.at
        there = at.z + 1 < at.nz if way == 0 else at.z > 0
        self.sends.go(
            src, self.ref(origin), self.zs.at[way, origin], self.zr.at[origin],
            only=there if only is None else there & only, context=at.z + (1 if way == 0 else -1),
        )

    def begin(self, src):
        for way in range(2):
            self.hand(way, self.at.z, src, None)

    def step(self, side, valid, origin):
        ref = self.ref(origin)
        landed(ref, self.zs.at[0, origin], self.zr.at[origin], only=valid, context=self.at.z)
        self.hand(0 if side < 0 else 1, origin, ref, valid)
        return ref


class ChainSum:
    def __init__(self, at, sends, bufs, sems):
        self.at, self.sends = at, sends
        stage, self.land = bufs
        self.stage = stage if callable(stage) else lambda z2: stage.at[z2]
        self.zs, self.zr = sems

    @staticmethod
    def sems(nz):
        dma = pltpu.SemaphoreType.DMA
        return [dma((nz,)), dma((nz + 1,))]

    @staticmethod
    def bufs(nz, shape, dtype=BF16):
        return [pltpu.VMEM((nz, *shape), dtype), pltpu.VMEM((nz + 1, *shape), dtype)]

    def put(self, z2, own):
        at = self.at
        stage, dtype = self.stage(z2), self.land.dtype

        def start(slot, before):
            slot_ref = self.land.at[z2]

            @pl.when(before)
            def _():
                landed(slot_ref, self.zs.at[z2], self.zr.at[z2], context=at.z)
                stage[...] = (own() + self.land[z2].astype(F32)).astype(dtype)

            @pl.when(jnp.logical_not(before))
            def _():
                stage[...] = own().astype(dtype)

            pltpu.make_async_remote_copy(
                src_ref=stage, dst_ref=self.land.at[slot], send_sem=self.zs.at[z2],
                recv_sem=self.zr.at[slot], device_id={"context": at.z + (1 if z2_right else -1)},
                device_id_type=MESH,
            ).start()

        for z2_right in (True, False):
            away = at.z < z2 if z2_right else at.z > z2

            @pl.when(away)
            def _(z2_right=z2_right):
                near = at.z + 1 == z2 if z2_right else at.z - 1 == z2
                slot = z2 if z2_right else z2 + near * (at.nz - z2)
                before = at.z > 0 if z2_right else at.z + 1 < at.nz
                start(slot, before)

        self.sends.remote.append((
            at.z != z2,
            lambda: pltpu.make_async_remote_copy(
                src_ref=stage, dst_ref=self.land.at[z2], send_sem=self.zs.at[z2],
                recv_sem=self.zr.at[z2], device_id={"context": at.z}, device_id_type=MESH,
            ).wait_send(),
        ))

    def total(self, own):
        at = self.at
        total = own
        for slot, there in ((at.z, at.z > 0), (at.nz, at.z + 1 < at.nz)):
            landed(self.land.at[slot], self.zs.at[0], self.zr.at[slot], only=there, context=at.z)
            total = total + jnp.where(there, self.land[slot].astype(F32), 0.0)
        return total


class Spread:
    def __init__(self, at, sends, src, dst, sems, same=False):
        self.at, self.sends, self.src, self.dst = at, sends, src, dst
        self.copy = None
        self.own, self.zs, self.zr, self.xs, self.xr, self.cs, self.cr, *chain = sems
        self.chain = Chain(at, sends, lambda z1: dst(at.s, z1), chain) if same else None

    @staticmethod
    def sems(ns, nz):
        dma, no = pltpu.SemaphoreType.DMA, ns // 2
        return [
            dma, dma((nz,)), dma((nz,)), dma((nz, no)), dma((nz, no)), dma((no, nz)), dma((no, nz)),
        ] + Chain.sems(nz)

    def over_z(self):
        at = self.at
        if self.chain is not None:
            self.chain.begin(self.src(at.z))
            return
        for there, z2 in at.near():
            self.sends.go(
                self.src(z2), self.dst(at.s, at.z), self.zs.at[z2], self.zr.at[at.z], only=there,
                context=z2,
            )

    def over_s(self, z1, ref, only=None):
        at = self.at
        for o in range(1, at.no):
            self.sends.go(
                ref, self.dst(at.s, z1), self.xs.at[z1, o], self.xr.at[z1, o], only=only,
                shard=at.s_to(o),
            )
        self.sends.go(
            ref, self.dst(at.s, z1), self.cs.at[0, z1], self.cr.at[0, z1], only=only, shard=at.mate
        )

    def own_block(self):
        at = self.at
        self.over_s(at.z, self.src(at.z))
        self.copy = pltpu.make_async_copy(self.src(at.z), self.dst(at.s, at.z), self.own)
        self.copy.start()

    def pass_z(self, steps=None):
        at = self.at
        if self.chain is not None:
            for side, valid, z1 in self.chain.hops(steps):
                self.over_s(z1, self.chain.step(side, valid, z1), only=valid)
            return
        for there, z1 in at.near():
            ref = self.dst(at.s, z1)
            landed(ref, self.zs.at[z1], self.zr.at[z1], only=there, context=z1)
            self.over_s(z1, ref, only=there)

    def pass_s(self):
        at = self.at
        for o in range(1, at.no):
            s1 = at.s_from(o)
            for d in range(at.nz):
                z1 = at.z_from(d)
                ref = self.dst(s1, z1)
                landed(ref, self.xs.at[z1, o], self.xr.at[z1, o], shard=s1)
                self.sends.go(ref, ref, self.cs.at[o, z1], self.cr.at[o, z1], shard=at.mate)

    def finish(self):
        at = self.at
        self.copy.wait()
        for o in range(at.no):
            for z1 in range(at.nz):
                ref = self.dst(at.mate_from(o), z1)
                landed(ref, self.cs.at[o, z1], self.cr.at[o, z1], shard=at.mate)

    def pass_all(self):
        self.pass_z()
        self.pass_s()


class Tokens:
    def __init__(self, at, sends, ref, sems):
        self.at, self.sends, self.ref = at, sends, ref
        self.ys, self.yr, *chain = sems
        self.chain = Chain(at, sends, lambda z1: ref.at[z1, at.y], chain)

    @staticmethod
    def sems(nz):
        dma = pltpu.SemaphoreType.DMA
        return [dma((nz,)), dma((nz,))] + Chain.sems(nz)

    def over_z(self, src):
        self.chain.begin(src)

    def over_y(self, z1, src, only=None):
        at = self.at
        self.sends.go(
            src, self.ref.at[z1, at.y], self.ys.at[z1], self.yr.at[z1], only=only, tensor=at.twin
        )

    def pass_z(self, steps=None):
        for side, valid, z1 in self.chain.hops(steps):
            self.over_y(z1, self.chain.step(side, valid, z1), only=valid)

    def wait_y(self, places, only=None):
        at = self.at
        for z1 in places:
            ref = self.ref.at[z1, at.twin]
            landed(
                ref, self.ys.at[z1], self.yr.at[z1], only=only and only(z1), tensor=at.twin
            )


def whole_lines(small, blocks, depth):
    tiles = []
    for t in range(blocks * depth // LANES):
        tile = jnp.zeros((8, LANES), F32)
        lane = lax.broadcasted_iota(jnp.int32, (8, LANES), 1) + t * LANES
        for b in range(t * LANES // depth, min(blocks, -(-(t + 1) * LANES // depth))):
            line = small[b, :8, :].astype(F32)
            shift = (b * depth - t * LANES) % LANES
            moved = pltpu.roll(line, shift, 1) if shift else line
            tile = jnp.where((lane >= b * depth) & (lane < (b + 1) * depth), moved, tile)
        tiles.append(tile)
    return jnp.concatenate(tiles, axis=1)


def turn_first(left, right):
    return lax.dot_general(left, right, (((0,), (0,)), ((), ())), preferred_element_type=F32)


def turn_last(left, right):
    return lax.dot_general(left, right, (((1,), (1,)), ((), ())), preferred_element_type=F32)


class Return:
    def __init__(self, at, sends, make, room, lands, out, sems):
        self.at, self.sends, self.make, self.out = at, sends, make, out
        self.stage, self.acc = room.at[pl.ds(0, at.no)], room.at[pl.ds(at.no, at.no)]
        self.landc, self.landx = lands
        self.cs, self.cr, self.xs, self.xr, self.zs, self.zr, self.own = sems
        self.chain, self.short = None, 0
        self.depth = self.acc.shape[1] // at.nz

    @staticmethod
    def sems(ns, nz):
        dma, no = pltpu.SemaphoreType.DMA, ns // 2
        return [
            dma((no,)), dma((no,)), dma((no, nz)), dma((no, nz)), dma((2, nz)), dma((2, nz)), dma((2,)),
        ]

    @staticmethod
    def lands(ns, nz, depth, cols):
        no = ns // 2
        return [pltpu.VMEM((n, nz * depth, cols), BF16) for n in (no, no - 1)]

    def to_mate(self, o):
        return pltpu.make_async_remote_copy(
            src_ref=self.stage.at[o], dst_ref=self.landc.at[o], send_sem=self.cs.at[o],
            recv_sem=self.cr.at[o], device_id={"shard": self.at.mate}, device_id_type=MESH,
        )

    def give_all(self):
        at = self.at

        @pl.loop(0, at.no)
        def _(i):
            o = at.no - 1 - i
            self.stage[o] = self.make(at.mate_to(o)).astype(BF16)
            self.to_mate(o).start()
            self.acc[o] = self.make(at.s_to(o)).astype(BF16)

        self.sends.remote += [(None, self.to_mate(o).wait_send) for o in range(at.no)]

    def rows(self, z2):
        start = z2 * self.depth
        start = start if isinstance(start, int) else pl.multiple_of(start, SUBLANES)
        return pl.ds(start, self.depth)

    def piece(self, z2):
        return self.acc.at[0, self.rows(z2)]

    def slots(self):
        if self.chain is not None:
            return [(None, z2) for z2 in far_first(self.at.nz)]
        return [*self.at.near(), (None, self.at.z)]

    def add(self, o, z2, others):
        line = self.rows(z2)
        total = self.acc[o, line, :].astype(F32)
        for other, k in others:
            total = total + other[k, line, :].astype(F32)
        self.acc[o, line, :] = total.astype(BF16)

    def over_s(self, first=True, last=True):
        at = self.at
        slots = self.slots()
        middle = len(slots) // 2
        slots = (slots[:middle] if first else []) + (slots[middle:] if last else [])
        for o in range(1, at.no):
            if first:
                landed(self.landc.at[o], self.cs.at[o], self.cr.at[o], shard=at.mate)
            for there, z2 in slots:
                line = self.rows(z2)
                guarded(there, lambda: self.add(o, z2, [(self.landc, o)]))
                self.sends.go(
                    self.acc.at[o, line], self.landx.at[o - 1, line], self.xs.at[o, z2],
                    self.xr.at[o, z2], only=there, shard=at.s_to(o),
                )
        if first:
            landed(self.landc.at[0], self.cs.at[0], self.cr.at[0], shard=at.mate)

    def over_z(self, first=True, last=True):
        at = self.at
        slots = self.slots()
        middle = len(slots) // 2
        slots = (slots[:middle] if first else []) + (slots[middle:] if last else [])
        for there, z2 in slots:
            line = self.rows(z2)
            for o in range(1, at.no):
                landed(
                    self.landx.at[o - 1, line], self.xs.at[o, z2], self.xr.at[o, z2], only=there,
                    shard=at.s_from(o),
                )
            terms = [(self.landc, 0)] + [(self.landx, o - 1) for o in range(1, at.no)]
            guarded(there, lambda: self.add(0, z2, terms))
            if self.chain is not None:
                self.chain.put(z2, lambda: self.piece(z2)[...].astype(F32))
                continue
            for w, (cols, whole) in enumerate(self.wings(at.z)):
                src, dst = self.piece(z2).at[:, cols], self.out(at.z, cols)
                if there is not None:
                    self.sends.go(
                        src, dst, self.zs.at[w, z2], self.zr.at[w, at.z], only=both(whole, there),
                        context=z2,
                    )
                else:
                    copy = pltpu.make_async_copy(src, dst, self.own.at[w])
                    guarded(whole, copy.start)

    def wings(self, z1):
        unit, short = self.acc.shape[2], self.short
        yield (pl.ds(0, unit - short), None)
        if short:
            yield (pl.ds(unit - short, short), z1 + 1 < self.at.nz)

    def finish(self):
        at = self.at
        for w, (cols, whole) in enumerate(self.wings(at.z)):
            copy = pltpu.make_async_copy(
                self.piece(at.z).at[:, cols], self.out(at.z, cols), self.own.at[w]
            )
            guarded(whole, copy.wait)
        for there, z1 in at.near():
            for w, (cols, whole) in enumerate(self.wings(z1)):
                landed(
                    self.out(z1, cols), self.zs.at[w, z1], self.zr.at[w, z1],
                    only=both(whole, there), context=z1,
                )


class Reduce:
    def __init__(self, at, sends, parts, bufs, sems):
        self.at, self.sends, self.parts = at, sends, parts
        self.landy, *chain = bufs
        self.ys, self.yr, *chain_sems = sems
        self.chain = ChainSum(at, sends, chain, chain_sems)

    @staticmethod
    def sems(nz):
        dma = pltpu.SemaphoreType.DMA
        return [dma((nz,)), dma((nz,))] + ChainSum.sems(nz)

    @staticmethod
    def bufs(nz, half, width):
        return [pltpu.VMEM((nz, half, width), BF16)] + ChainSum.bufs(nz, (half, width))

    def over_y(self, places):
        at = self.at
        for z2 in places:
            self.sends.go(
                self.parts.at[z2, at.twin], self.landy.at[z2], self.ys.at[z2], self.yr.at[z2],
                tensor=at.twin,
            )

    def own(self, z2):
        return self.parts[z2, self.at.y].astype(F32) + self.landy[z2].astype(F32)

    def pass_y(self, places):
        at = self.at
        for z2 in places:
            landed(self.landy.at[z2], self.ys.at[z2], self.yr.at[z2], tensor=at.twin)
            self.chain.put(z2, lambda z2=z2: self.own(z2))

    def total(self):
        return self.chain.total(self.own(self.at.z))


def piece_of_lines(lines, b, depth):
    first, off = divmod(b * depth, LANES)
    tile = lines[:, first * LANES:(first + 1) * LANES]
    if not off:
        return tile
    tile = pltpu.roll(tile, LANES - off, 1)
    if off + depth <= LANES:
        return tile
    after = pltpu.roll(lines[:, (first + 1) * LANES:(first + 2) * LANES], LANES - off, 1)
    lane = lax.broadcasted_iota(jnp.int32, (8, LANES), 1)
    return jnp.where(lane < LANES - off, tile, after)


class Refs:
    def __init__(self, refs):
        self.refs, self.next = refs, 0

    def take(self, n):
        self.next += n
        return self.refs[self.next - n:self.next]


def layer_kernel(ns, nz, heads, kv, *refs):
    refs = Refs(refs)
    (qkv_in, out_in, small_in, gate_in, up_in, down_in, hidden, cot_in, segments) = refs.take(9)
    (block_out, input_grad, qkv_grad, out_grad, small_out, *ffn_out) = refs.take(8)
    at = Place(ns, nz)
    w_sends, sends = Sends(), Sends()
    depth = qkv_in.shape[0]
    rows, width = hidden.shape
    half = rows // 2
    group_rows = nz * rows
    q_cols = heads * HD
    qkv_cols = q_cols + 2 * kv * HD
    wide = nz * depth
    scale = HD ** (-0.5)
    repeat = heads // kv

    wa, gate_w, up_w, down_w = refs.take(4)
    n_spread, n_tokens, n_ret = len(Spread.sems(ns, nz)), len(Tokens.sems(nz)), len(Return.sems(ns, nz))
    n_red, n_sum = len(Reduce.sems(nz)), len(ChainSum.sems(nz))
    (small, ypart, yland, n2, cot, resid, query, kv_all, probs, attn) = refs.take(10)

    def block(ref):
        return lambda s1, z1: ref.at[s1, pl.ds(pl.multiple_of(z1 * depth, SUBLANES), depth)]

    w_qkv, w_out = (
        Spread(at, w_sends, lambda z2, src=src: src, block(dst), refs.take(n_spread), True)
        for src, dst in (
            (qkv_in, wa.at[:, :, pl.ds(0, qkv_cols)]), (out_in, wa.at[:, :, pl.ds(qkv_cols, q_cols)]),
        )
    )
    w_small = Spread(
        at, w_sends, lambda z2: small_in, lambda s1, z1: small.at[s1 * nz + z1],
        refs.take(n_spread), True,
    )
    ffn = [
        Spread(at, w_sends, lambda z2, src=src: src.at[z2], block(dst), refs.take(n_spread))
        for src, dst in ((gate_in, gate_w), (up_in, up_w), (down_in, down_w))
    ]
    t_cot = Tokens(at, sends, cot, refs.take(n_tokens))
    t_n2 = Tokens(at, sends, n2, refs.take(n_tokens))
    kvs, kvr, yps, ypr, cot_sem = refs.take(5)
    gate, up_val, d_act, act, d_gate, d_up, ffn_part, dn2_part = refs.take(8)
    normed1_b, d_resid_b, d_projb = refs.take(3)

    def columns(ref, s1):
        return ref[..., pl.ds(pl.multiple_of(s1 * wide, LANES), wide)].reshape(-1, wide)

    unit = gate_w.shape[2]

    def out_place(ref):
        return lambda z1, cols: ref.at[
            :, pl.ds(pl.multiple_of(z1 * unit + cols.start, LANES), cols.size)
        ]

    makers = (
        lambda s1: turn_first(columns(n2, s1), d_gate[...]),
        lambda s1: turn_first(columns(n2, s1), d_up[...]),
        lambda s1: turn_first(columns(cot, s1), act[...]),
    )
    rets = [
        Return(at, sends, makers[i], room, refs.take(2), out_place(ffn_out[i]), refs.take(n_ret))
        for i, room in enumerate((gate_w, up_w, down_w))
    ]
    for ret, out in zip(rets, ffn_out):
        ret.short = nz * unit - out.shape[1]

    def summed(make, first, cols):
        room = wa.at[:, :, pl.ds(first, cols)]
        ret = Return(at, sends, make, room, refs.take(2), None, refs.take(n_ret))
        (land,) = refs.take(1)
        ret.chain = ChainSum(at, sends, (ret.piece, land), refs.take(n_sum))
        return ret

    r_qkv = summed(lambda s1: turn_first(columns(normed1_b, s1), d_projb[...]), 0, qkv_cols)
    r_out = summed(lambda s1: turn_first(columns(d_resid_b, s1), attn[...]), qkv_cols, q_cols)
    r_dn2, r_ffn = (
        Reduce(at, sends, parts, refs.take(3), refs.take(n_red)) for parts in (dn2_part, ffn_part)
    )
    (d_resid_f, d_attn, d_score, dkv, dkv_land, dn1_part, dn1_land, small_b, small_land, small_z,
     small_zland, small_y, small_yland, cosine, sine, mask, dkvs, dkvr, shs, shr, szs, szr, ysems,
     yrecv) = refs.take(24)

    at.greet(everyone=True)
    w_small.over_z()
    w_small.own_block()
    for item in (w_qkv, w_out):
        item.over_z()
        item.own_block()
    my_half = cot_in.at[pl.ds(pl.multiple_of(at.y * half, SUBLANES), half)]
    sends.here(cot_in.at[pl.ds(0, half)], cot.at[at.z, 0], cot_sem.at[0])
    sends.here(cot_in.at[pl.ds(half, half)], cot.at[at.z, 1], cot_sem.at[1])
    seg = segments[...].astype(F32)
    row = lax.broadcasted_iota(jnp.int32, (rows, group_rows), 0) + at.z * rows
    col = lax.broadcasted_iota(jnp.int32, (rows, group_rows), 1)
    seg_row = jnp.sum(jnp.where(row == col, seg, 0.0), axis=1, keepdims=True)
    earlier = jnp.sum(jnp.where(seg < seg_row, 1.0, 0.0), axis=1, keepdims=True)
    mask[...] = jnp.where((seg == seg_row) & (col <= row), 1.0, 0.0)
    position = row[:, :1].astype(F32) - earlier
    lane = lax.broadcasted_iota(jnp.int32, (1, HD), 1)
    pair = lax.rem(lane, HD // 2).astype(F32)
    angle = position * jnp.exp(pair * (-2.0 * math.log(THETA) / HD))
    cosine[...] = jnp.cos(angle)
    sine[...] = jnp.sin(angle) * jnp.where(lane < HD // 2, -1.0, 1.0)
    for k in range(1, nz):
        for item in (w_small, w_qkv, w_out):
            item.pass_z([k])
    ffn[0].over_z()
    ffn[1].over_z()
    for item in ffn:
        item.own_block()

    hidden_f = hidden[...].astype(F32)
    factor1 = lax.rsqrt(jnp.mean(hidden_f * hidden_f, axis=1, keepdims=True) + EPSILON)
    w_small.pass_s()
    w_qkv.pass_s()
    w_out.pass_s()
    w_small.finish()
    gains = whole_lines(small, ns * nz, depth)
    normed1_b[...] = (hidden[...].astype(F32) * factor1 * gains[0:1, :]).astype(BF16)
    width_each = HD // (ns * nz)
    lane = lax.broadcasted_iota(jnp.int32, (8, LANES), 1)
    bias = jnp.zeros((8, LANES), F32)
    for b in range(ns * nz):
        line = small[b, 8:16, :].astype(F32)
        moved = pltpu.roll(line, b * width_each, 1) if b else line
        bias = jnp.where((lane >= b * width_each) & (lane < (b + 1) * width_each), moved, bias)
    w_qkv.finish()
    cos_t, sin_t = cosine[...], sine[...]

    def projected(head):
        weight = wa[:, :, head * HD:(head + 1) * HD].reshape(width, HD)
        return jnp.dot(normed1_b[...], weight, preferred_element_type=F32) + bias[head:head + 1, :]

    def rotated(values):
        return values * cos_t + pltpu.roll(values, HD // 2, 1) * sin_t

    for j in range(kv):
        kv_all[at.z, :, j * HD:(j + 1) * HD] = rotated(projected(heads + j)).astype(BF16)
        kv_all[at.z, :, (kv + j) * HD:(kv + j + 1) * HD] = projected(heads + kv + j).astype(BF16)
    for there, z2 in at.near():
        sends.go(
            kv_all.at[at.z], kv_all.at[at.z], kvs.at[z2], kvr.at[at.z], only=there, context=z2
        )
    ffn[2].over_z()
    t_cot.over_z(my_half)
    for h in range(heads):
        query[:, h * HD:(h + 1) * HD] = rotated(projected(h)).astype(BF16)
    ffn[0].pass_z()
    ffn[1].pass_z()
    for d in range(1, nz):
        z1 = at.z_from(d)
        landed(kv_all.at[z1], kvs.at[z1], kvr.at[z1], context=z1)

    def keys_of(j):
        return kv_all[:, :, j * HD:(j + 1) * HD].reshape(group_rows, HD)

    keep = mask[...] > 0
    for h in range(heads):
        keys, values = keys_of(h // repeat), keys_of(kv + h // repeat)
        scores = turn_last(query[:, h * HD:(h + 1) * HD], keys)
        scores = jnp.where(keep, scores * scale, -1e30)
        peak = jnp.max(scores, axis=1, keepdims=True)
        lse = peak + jnp.log(jnp.sum(jnp.exp(scores - peak), axis=1, keepdims=True))
        p = jnp.exp(scores - lse)
        probs[h * rows:(h + 1) * rows, :] = p
        out = jnp.dot(p.astype(BF16), values, preferred_element_type=F32)
        attn[:, h * HD:(h + 1) * HD] = out.astype(BF16)
    w_out.finish()
    out_w = wa[:, :, qkv_cols:qkv_cols + q_cols].reshape(width, q_cols)
    part = turn_last(attn[...], out_w).astype(BF16)
    ypart[0] = part[:half]
    ypart[1] = part[half:]
    sends.go(ypart.at[at.twin], yland, yps, ypr, tensor=at.twin)
    ffn[0].pass_s()

    landed(yland, yps, ypr, tensor=at.twin)
    base = pl.multiple_of(at.y * half, SUBLANES)
    total = ypart[at.y].astype(F32) + yland[...].astype(F32)
    res = hidden[pl.ds(base, half), :].astype(F32) + total
    resid[...] = res
    factor2 = lax.rsqrt(jnp.mean(res * res, axis=1, keepdims=True) + EPSILON)
    n2[at.z, at.y] = (res * factor2 * gains[1:2, :]).astype(BF16)
    t_n2.over_z(n2.at[at.z, at.y])
    t_n2.over_y(at.z, n2.at[at.z, at.y])
    ffn[1].pass_s()
    ffn[2].pass_z()
    t_cot.pass_z()
    t_n2.pass_z([1])
    ffn[2].pass_s()
    t_cot.wait_y(range(nz), lambda z1: at.z != z1)
    for item in ffn:
        item.finish()
    for copy in sends.local:
        copy.wait()
    sends.local = []

    def weight(ref):
        return ref[...].reshape(width, -1)

    d_act[...] = jnp.dot(cot[...].reshape(group_rows, width), weight(down_w), preferred_element_type=F32)
    few, tall = nz // 2, 32
    chunk = few * rows

    def half_block(first):
        t_n2.wait_y([first * few + i for i in range(few)])
        start = pl.multiple_of(first * chunk, chunk)
        mine = n2[pl.ds(first * few, few)].reshape(chunk, width)
        gate[...] = jnp.dot(mine, weight(gate_w), preferred_element_type=F32)
        up_val[...] = jnp.dot(mine, weight(up_w), preferred_element_type=F32)

        @pl.loop(0, chunk // tall)
        def _(i):
            line = pl.ds(pl.multiple_of(i * tall, tall), tall)
            whole = pl.ds(pl.multiple_of(start + i * tall, tall), tall)
            g, u, d = gate[line, :], up_val[line, :], d_act[whole, :]
            sigma = jax.nn.sigmoid(g)
            silu_val = g * sigma
            act[whole, :] = (silu_val * u).astype(BF16)
            d_gate[whole, :] = (d * u * sigma * (1.0 + g * (1.0 - sigma))).astype(BF16)
            d_up[whole, :] = (d * silu_val).astype(BF16)

        span = pl.ds(start, chunk)
        dn2_part[pl.ds(first * few, few)] = (
            turn_last(d_gate[span, :], weight(gate_w)) + turn_last(d_up[span, :], weight(up_w))
        ).astype(BF16).reshape(few, 2, half, width)
        r_dn2.over_y([first * few + i for i in range(few)])

    nearer = lax.div(at.z, few)
    t_n2.pass_z(range(2, nz - 1))
    half_block(nearer)
    t_n2.pass_z([nz - 1])
    half_block(1 - nearer)
    w_sends.drain()

    rets[0].give_all()
    rets[0].over_s()
    r_dn2.pass_y(far_first(nz))
    rets[0].over_z(last=False)
    rets[1].give_all()
    rets[1].over_s()
    res = resid[...]
    factor2 = lax.rsqrt(jnp.mean(res * res, axis=1, keepdims=True) + EPSILON)
    unit2 = res * factor2
    dn2 = r_dn2.total()
    grad_g2 = jnp.sum(dn2 * unit2, axis=0, keepdims=True)
    scaled = dn2 * gains[1:2, :]
    back2 = factor2 * (scaled - unit2 * jnp.mean(scaled * unit2, axis=1, keepdims=True))
    d_res = cot[at.z, at.y].astype(F32) + back2
    d_resid_f[at.y] = d_res
    d_resid_b[at.y] = d_res.astype(BF16)
    mine_b, mine_f = d_resid_b.at[at.y], d_resid_f.at[at.y]
    sends.go(mine_b, mine_b, ysems.at[0], yrecv.at[0], tensor=at.twin)
    ffn_part[...] = turn_last(act[...], weight(down_w)).astype(BF16).reshape(nz, 2, half, width)
    rets[2].give_all()
    rets[2].over_s()
    rets[0].over_z(first=False)
    landed(d_resid_b.at[at.twin], ysems.at[0], yrecv.at[0], tensor=at.twin)
    r_ffn.over_y(far_first(nz))
    sends.go(mine_f, mine_f, ysems.at[1], yrecv.at[1], tensor=at.twin)

    d_resid_all = d_resid_b[...].reshape(rows, width)
    out_w = wa[:, :, qkv_cols:qkv_cols + q_cols].reshape(width, q_cols)
    d_attn[...] = jnp.dot(d_resid_all, out_w, preferred_element_type=F32).astype(BF16)
    r_out.give_all()
    r_out.over_s()

    def unrotated(values):
        return values * cos_t - pltpu.roll(values, HD // 2, 1) * sin_t

    bias_rows = [None] * (heads + 2 * kv)

    def place(head, grad):
        bias_rows[head] = jnp.sum(grad, axis=0, keepdims=True)
        d_projb[:, head * HD:(head + 1) * HD] = grad.astype(BF16)

    for j in range(kv):
        keys, values = keys_of(j), keys_of(kv + j)
        d_values = jnp.zeros((group_rows, HD), F32)
        d_keys = jnp.zeros((group_rows, HD), F32)
        for h in range(j * repeat, (j + 1) * repeat):
            d_out = d_attn[:, h * HD:(h + 1) * HD]
            p = probs[h * rows:(h + 1) * rows, :]
            d_prob = turn_last(d_out, values)
            delta = jnp.sum(
                d_out.astype(F32) * attn[:, h * HD:(h + 1) * HD].astype(F32), axis=1, keepdims=True
            )
            d_score[...] = (p * (d_prob - delta)).astype(BF16)
            d_query = jnp.dot(d_score[...], keys, preferred_element_type=F32)
            place(h, unrotated(d_query * scale))
            d_keys = d_keys + turn_first(d_score[...], query[:, h * HD:(h + 1) * HD])
            d_values = d_values + turn_first(p.astype(BF16), d_out)
        for i, grad in ((j, d_keys * scale), (kv + j, d_values)):
            dkv[:, :, i * HD:(i + 1) * HD] = grad.astype(BF16).reshape(nz, rows, HD)
    for there, z2 in at.near():
        sends.go(dkv.at[z2], dkv_land.at[at.z], dkvs.at[z2], dkvr.at[at.z], only=there, context=z2)
    rets[1].over_z(last=False)
    d_own = dkv[at.z].astype(F32)
    for d in range(1, nz):
        z1 = at.z_from(d)
        landed(dkv_land.at[z1], dkvs.at[z1], dkvr.at[z1], context=z1)
        d_own = d_own + dkv_land[z1].astype(F32)
    for j in range(kv):
        place(heads + j, unrotated(d_own[:, j * HD:(j + 1) * HD]))
        place(heads + kv + j, d_own[:, (kv + j) * HD:(kv + j + 1) * HD])
    qkv_w = wa[:, :, :qkv_cols].reshape(width, qkv_cols)
    dn1_part[...] = turn_last(d_projb[...], qkv_w).astype(BF16)
    sends.go(dn1_part, dn1_land, ysems.at[2], yrecv.at[2], tensor=at.twin)
    r_qkv.give_all()
    r_qkv.over_s()
    rets[1].over_z(first=False)
    r_ffn.pass_y(far_first(nz))
    rets[2].over_z(last=False)
    r_out.over_z()

    block_out[at.y] = (r_ffn.total() + resid[...]).astype(BF16)
    sends.go(block_out.at[at.y], block_out.at[at.y], ysems.at[3], yrecv.at[3], tensor=at.twin)

    landed(dn1_land, ysems.at[2], yrecv.at[2], tensor=at.twin)
    landed(d_resid_f.at[at.twin], ysems.at[1], yrecv.at[1], tensor=at.twin)
    dn1 = dn1_part[...].astype(F32) + dn1_land[...].astype(F32)
    hidden_f = hidden[...].astype(F32)
    factor1 = lax.rsqrt(jnp.mean(hidden_f * hidden_f, axis=1, keepdims=True) + EPSILON)
    unit1 = hidden_f * factor1
    row = lax.broadcasted_iota(jnp.int32, (rows, 1), 0)
    my_row = (row >= at.y * half) & (row < (at.y + 1) * half)
    grad_g1 = jnp.sum(jnp.where(my_row, dn1 * unit1, 0.0), axis=0, keepdims=True)
    scaled = dn1 * gains[0:1, :]
    back1 = factor1 * (scaled - unit1 * jnp.mean(scaled * unit1, axis=1, keepdims=True))
    input_grad[...] = d_resid_f[...].reshape(rows, width) + back1

    both = jnp.concatenate([grad_g1, grad_g2, jnp.zeros((6, width), F32)], axis=0)
    bias = jnp.concatenate(bias_rows, axis=0)
    for b in range(ns * nz):
        moved = pltpu.roll(bias, LANES - b * width_each, 1) if b else bias
        small_b[b // nz, b % nz] = jnp.concatenate([piece_of_lines(both, b, depth), moved], axis=0)
    for k in range(1, ns):
        s2 = lax.rem(at.s + k, ns)
        sends.go(small_b.at[s2], small_land.at[k], shs.at[k], shr.at[k], shard=s2)
    rets[2].over_z(first=False)
    total = small_b[at.s]
    for k in range(1, ns):
        s1 = lax.rem(at.s - k + ns, ns)
        landed(small_land.at[k], shs.at[k], shr.at[k], shard=s1)
        total = total + small_land[k]
    small_z[...] = total
    for d in range(1, nz):
        sends.go(small_z.at[at.z_to(d)], small_zland.at[d], szs.at[d], szr.at[d], context=at.z_to(d))
    r_qkv.over_z()
    total = small_z[at.z]
    for d in range(1, nz):
        landed(small_zland.at[d], szs.at[d], szr.at[d], context=at.z_from(d))
        total = total + small_zland[d]
    small_y[...] = total
    sends.go(small_y, small_yland, ysems.at[4], yrecv.at[4], tensor=at.twin)
    out_grad[...] = r_out.chain.total(r_out.piece(at.z)[...].astype(F32))
    qkv_grad[...] = r_qkv.chain.total(r_qkv.piece(at.z)[...].astype(F32))
    landed(small_yland, ysems.at[4], yrecv.at[4], tensor=at.twin)
    small_out[:8, :] = small_y[:8, :] + small_yland[:8, :]
    small_out[8:, :] = small_y[8:, :]
    landed(block_out.at[at.twin], ysems.at[3], yrecv.at[3], tensor=at.twin)
    for ret in rets:
        ret.finish()
    sends.drain()


def layer(ns, nz, heads, kv, hidden_units, qkv_in, out_in, small_in, ffn_in, hidden, cot, segments):
    rows, width = hidden.shape
    owners, half, group_rows = ns * nz, rows // 2, nz * rows
    depth, cols = qkv_in.shape[0], qkv_in.shape[1] + out_in.shape[1]
    unit = ffn_in[0].shape[2]
    q_cols, kv_cols = heads * HD, 2 * kv * HD
    qkv_cols = q_cols + kv_cols
    dma = pltpu.SemaphoreType.DMA
    shape = jax.ShapeDtypeStruct
    room = pltpu.VMEM
    vmem = pl.BlockSpec(memory_space=pltpu.VMEM)
    anyspace = pl.BlockSpec(memory_space=pl.ANY)
    scratch = [room((ns, nz * depth, cols), BF16)] + [room((ns, nz * depth, unit), BF16)] * 3
    scratch += [
        room((owners, 16, LANES), BF16),
        room((2, half, width), BF16),
        room((half, width), BF16),
        room((nz, 2, half, width), BF16),
        room((nz, 2, half, width), BF16),
        room((half, width), F32),
        room((rows, q_cols), BF16),
        room((nz, rows, kv_cols), BF16),
        room((heads * rows, group_rows), F32),
        room((rows, q_cols), BF16),
    ]
    scratch += Spread.sems(ns, nz) * 6 + Tokens.sems(nz) * 2
    scratch += [dma((nz,)), dma((nz,)), dma, dma, dma((2,))]
    scratch += [room((group_rows // 2, unit), F32)] * 2 + [room((group_rows, unit), F32)]
    scratch += [room((group_rows, unit), BF16)] * 3 + [room((nz, 2, half, width), BF16)] * 2
    scratch += [
        room((rows, width), BF16), room((2, half, width), BF16), room((rows, qkv_cols), BF16),
    ]
    for _ in range(3):
        scratch += Return.lands(ns, nz, depth, unit) + Return.sems(ns, nz)
    for n in (qkv_cols, q_cols):
        scratch += Return.lands(ns, nz, depth, n) + Return.sems(ns, nz)
        scratch += ChainSum.bufs(nz, (depth, n))[1:] + ChainSum.sems(nz)
    for _ in range(2):
        scratch += Reduce.bufs(nz, half, width) + Reduce.sems(nz)
    scratch += [
        room((2, half, width), F32),
        room((rows, q_cols), BF16),
        room((rows, group_rows), BF16),
        room((nz, rows, kv_cols), BF16),
        room((nz, rows, kv_cols), BF16),
        room((rows, width), BF16),
        room((rows, width), BF16),
        room((ns, nz, 16, LANES), F32),
        room((ns, nz, 16, LANES), F32),
        room((nz, 16, LANES), F32),
        room((nz, 16, LANES), F32),
        room((16, LANES), F32),
        room((16, LANES), F32),
        room((rows, HD), F32),
        room((rows, HD), F32),
        room((rows, group_rows), F32),
        dma((nz,)), dma((nz,)), dma((ns,)), dma((ns,)), dma((nz,)), dma((nz,)), dma((5,)), dma((5,)),
    ]
    return pl.pallas_call(
        functools.partial(layer_kernel, ns, nz, heads, kv),
        out_shape=[
            shape((2, half, width), BF16),
            shape((rows, width), F32),
            shape((depth, qkv_cols), F32),
            shape((depth, q_cols), F32),
            shape((16, LANES), F32),
            *[shape((depth, hidden_units), BF16)] * 3,
        ],
        in_specs=[anyspace] * 6 + [vmem, anyspace, vmem],
        out_specs=[vmem] * 5 + [anyspace] * 3,
        scratch_shapes=scratch,
        compiler_params=pltpu.CompilerParams(
            collective_id=0, has_side_effects=True, vmem_limit_bytes=VMEM_BYTES
        ),
    )(qkv_in, out_in, small_in, *ffn_in, hidden, cot, segments)


def fast_step(
    ns,
    nz,
    hidden_in,
    segment_ids,
    attn_gain,
    qkv_weight,
    qkv_bias,
    out_weight,
    ffn_gain,
    gate_weight,
    up_weight,
    down_weight,
    out_cotangent,
):
    rows, width = hidden_in.shape
    depth, hidden_units = gate_weight.shape
    parts = 2
    heads = H // parts
    kv = KVH // parts
    unit_cols = -(-hidden_units // (nz * LANES)) * LANES
    padded = unit_cols * nz

    def by_place(weight):
        full = jnp.pad(weight, ((0, 0), (0, padded - hidden_units)))
        return jnp.transpose(full.reshape(depth, nz, unit_cols), (1, 0, 2))

    ffn_in = [by_place(w) for w in (gate_weight, up_weight, down_weight.T)]
    gains_in = jnp.pad(jnp.stack([attn_gain, ffn_gain]), ((0, 6), (0, LANES - depth)))
    bias_in = jnp.pad(qkv_bias, ((0, 0), (0, LANES - qkv_bias.shape[1])))
    small_in = jnp.concatenate([gains_in, bias_in], axis=0)

    block_out, input_grad, grad_qkv, grad_out, small, grad_gate, grad_up, grad_down = layer(
        ns, nz, heads, kv, hidden_units, qkv_weight, out_weight.T, small_in, ffn_in, hidden_in,
        out_cotangent, segment_ids,
    )

    return (
        block_out.reshape(rows, width),
        input_grad,
        small[0, :depth],
        grad_qkv,
        small[8:, : qkv_bias.shape[1]],
        grad_out.T,
        small[1, :depth],
        grad_gate.astype(F32),
        grad_up.astype(F32),
        grad_down.astype(F32).T,
    )


def general_step(
    hidden_in,
    segment_ids,
    attn_gain,
    qkv_weight,
    qkv_bias,
    out_weight,
    ffn_gain,
    gate_weight,
    up_weight,
    down_weight,
    out_cotangent,
):
    rows, width = hidden_in.shape
    depth = gate_weight.shape[0]
    hidden_units = gate_weight.shape[1]
    parts = lax.axis_size("tensor")
    blocks = lax.axis_size("context")
    heads = H // parts
    kv = KVH // parts
    repeat = H // KVH
    scale = HD ** (-0.5)
    block_index = lax.axis_index("context")
    part_index = lax.axis_index("tensor")
    half_rows = rows // parts
    unit_cols = -(-hidden_units // (blocks * LANES)) * LANES
    padded = unit_cols * blocks

    def spread(weight):
        full = jnp.pad(weight, ((0, 0), (0, padded - hidden_units)))
        mine = lax.all_to_all(full, "context", split_axis=1, concat_axis=0, tiled=True)
        mine = mine.reshape(blocks * depth, unit_cols)
        return lax.all_gather(mine, "shard", axis=0, tiled=True)

    gate_full = spread(gate_weight)
    up_full = spread(up_weight)
    down_full = spread(down_weight.T)
    gain_one = lax.all_gather(attn_gain, OWNERS, axis=0, tiled=True).astype(F32)
    gain_two = lax.all_gather(ffn_gain, OWNERS, axis=0, tiled=True).astype(F32)
    bias = lax.all_gather(qkv_bias, OWNERS, axis=1, tiled=True).reshape(-1).astype(F32)
    qkv_full = lax.all_gather(qkv_weight, OWNERS, axis=0, tiled=True)
    out_full = lax.all_gather(out_weight.T, OWNERS, axis=0, tiled=True)

    seg_all = segment_ids[0]
    group_rows = seg_all.shape[0]
    first_row = block_index * rows
    index_all = jnp.arange(group_rows, dtype=jnp.int32)
    earlier = jnp.sum((seg_all[None, :] < seg_all[:, None]).astype(jnp.int32), axis=1)
    positions = index_all - earlier
    seg_local = lax.dynamic_slice_in_dim(seg_all, first_row, rows)
    index_local = first_row + jnp.arange(rows, dtype=jnp.int32)
    allowed = (seg_local[:, None] == seg_all[None, :]) & (
        index_local[:, None] >= index_all[None, :]
    )
    cosine, sine = rotary_tables(positions)
    cos_local = lax.dynamic_slice_in_dim(cosine, first_row, rows)
    sin_local = lax.dynamic_slice_in_dim(sine, first_row, rows)

    hidden_all = lax.all_gather(hidden_in, "context", axis=0, tiled=True)
    normed_all, _, _ = norm_forward(hidden_all.astype(F32), gain_one)
    hidden_f = hidden_in.astype(F32)
    normed1, unit1, factor1 = norm_forward(hidden_f, gain_one)
    q_cols = heads * HD
    k_cols = kv * HD
    query_f = dot(normed1, qkv_full[:, :q_cols]) + bias[:q_cols]
    kv_f = dot(normed_all, qkv_full[:, q_cols:]) + bias[q_cols:]
    query = jnp.transpose(query_f.reshape(rows, heads, HD), (1, 0, 2))
    query = rotate(query, cos_local, sin_local).astype(BF16)
    keys = jnp.transpose(kv_f[:, :k_cols].reshape(group_rows, kv, HD), (1, 0, 2))
    keys = rotate(keys, cosine, sine).astype(BF16)
    values = jnp.transpose(kv_f[:, k_cols:].reshape(group_rows, kv, HD), (1, 0, 2)).astype(BF16)
    query = query.reshape(kv, repeat * rows, HD)
    mask = jnp.tile(allowed, (repeat, 1))
    scores = jnp.where(mask, batched(query, keys, 2, 2) * scale, -1e30)
    peak = jnp.max(scores, axis=2, keepdims=True)
    lse = peak + jnp.log(jnp.sum(jnp.exp(scores - peak), axis=2, keepdims=True))
    p_soft = jnp.exp(scores - lse)
    probs = p_soft.astype(BF16)
    outs = batched(probs, values, 2, 1).astype(BF16)
    attn = jnp.transpose(outs.reshape(heads, rows, HD), (1, 0, 2)).reshape(rows, q_cols)
    attn_part = contract_last(attn, out_full).astype(BF16)

    mine = part_index * half_rows
    attn_half = lax.psum_scatter(attn_part, "tensor", scatter_dimension=0, tiled=True)
    resid_half = lax.dynamic_slice_in_dim(hidden_f, mine, half_rows) + attn_half.astype(F32)
    normed2_half, unit2, factor2 = norm_forward(resid_half, gain_two)
    normed2 = lax.all_gather(normed2_half, TEAM, axis=0, tiled=True)
    cot_half = lax.dynamic_slice_in_dim(out_cotangent, mine, half_rows)
    cot = lax.all_gather(cot_half, TEAM, axis=0, tiled=True)

    gate = dot(normed2, gate_full)
    up_val = dot(normed2, up_full)
    sigma = jax.nn.sigmoid(gate)
    silu_val = gate * sigma
    act = (silu_val * up_val).astype(BF16)
    ffn_part = contract_last(act, down_full).astype(BF16)
    d_act = dot(cot, down_full)
    d_gate = (d_act * up_val * sigma * (1.0 + gate * (1.0 - sigma))).astype(BF16)
    d_up = (d_act * silu_val).astype(BF16)
    dn2_part = (contract_last(d_gate, gate_full) + contract_last(d_up, up_full)).astype(BF16)
    ffn_half = lax.psum_scatter(ffn_part, TEAM, scatter_dimension=0, tiled=True)
    block_half = (resid_half + ffn_half.astype(F32)).astype(BF16)
    block_out = lax.all_gather(block_half, "tensor", axis=0, tiled=True)
    dn2_half = lax.psum_scatter(dn2_part, TEAM, scatter_dimension=0, tiled=True).astype(F32)
    grad_g2, d_back2 = norm_backward(dn2_half, unit2, factor2, gain_two)
    d_resid_half = cot_half.astype(F32) + d_back2

    def give_back(grad):
        part = lax.psum_scatter(grad.astype(BF16), "shard", scatter_dimension=0, tiled=True)
        part = part.reshape(blocks, depth, unit_cols)
        part = lax.all_to_all(part, "context", split_axis=0, concat_axis=2, tiled=True)
        return part.reshape(depth, padded)[:, :hidden_units].astype(F32)

    sum_gate = give_back(contract_first(normed2, d_gate))
    sum_up = give_back(contract_first(normed2, d_up))
    sum_down = give_back(contract_first(cot, act)).T

    d_resid_b = lax.all_gather(d_resid_half.astype(BF16), "tensor", axis=0, tiled=True)
    grad_out = contract_first(d_resid_b, attn)
    d_attn = dot(d_resid_b, out_full).astype(BF16)
    d_outs = jnp.transpose(d_attn.reshape(rows, heads, HD), (1, 0, 2)).reshape(
        kv, repeat * rows, HD
    )
    d_prob = batched(d_outs, values, 2, 2)
    delta = jnp.sum(d_outs.astype(F32) * outs.astype(F32), axis=2, keepdims=True)
    d_score = (p_soft * (d_prob - delta)).astype(BF16)
    d_query = batched(d_score, keys, 2, 1) * scale
    d_keys = batched(d_score, query, 1, 1) * scale
    d_values = batched(probs, d_outs, 1, 1)
    d_kv = jnp.concatenate([d_keys, d_values], axis=0).astype(BF16)
    d_kv = lax.psum_scatter(d_kv, "context", scatter_dimension=1, tiled=True).astype(F32)
    d_query = unrotate(d_query.reshape(heads, rows, HD), cos_local, sin_local)
    d_keys = unrotate(d_kv[:kv], cos_local, sin_local)
    d_proj = jnp.transpose(jnp.concatenate([d_query, d_keys, d_kv[kv:]], axis=0), (1, 0, 2))
    grad_bias = jnp.sum(d_proj, axis=0)
    d_projb = d_proj.reshape(rows, -1).astype(BF16)
    grad_qkv = contract_first(normed1, d_projb)
    dn1_part = contract_last(d_projb, qkv_full).astype(BF16)
    dn1_half = lax.psum_scatter(dn1_part, "tensor", scatter_dimension=0, tiled=True).astype(F32)
    unit1_half = lax.dynamic_slice_in_dim(unit1, mine, half_rows)
    factor1_half = lax.dynamic_slice_in_dim(factor1, mine, half_rows)
    grad_g1, d_back1 = norm_backward(dn1_half, unit1_half, factor1_half, gain_one)
    input_grad = lax.all_gather(d_resid_half + d_back1, "tensor", axis=0, tiled=True)

    gains = lax.psum(jnp.stack([grad_g1, grad_g2]), "tensor")
    sum_gains = lax.psum_scatter(gains, OWNERS, scatter_dimension=1, tiled=True)
    sum_qkv = lax.psum_scatter(grad_qkv.astype(BF16), OWNERS, scatter_dimension=0, tiled=True)
    sum_bias = lax.psum_scatter(grad_bias, OWNERS, scatter_dimension=1, tiled=True)
    sum_out = lax.psum_scatter(grad_out.astype(BF16), OWNERS, scatter_dimension=0, tiled=True)
    return (
        block_out,
        input_grad,
        sum_gains[0],
        sum_qkv.astype(F32),
        sum_bias,
        sum_out.astype(F32).T,
        sum_gains[1],
        sum_gate,
        sum_up,
        sum_down,
    )


def solution(mesh):
    ns, nz, parts = (mesh.shape[a] for a in ("shard", "context", "tensor"))
    rows = P(OWNERS, None)

    def local(*args):
        depth = args[7].shape[0]
        if depth % SUBLANES == 0 and ns % 2 == 0 and ns > 2 and nz % 2 == 0 and parts == 2:
            return fast_step(ns, nz, *args)
        return general_step(*args)

    placed = (
        rows,
        P("shard", None),
        P(OWNERS),
        P(OWNERS, "tensor"),
        P("tensor", OWNERS),
        P("tensor", OWNERS),
        P(OWNERS),
        P(OWNERS, "tensor"),
        P(OWNERS, "tensor"),
        P("tensor", OWNERS),
        rows,
    )
    return jax.shard_map(
        local,
        mesh=mesh,
        in_specs=placed,
        out_specs=(
            rows,
            rows,
            P(OWNERS),
            P(OWNERS, "tensor"),
            P("tensor", OWNERS),
            P("tensor", OWNERS),
            P(OWNERS),
            P(OWNERS, "tensor"),
            P(OWNERS, "tensor"),
            P("tensor", OWNERS),
        ),
        check_vma=False,
    )
```
